32 devices in a mesh: dp: 4 (over z), seq: 8 (over y, x, core).
Axes of the slice: x: 2, y: 2, z: 4, core: 2. Of those that a mesh axis runs over, the one named last changes fastest.
Arguments:
- inputs: bfloat16 [32, 2048, 512], P('dp', 'seq'), may hold values from -6 to 6
- segments: int32 [32, 2048], P('dp'), may hold values from 0 to 7, never falling along the last dimension, each value on 1 to 1024 neighbouring positions
- w_qkv: bfloat16 [2, 512, 1536], P(None, ('dp', 'seq')), may hold values from -0.25 to 0.25
- w_out: bfloat16 [2, 512, 512], P(None, ('dp', 'seq')), may hold values from -1 to 1
- w_up: bfloat16 [2, 512, 2048], P(None, ('dp', 'seq')), may hold values from -0.25 to 0.25
- w_down: bfloat16 [2, 2048, 512], P(None, ('dp', 'seq')), may hold values from -0.125 to 0.125
- gain_attn: bfloat16 [2, 512], P(None, ('dp', 'seq')), may hold values from 0.5 to 1.5
- gain_mlp: bfloat16 [2, 512], P(None, ('dp', 'seq')), may hold values from 0.5 to 1.5
- cotangent: bfloat16 [32, 2048, 512], P('dp', 'seq'), may hold values from -6 to 6
Outputs:
- outputs: bfloat16 [32, 2048, 512], P('dp', 'seq')
- input_grad: float32 [32, 2048, 512], P('dp', 'seq')
- grad_qkv: float32 [2, 512, 1536], P(None, ('dp', 'seq'))
- grad_out: float32 [2, 512, 512], P(None, ('dp', 'seq'))
- grad_up: float32 [2, 512, 2048], P(None, ('dp', 'seq'))
- grad_down: float32 [2, 2048, 512], P(None, ('dp', 'seq'))
- grad_gain_attn: float32 [2, 512], P(None, ('dp', 'seq'))
- grad_gain_mlp: float32 [2, 512], P(None, ('dp', 'seq'))
The draws below stay inside these ranges and needn't reach their ends.
Inputs may be any that keep to these rules, and one draw needn't show every extreme that they name: `segments`: in each sequence the ids never fall, each document has 1 to 1024 tokens, and one has exactly 1024.
All inputs are finite; a program needn't handle non-finite values.
Results may differ from the reference program's by a relative error of at most 0.017.
Values may be sent and summed in bfloat16 or wider, within the bound.
A program may use at most 256 MiB of HBM per device.

```python
import math
import jax
import jax.numpy as jnp
import numpy as np
from jax import lax

D = 512
HEADS = 8
HEAD = 64
FF = 2048
SPAN = 128
LAYERS = 2
DOCS = 8
LEN = 2048
BATCH = 32


def shard_levels(stream_key, dims, shards, least, largest):
    def one(axis_at, blocks):
        draws = jax.random.uniform(jax.random.fold_in(jax.random.fold_in(stream_key, 6), axis_at), (blocks,), jnp.float32, least / len(shards), largest / len(shards))
        return jnp.repeat(jnp.exp(draws), dims[axis_at] // blocks).reshape((-1,) + (1,) * (len(dims) - axis_at - 1))

    level = one(*shards[0])
    for cut in shards[1:]:
        level = level * one(*cut)
    return level


def length_profile(count, total, most, lean):
    portions = [(1 << 20) // math.isqrt(rank ** lean) + 1 for rank in range(2, count + 1)]
    spare, counts = total - most - (count - 1), [1] * (count - 1)
    while spare > 0:
        free = [i for i in range(count - 1) if counts[i] < most]
        pool, budget = sum([portions[i] for i in free]), spare
        for i in free:
            extra = min(most - counts[i], max(1, budget * portions[i] // pool), spare)
            counts[i] = counts[i] + extra
            spare = spare - extra
    return np.array([most] + counts)


def ragged(key, count, total, most, skew):
    if count == 2:
        one = jax.random.randint(key, (), max(1, total - most), min(most, total - 1) + 1)
        return jnp.stack([one, total - one])
    sizes = jnp.asarray(length_profile(count, total, most, skew), jnp.int32)
    twos = (count - 1) // 2
    donor, sink = sizes[1:1 + 2 * twos:2], sizes[2:2 + 2 * twos:2]
    room = jnp.minimum(donor - 1, most - sink)
    passed = jax.random.randint(jax.random.fold_in(key, 1), (twos,), 0, 1 << 20) % (room + 1)
    sizes = sizes.at[1:1 + 2 * twos:2].set(donor - passed).at[2:2 + 2 * twos:2].set(sink + passed)
    return sizes[jax.random.permutation(jax.random.fold_in(key, 2), count)]


def gaussian(own_key, dims, spread, bound, split=(), held_as=jnp.bfloat16):
    values = spread * jax.random.normal(own_key, dims, jnp.float32)
    if split:
        values = values * shard_levels(own_key, dims, split, -0.22, 0.18)
    return jnp.clip(values, -bound, bound).astype(held_as)


def setup_inputs(seed: int = 0) -> dict:
    arg_keys = jax.random.split(jax.random.key(seed), 10)
    return {
        "inputs": gaussian(arg_keys[0], (BATCH, LEN, D), 1.0, 6.0, ((0, 4), (1, 8))),
        "segments": jax.vmap(lambda own: jnp.searchsorted(jnp.cumsum(ragged(own, DOCS, LEN, LEN // 2, 2)), jnp.arange(LEN), side="right"))(jax.random.split(arg_keys[1], BATCH)).reshape((BATCH, LEN)).astype(jnp.int32),
        "w_qkv": gaussian(arg_keys[2], (LAYERS, D, 3 * D), D ** -0.5, 0.25, ((1, 32),)),
        "w_out": gaussian(arg_keys[3], (LAYERS, D, D), (D // 16) ** -0.5, 1.0, ((1, 32),)),
        "w_up": gaussian(arg_keys[4], (LAYERS, D, FF), D ** -0.5, 0.25, ((1, 32),)),
        "w_down": gaussian(arg_keys[5], (LAYERS, FF, D), FF ** -0.5, 0.125, ((1, 32),)),
        "gain_attn": jnp.clip(1.0 + 0.1 * jax.random.normal(arg_keys[6], (LAYERS, D), jnp.float32), 0.5, 1.5).astype(jnp.bfloat16),
        "gain_mlp": jnp.clip(1.0 + 0.1 * jax.random.normal(arg_keys[7], (LAYERS, D), jnp.float32), 0.5, 1.5).astype(jnp.bfloat16),
        "cotangent": gaussian(arg_keys[8], (BATCH, LEN, D), 1.0, 6.0, ((0, 4), (1, 8))),
    }


@jax.custom_vjp
def low(v):
    return lax.optimization_barrier(v.astype(jnp.bfloat16)).astype(jnp.float32)

@jax.custom_vjp
def low_back(v):
    return v

def low_keep(v):
    return (low(v), None)

def low_pass(kept, grad):
    return (grad,)

def back_keep(v):
    return (v, None)

def back_low(kept, grad):
    return (low(grad),)
low.defvjp(low_keep, low_pass)
low_back.defvjp(back_keep, back_low)
EPS = 1e-05
NEG = -1000000000.0
HI = lax.Precision.HIGHEST

def layer_norm(values, gain):
    mean = lax.optimization_barrier(jnp.mean(values, -1, keepdims=True))
    centred = values - mean
    var = lax.optimization_barrier(jnp.mean(centred * centred, -1, keepdims=True))
    return centred * lax.rsqrt(var + EPS) * gain

def gelu(values):
    return 0.5 * values * (1.0 + jnp.tanh(0.7978845608 * (values + 0.044715 * values * values * values)))

def matmul(left, right):
    return jnp.dot(left, right, precision=HI)

def attend(qkv, seg):
    length = qkv.shape[0]
    spans = length // SPAN
    query = qkv[:, :D].reshape(spans, SPAN, HEADS, HEAD)
    keys = qkv[:, D:2 * D].reshape(spans, SPAN, HEADS, HEAD)
    values = qkv[:, 2 * D:].reshape(spans, SPAN, HEADS, HEAD)
    ksum = low(lax.optimization_barrier(jnp.mean(qkv[:, D:2 * D].reshape(spans, SPAN, D), 1))).reshape(spans, HEADS, HEAD)
    vsum = low(lax.optimization_barrier(jnp.mean(qkv[:, 2 * D:].reshape(spans, SPAN, D), 1))).reshape(spans, HEADS, HEAD)
    scale = HEAD ** (-0.5)
    near = jnp.einsum('nqhe,nkhe->nhqk', query, keys, precision=HI) * scale
    far = jnp.einsum('nqhe,mhe->nhqm', query, ksum, precision=HI) * scale
    scores = low_back(jnp.concatenate([near, far], -1))
    segq = seg.reshape(spans, SPAN)
    ends = segq[:, SPAN - 1]
    pos = jnp.arange(SPAN)
    near_mask = (segq[:, :, None] == segq[:, None, :]) & (pos[None, :, None] >= pos[None, None, :])
    span_ids = jnp.arange(spans)
    far_mask = (span_ids[None, None, :] < span_ids[:, None, None]) & (ends[None, None, :] == segq[:, :, None])
    mask = jnp.concatenate([near_mask, far_mask], -1)[:, None]
    scores = jnp.where(mask, scores, NEG)
    prob = low(jax.nn.softmax(scores, -1))
    out = jnp.einsum('nhqk,nkhe->nqhe', prob[..., :SPAN], values, precision=HI)
    out = out + jnp.einsum('nhqm,mhe->nqhe', prob[..., SPAN:], vsum, precision=HI)
    return low(low_back(out.reshape(length, D)))

def layer(xs, seg, wq, wo, wu, wd, g1, g2):
    n1 = low(layer_norm(xs, g1))
    qkv = low(low_back(matmul(n1, wq)))
    o = attend(qkv, seg)
    h = xs + low_back(matmul(o, wo))
    n2 = low(layer_norm(h, g2))
    u = low_back(matmul(n2, wu))
    act = low(gelu(u))
    return h + low_back(matmul(act, wd))

def reference(inputs, segments, w_qkv, w_out, w_up, w_down, gain_attn, gain_mlp, cotangent):
    floats = [a.astype(jnp.float32) for a in (inputs, w_qkv, w_out, w_up, w_down, gain_attn, gain_mlp)]

    def forward(x, wq, wo, wu, wd, g1, g2):

        def one(pair):
            xs, seg = pair
            for index in range(LAYERS):
                xs = layer(xs, seg, wq[index], wo[index], wu[index], wd[index], g1[index], g2[index])
            return xs
        return lax.map(jax.checkpoint(one), (x, segments))
    result, pull = jax.vjp(forward, *floats)
    grads = pull(cotangent.astype(jnp.float32))
    return (result.astype(jnp.bfloat16), grads[0], grads[1], grads[2], grads[3], grads[4], grads[5], grads[6])
```

```python
import functools

import jax
import jax.numpy as jnp
from jax import lax
from jax.experimental import pallas as pl
from jax.experimental.pallas import tpu as pltpu
from jax.sharding import PartitionSpec as P

D = 512
HEADS = 8
HEAD = 64
SPAN = 128
PAIRS = HEADS // 2
EPS = 1e-05
NEG = -1000000000.0
SCALE = HEAD ** (-0.5)
F32 = jnp.float32
BF16 = jnp.bfloat16
CHUNK = 512
VMEM_LIMIT = 60 * 1024 * 1024

NN = (((1,), (0,)), ((), ()))
NT = (((1,), (1,)), ((), ()))
TN = (((0,), (0,)), ((), ()))


def dot(left, right, dims=NN):
    return lax.dot_general(left, right, dims, preferred_element_type=F32)


def normed(values):
    mean = jnp.mean(values, -1, keepdims=True)
    centred = values - mean
    var = jnp.mean(centred * centred, -1, keepdims=True)
    rstd = lax.rsqrt(var + EPS)
    return centred * rstd, rstd


def norm_backward(dnorm, unit, rstd, gain):
    grad_gain = jnp.sum(dnorm * unit, 0, keepdims=True)
    scaled = dnorm * gain
    first = jnp.mean(scaled, -1, keepdims=True)
    second = jnp.mean(scaled * unit, -1, keepdims=True)
    return rstd * (scaled - first - unit * second), grad_gain


def project_qkv(x32, gain, wq_ref, qkv_ref, sums_ref):
    unit, _ = normed(x32)
    n_one = (unit * gain).astype(BF16)
    spans = x32.shape[0] // SPAN
    for part in range(3):
        block = dot(n_one, wq_ref[:, part * D : (part + 1) * D]).astype(BF16)
        qkv_ref[0, :, part * D : (part + 1) * D] = block
        if part > 0:
            wide = block.astype(F32)
            for span in range(spans):
                mean = jnp.sum(wide[span * SPAN : (span + 1) * SPAN], 0, keepdims=True) * (1.0 / SPAN)
                sums_ref[0, span : span + 1, (part - 1) * D : part * D] = mean.astype(BF16)


def lane_halves():
    lane = lax.broadcasted_iota(jnp.int32, (1, 2 * HEAD), 1)
    low = lane < HEAD
    return low


def head_stack(block, low, factor):
    one = jnp.where(low, factor, 0.0).astype(BF16)
    two = jnp.where(low, 0.0, factor).astype(BF16)
    return jnp.concatenate([block * one, block * two], 0)


def pair_operands(qkv_ref, sums_ref, span, pair):
    rows = slice(span * SPAN, (span + 1) * SPAN)
    lanes = slice(pair * 128, (pair + 1) * 128)
    keys = jnp.concatenate(
        [qkv_ref[0, rows, D + pair * 128 : D + (pair + 1) * 128], sums_ref[0, :, lanes]], 0
    )
    values = jnp.concatenate(
        [
            qkv_ref[0, rows, 2 * D + pair * 128 : 2 * D + (pair + 1) * 128],
            sums_ref[0, :, D + pair * 128 : D + (pair + 1) * 128],
        ],
        0,
    )
    query = qkv_ref[0, rows, lanes]
    return query, keys, values


def attention_forward(qkv_ref, sums_ref, bias_ref, prob_ref, o_ref):
    low = lane_halves()
    spans = qkv_ref.shape[1] // SPAN
    for span in range(spans):
        bias = bias_ref[0, span]
        bias = jnp.concatenate([bias, bias], 1)
        for pair in range(PAIRS):
            query, keys, values = pair_operands(qkv_ref, sums_ref, span, pair)
            scores = dot(keys, head_stack(query, low, SCALE), NT) + bias
            top = jnp.max(scores, 0, keepdims=True)
            exps = jnp.exp(scores - top)
            total = jnp.sum(exps, 0, keepdims=True)
            prob = (exps * (1.0 / total)).astype(BF16)
            prob_ref[0, span, pair] = prob
            both = dot(prob, values, TN)
            o_ref[0, span * SPAN : (span + 1) * SPAN, pair * 128 : (pair + 1) * 128] = jnp.where(
                low, both[:SPAN], both[SPAN:]
            ).astype(BF16)


def attention_backward(qkv_ref, sums_ref, prob_ref, dout, dqkv_ref, dsums_ref):
    low = lane_halves()
    spans = qkv_ref.shape[1] // SPAN
    for pair in range(PAIRS):
        lanes = slice(pair * 128, (pair + 1) * 128)
        klanes = slice(D + pair * 128, D + (pair + 1) * 128)
        vlanes = slice(2 * D + pair * 128, 2 * D + (pair + 1) * 128)
        dksum = dvsum = 0.0
        for span in range(spans):
            rows = slice(span * SPAN, (span + 1) * SPAN)
            query, keys, values = pair_operands(qkv_ref, sums_ref, span, pair)
            q_stack = head_stack(query, low, SCALE)
            do_stack = head_stack(dout[rows, lanes], low, 1.0)
            prob = prob_ref[0, span, pair]
            wide = prob.astype(F32)
            dprob = dot(values, do_stack, NT)
            rowdot = jnp.sum(wide * dprob, 0, keepdims=True)
            dscore = (wide * (dprob - rowdot)).astype(BF16)
            dboth = dot(dscore, keys, TN)
            dquery = jnp.where(low, dboth[:SPAN], dboth[SPAN:]) * SCALE
            dkeys = dot(dscore, q_stack)
            dvalues = dot(prob, do_stack)
            dqkv_ref[0, rows, lanes] = dquery.astype(BF16)
            dqkv_ref[0, rows, klanes] = dkeys[:SPAN].astype(BF16)
            dqkv_ref[0, rows, vlanes] = dvalues[:SPAN].astype(BF16)
            dksum = dksum + dkeys[SPAN:]
            dvsum = dvsum + dvalues[SPAN:]
        dsums_ref[0, :, pair * 128 : (pair + 1) * 128] = dksum.astype(BF16)
        dsums_ref[0, :, D + pair * 128 : D + (pair + 1) * 128] = dvsum.astype(BF16)


G0 = 0.7978845608
G1 = 0.7978845608 * 0.044715


def gelu(values):
    squared = values * values
    slope = jnp.tanh(values * (G0 + G1 * squared))
    half = 0.5 * values
    return half + half * slope


def gelu_both(values):
    squared = values * values
    slope = jnp.tanh(values * (G0 + G1 * squared))
    half = 0.5 * values
    rise = 0.5 + 0.5 * slope
    inner = G0 + (3.0 * G1) * squared
    return values * rise, rise + half * (1.0 - slope * slope) * inner


def mlp_forward(h32, gain, wu_ref, wd_ref, u_ref):
    unit, _ = normed(h32)
    n_two = (unit * gain).astype(BF16)
    total = h32
    for start in range(0, wu_ref.shape[1], CHUNK):
        upper = dot(n_two, wu_ref[:, start : start + CHUNK])
        u_ref[0, :, start : start + CHUNK] = upper.astype(BF16)
        total = total + dot(gelu(upper).astype(BF16), wd_ref[start : start + CHUNK, :])
    return total


def first_kernel(x_ref, gain_ref, wq_ref, qkv_ref, sums_ref):
    project_qkv(x_ref[0].astype(F32), gain_ref[...], wq_ref, qkv_ref, sums_ref)


def layer_kernel(last, *refs):
    if last:
        (x_ref, qkv_ref, sums_ref, bias_ref, gain_ref, wo_ref, wu_ref, wd_ref,
         prob_ref, o_ref, h_ref, u_ref, next_ref) = refs
    else:
        (x_ref, qkv_ref, sums_ref, bias_ref, gain_ref, wo_ref, wu_ref, wd_ref, gain_next_ref, wq_ref,
         prob_ref, o_ref, h_ref, u_ref, next_ref, qkv_next_ref, sums_next_ref) = refs
    attention_forward(qkv_ref, sums_ref, bias_ref, prob_ref, o_ref)
    hidden = x_ref[0].astype(F32) + dot(o_ref[0], wo_ref[...])
    h_ref[0] = hidden
    result = mlp_forward(hidden, gain_ref[...], wu_ref, wd_ref, u_ref)
    next_ref[0] = result.astype(next_ref.dtype)
    if not last:
        project_qkv(result, gain_next_ref[...], wq_ref, qkv_next_ref, sums_next_ref)


def accumulate(ref, index, value, first):
    @pl.when(first)
    def _():
        ref[index] = value

    @pl.when(jnp.logical_not(first))
    def _():
        ref[index] = ref[index] + value


def mlp_attention_backward(dy32, u_ref, h_ref, o_ref, prob_ref, qkv_ref, sums_ref, gain_ref,
                           wo_ref, wu_ref, wd_ref, dh_ref, dqkv_ref, dsums_ref, gd_ref, gu_ref,
                           go_ref, gg_ref):
    ddown = dy32.astype(BF16)
    unit, rstd = normed(h_ref[0])
    n_two = (unit * gain_ref[...]).astype(BF16)
    dn_two = 0.0
    for start in range(0, wu_ref.shape[1], CHUNK):
        cols = slice(start, start + CHUNK)
        dactive = dot(ddown, wd_ref[cols, :], NT)
        active, slope = gelu_both(u_ref[0, :, cols].astype(F32))
        gd_ref[cols, :] += dot(active.astype(BF16), ddown, TN)
        dupper = (dactive * slope).astype(BF16)
        gu_ref[:, cols] += dot(n_two, dupper, TN)
        dn_two = dn_two + dot(dupper, wu_ref[:, cols], NT)
    dnorm, grad_gain = norm_backward(dn_two, unit, rstd, gain_ref[...])
    gg_ref[...] += grad_gain
    dhidden = dy32 + dnorm
    dh_ref[0] = dhidden
    dattn = dhidden.astype(BF16)
    go_ref[...] += dot(o_ref[0], dattn, TN)
    dout = dot(dattn, wo_ref[...], NT).astype(BF16)
    attention_backward(qkv_ref, sums_ref, prob_ref, dout, dqkv_ref, dsums_ref)


def back_kernel(dy_ref, u_ref, h_ref, o_ref, prob_ref, qkv_ref, sums_ref, gain_ref,
                wo_ref, wu_ref, wd_ref, dh_ref, dqkv_ref, dsums_ref, gd_out, gu_out, go_out,
                gg_ref, gd_ref, gu_ref, go_ref):
    step = pl.program_id(0)

    @pl.when(step == 0)
    def _():
        gd_ref[...] = jnp.zeros_like(gd_ref)
        gu_ref[...] = jnp.zeros_like(gu_ref)
        go_ref[...] = jnp.zeros_like(go_ref)
        gg_ref[...] = jnp.zeros_like(gg_ref)

    mlp_attention_backward(dy_ref[0].astype(F32), u_ref, h_ref, o_ref, prob_ref, qkv_ref, sums_ref,
                           gain_ref, wo_ref, wu_ref, wd_ref, dh_ref, dqkv_ref, dsums_ref, gd_ref,
                           gu_ref, go_ref, gg_ref)

    @pl.when(step == pl.num_programs(0) - 1)
    def _():
        gd_out[...] = gd_ref[...].astype(BF16)
        gu_out[...] = gu_ref[...].astype(BF16)
        go_out[...] = go_ref[...].astype(BF16)


def qkv_backward(x32, gain, near_ref, dsums_ref, dh, wq_ref, gq_ref, gg_ref):
    unit, rstd = normed(x32)
    n_one = (unit * gain).astype(BF16)
    dn_one = 0.0
    tokens = x32.shape[0]
    for part in range(3):
        cols = slice(part * D, (part + 1) * D)
        block = near_ref[0, :, cols]
        if part > 0:
            pieces = []
            for span in range(tokens // SPAN):
                share = dsums_ref[0, span : span + 1, (part - 1) * D : part * D].astype(F32) * (1.0 / SPAN)
                pieces.append(block[span * SPAN : (span + 1) * SPAN].astype(F32) + share)
            block = jnp.concatenate(pieces, 0).astype(BF16)
        gq_ref[:, cols] += dot(n_one, block, TN)
        dn_one = dn_one + dot(block, wq_ref[:, cols], NT)
    dnorm, grad_gain = norm_backward(dn_one, unit, rstd, gain)
    gg_ref[...] += grad_gain
    return dh + dnorm


def last_kernel(x_ref, gain_ref, near_ref, dsums_ref, dh_ref, wq_ref, dx_ref, gq_out, gg_ref, gq_ref):
    step = pl.program_id(0)

    @pl.when(step == 0)
    def _():
        gq_ref[...] = jnp.zeros_like(gq_ref)
        gg_ref[...] = jnp.zeros_like(gg_ref)

    dx_ref[0] = qkv_backward(x_ref[0].astype(F32), gain_ref[...], near_ref, dsums_ref, dh_ref[0], wq_ref,
                             gq_ref, gg_ref)

    @pl.when(step == pl.num_programs(0) - 1)
    def _():
        gq_out[...] = gq_ref[...].astype(BF16)


def per_seq(shape):
    rest = len(shape) - 1
    return pl.BlockSpec((1,) + tuple(shape[1:]), lambda b: (b,) + (0,) * rest)


def whole(shape):
    rank = len(shape)
    return pl.BlockSpec(tuple(shape), lambda b: (0,) * rank, pipeline_mode=pl.Buffered(1))


def sds(shape, dtype):
    return jax.ShapeDtypeStruct(tuple(shape), dtype)


def params():
    return pltpu.CompilerParams(dimension_semantics=("arbitrary",), vmem_limit_bytes=VMEM_LIMIT)


def call_first(x, gain, wq):
    batch, tokens, _ = x.shape
    spans = tokens // SPAN
    outs = (sds((batch, tokens, 3 * D), BF16), sds((batch, spans, 2 * D), BF16))
    return pl.pallas_call(
        first_kernel,
        grid=(batch,),
        in_specs=[per_seq(x.shape), whole(gain.shape), whole(wq.shape)],
        out_specs=[per_seq(o.shape) for o in outs],
        out_shape=outs,
        compiler_params=params(),
        name="first",
    )(x, gain, wq)


def call_layer(x, qkv, sums, bias, gain, wo, wu, wd, gain_next=None, wq=None):
    batch, tokens, _ = x.shape
    spans = tokens // SPAN
    last = wq is None
    keys = SPAN + sums.shape[1]
    outs = [
        sds((batch, spans, PAIRS, keys, 2 * SPAN), BF16),
        sds((batch, tokens, D), BF16),
        sds((batch, tokens, D), F32),
        sds((batch, tokens, wu.shape[1]), BF16),
        sds((batch, tokens, D), BF16 if last else F32),
    ]
    args = [x, qkv, sums, bias, gain, wo, wu, wd]
    if not last:
        outs += [sds((batch, tokens, 3 * D), BF16), sds((batch, spans, 2 * D), BF16)]
        args += [gain_next, wq]
    specs = [per_seq(a.shape) for a in args[:4]] + [whole(a.shape) for a in args[4:]]
    return pl.pallas_call(
        functools.partial(layer_kernel, last),
        grid=(batch,),
        in_specs=specs,
        out_specs=[per_seq(o.shape) for o in outs],
        out_shape=outs,
        compiler_params=params(),
        name="layer",
    )(*args)


def call_back(dy, u, h, o, prob, qkv, sums, gain, wo, wu, wd):
    batch, tokens, _ = dy.shape
    args = [dy, u, h, o, prob, qkv, sums, gain, wo, wu, wd]
    specs = [per_seq(a.shape) for a in args[:7]] + [whole(a.shape) for a in args[7:]]
    outs = [sds(h.shape, F32), sds(qkv.shape, BF16), sds(sums.shape, BF16),
            sds(wd.shape, BF16), sds(wu.shape, BF16), sds(wo.shape, BF16), sds((1, D), F32)]
    return pl.pallas_call(
        back_kernel,
        grid=(batch,),
        in_specs=specs,
        out_specs=[per_seq(o.shape) for o in outs[:3]] + [whole(o.shape) for o in outs[3:]],
        out_shape=outs,
        scratch_shapes=[pltpu.VMEM(wd.shape, F32), pltpu.VMEM(wu.shape, F32), pltpu.VMEM(wo.shape, F32)],
        compiler_params=params(),
        name="back",
    )(*args)


def call_last(x, gain, near, dsums, dh, wq):
    batch, tokens, _ = x.shape
    outs = [sds((batch, tokens, D), F32), sds(wq.shape, BF16), sds((1, D), F32)]
    return pl.pallas_call(
        last_kernel,
        grid=(batch,),
        in_specs=[per_seq(x.shape), whole(gain.shape), per_seq(near.shape), per_seq(dsums.shape),
                  per_seq(dh.shape), whole(wq.shape)],
        out_specs=[per_seq(outs[0].shape), whole(outs[1].shape), whole(outs[2].shape)],
        out_shape=outs,
        scratch_shapes=[pltpu.VMEM(wq.shape, F32)],
        compiler_params=params(),
        name="last",
    )(x, gain, near, dsums, dh, wq)


def mask_bias(segments, stretch):
    batch, length = segments.shape
    rank = lax.axis_index("seq")
    own = lax.dynamic_slice_in_dim(segments, rank * stretch, stretch, 1).reshape(batch, -1, SPAN)
    ends = segments.reshape(batch, -1, SPAN)[:, :, SPAN - 1]
    spans = own.shape[1]
    pos = jnp.arange(SPAN)
    near = (own[:, :, :, None] == own[:, :, None, :]) & (pos[:, None] <= pos[None, :])
    ids = rank * spans + jnp.arange(spans)
    before = jnp.arange(ends.shape[1])[None, :] < ids[:, None]
    far = (ends[:, None, :, None] == own[:, :, None, :]) & before[None, :, :, None]
    return jnp.where(jnp.concatenate([near, far], 2), 0.0, NEG).astype(F32)


def gather(shard):
    return lax.all_gather(shard, ("dp", "seq"), axis=0, tiled=True)


def scatter(grad):
    return lax.psum_scatter(grad, ("dp", "seq"), scatter_dimension=0, tiled=True)


def on_device(inputs, segments, w_qkv, w_out, w_up, w_down, gain_attn, gain_mlp, cotangent):
    layers = w_qkv.shape[0]
    stretch = inputs.shape[1]
    gains = lax.all_gather(
        jnp.concatenate([gain_attn, gain_mlp], 0), ("dp", "seq"), axis=1, tiled=True
    ).astype(F32)
    g_one = [gains[l : l + 1] for l in range(layers)]
    g_two = [gains[layers + l : layers + l + 1] for l in range(layers)]
    wq = [gather(w_qkv[l]) for l in range(layers)]
    wo = [gather(w_out[l]) for l in range(layers)]
    wu = [gather(w_up[l]) for l in range(layers)]
    wd = [gather(w_down[l]) for l in range(layers)]
    bias = mask_bias(segments, stretch)

    def spread(sums):
        return lax.all_gather(sums, "seq", axis=1, tiled=True)

    def collect(dsums):
        return lax.psum_scatter(dsums, "seq", scatter_dimension=1, tiled=True)

    x = inputs
    qkv, own = call_first(x, g_one[0], wq[0])
    kept = []
    for l in range(layers):
        sums = spread(own)
        if l + 1 < layers:
            prob, o, h, u, x_next, qkv_next, own = call_layer(
                x, qkv, sums, bias, g_two[l], wo[l], wu[l], wd[l], g_one[l + 1], wq[l + 1]
            )
        else:
            prob, o, h, u, x_next = call_layer(x, qkv, sums, bias, g_two[l], wo[l], wu[l], wd[l])
            qkv_next = None
        kept.append((x, qkv, sums, prob, o, h, u))
        x, qkv = x_next, qkv_next
    outputs = x
    dy = cotangent
    shares = [None] * layers
    for l in reversed(range(layers)):
        x, qkv, sums, prob, o, h, u = kept[l]
        dh, near, dsums, gd, gu, go, gg_two = call_back(
            dy, u, h, o, prob, qkv, sums, g_two[l], wo[l], wu[l], wd[l]
        )
        dy, gq, gg_one = call_last(x, g_one[l], near, collect(dsums), dh, wq[l])
        shares[l] = (scatter(gq), scatter(go), scatter(gu), scatter(gd), gg_one, gg_two)
    gain_grads = jnp.concatenate(
        [shares[l][4] for l in range(layers)] + [shares[l][5] for l in range(layers)], 0
    )
    gain_grads = lax.psum_scatter(gain_grads, ("dp", "seq"), scatter_dimension=1, tiled=True)
    stacked = [jnp.stack([shares[l][m] for l in range(layers)]).astype(F32) for m in range(4)]
    return (outputs, dy, *stacked, gain_grads[:layers], gain_grads[layers:])


def solution(mesh):
    weights = P(None, ("dp", "seq"), None)
    gains = P(None, ("dp", "seq"))
    rows = P("dp", "seq", None)
    return jax.shard_map(
        on_device,
        mesh=mesh,
        in_specs=(rows, P("dp", None), weights, weights, weights, weights, gains, gains, rows),
        out_specs=(rows, rows, weights, weights, weights, weights, gains, gains),
        check_vma=False,
    )
```

```python
import functools

import jax
import jax.numpy as jnp
from jax import lax
from jax.experimental import pallas as pl
from jax.experimental.pallas import tpu as pltpu
from jax.sharding import PartitionSpec as P

D = 512
HEADS = 8
HEAD = 64
SPAN = 128
PAIRS = HEADS // 2
EPS = 1e-05
NEG = -1000000000.0
SCALE = HEAD ** (-0.5)
F32 = jnp.float32
BF16 = jnp.bfloat16
CHUNK = 512
VMEM_LIMIT = 60 * 1024 * 1024

NN = (((1,), (0,)), ((), ()))
NT = (((1,), (1,)), ((), ()))
TN = (((0,), (0,)), ((), ()))


def dot(left, right, dims=NN):
    return lax.dot_general(left, right, dims, preferred_element_type=F32)


def normed(values):
    mean = jnp.mean(values, -1, keepdims=True)
    centred = values - mean
    var = jnp.mean(centred * centred, -1, keepdims=True)
    rstd = lax.rsqrt(var + EPS)
    return centred * rstd, rstd


def norm_backward(dnorm, unit, rstd, gain):
    grad_gain = jnp.sum(dnorm * unit, 0, keepdims=True)
    scaled = dnorm * gain
    first = jnp.mean(scaled, -1, keepdims=True)
    second = jnp.mean(scaled * unit, -1, keepdims=True)
    return rstd * (scaled - first - unit * second), grad_gain


def project_qkv(x32, gain, wq_ref, qkv_ref, sums_ref):
    unit, _ = normed(x32)
    n_one = (unit * gain).astype(BF16)
    spans = x32.shape[0] // SPAN
    for part in range(3):
        block = dot(n_one, wq_ref[:, part * D : (part + 1) * D]).astype(BF16)
        qkv_ref[0, :, part * D : (part + 1) * D] = block
        if part > 0:
            wide = block.astype(F32)
            for span in range(spans):
                mean = jnp.sum(wide[span * SPAN : (span + 1) * SPAN], 0, keepdims=True) * (1.0 / SPAN)
                sums_ref[0, span : span + 1, (part - 1) * D : part * D] = mean.astype(BF16)


def lane_halves():
    lane = lax.broadcasted_iota(jnp.int32, (1, 2 * HEAD), 1)
    low = lane < HEAD
    return low


def head_stack(block, low, factor):
    one = jnp.where(low, factor, 0.0).astype(BF16)
    two = jnp.where(low, 0.0, factor).astype(BF16)
    return jnp.concatenate([block * one, block * two], 0)


def pair_operands(qkv_ref, sums_ref, span, pair):
    rows = slice(span * SPAN, (span + 1) * SPAN)
    lanes = slice(pair * 128, (pair + 1) * 128)
    keys = jnp.concatenate(
        [qkv_ref[0, rows, D + pair * 128 : D + (pair + 1) * 128], sums_ref[0, :, lanes]], 0
    )
    values = jnp.concatenate(
        [
            qkv_ref[0, rows, 2 * D + pair * 128 : 2 * D + (pair + 1) * 128],
            sums_ref[0, :, D + pair * 128 : D + (pair + 1) * 128],
        ],
        0,
    )
    query = qkv_ref[0, rows, lanes]
    return query, keys, values


def attention_forward(qkv_ref, sums_ref, bias_ref, prob_ref, o_ref):
    low = lane_halves()
    spans = qkv_ref.shape[1] // SPAN
    for span in range(spans):
        bias = bias_ref[0, span]
        bias = jnp.concatenate([bias, bias], 1)
        for pair in range(PAIRS):
            query, keys, values = pair_operands(qkv_ref, sums_ref, span, pair)
            scores = dot(keys, head_stack(query, low, SCALE), NT) + bias
            top = jnp.max(scores, 0, keepdims=True)
            exps = jnp.exp(scores - top)
            total = jnp.sum(exps, 0, keepdims=True)
            prob = (exps * (1.0 / total)).astype(BF16)
            prob_ref[0, span, pair] = prob
            both = dot(prob, values, TN)
            o_ref[0, span * SPAN : (span + 1) * SPAN, pair * 128 : (pair + 1) * 128] = jnp.where(
                low, both[:SPAN], both[SPAN:]
            ).astype(BF16)


def attention_backward(qkv_ref, sums_ref, prob_ref, dout, dqkv_ref, dsums_ref):
    low = lane_halves()
    spans = qkv_ref.shape[1] // SPAN
    for pair in range(PAIRS):
        lanes = slice(pair * 128, (pair + 1) * 128)
        klanes = slice(D + pair * 128, D + (pair + 1) * 128)
        vlanes = slice(2 * D + pair * 128, 2 * D + (pair + 1) * 128)
        dksum = dvsum = 0.0
        for span in range(spans):
            rows = slice(span * SPAN, (span + 1) * SPAN)
            query, keys, values = pair_operands(qkv_ref, sums_ref, span, pair)
            q_stack = head_stack(query, low, SCALE)
            do_stack = head_stack(dout[rows, lanes], low, 1.0)
            prob = prob_ref[0, span, pair]
            wide = prob.astype(F32)
            dprob = dot(values, do_stack, NT)
            rowdot = jnp.sum(wide * dprob, 0, keepdims=True)
            dscore = (wide * (dprob - rowdot)).astype(BF16)
            dboth = dot(dscore, keys, TN)
            dquery = jnp.where(low, dboth[:SPAN], dboth[SPAN:]) * SCALE
            dkeys = dot(dscore, q_stack)
            dvalues = dot(prob, do_stack)
            dqkv_ref[0, rows, lanes] = dquery.astype(BF16)
            dqkv_ref[0, rows, klanes] = dkeys[:SPAN].astype(BF16)
            dqkv_ref[0, rows, vlanes] = dvalues[:SPAN].astype(BF16)
            dksum = dksum + dkeys[SPAN:]
            dvsum = dvsum + dvalues[SPAN:]
        dsums_ref[0, :, pair * 128 : (pair + 1) * 128] = dksum.astype(BF16)
        dsums_ref[0, :, D + pair * 128 : D + (pair + 1) * 128] = dvsum.astype(BF16)


G0 = 0.7978845608
G1 = 0.7978845608 * 0.044715


def gelu(values):
    squared = values * values
    slope = jnp.tanh(values * (G0 + G1 * squared))
    half = 0.5 * values
    return half + half * slope


def gelu_both(values):
    squared = values * values
    slope = jnp.tanh(values * (G0 + G1 * squared))
    half = 0.5 * values
    rise = 0.5 + 0.5 * slope
    inner = G0 + (3.0 * G1) * squared
    return values * rise, rise + half * (1.0 - slope * slope) * inner


def mlp_forward(h32, gain, wu_ref, wd_ref, u_ref):
    unit, _ = normed(h32)
    n_two = (unit * gain).astype(BF16)
    total = h32
    for start in range(0, wu_ref.shape[1], CHUNK):
        upper = dot(n_two, wu_ref[:, start : start + CHUNK])
        u_ref[0, :, start : start + CHUNK] = upper.astype(BF16)
        total = total + dot(gelu(upper).astype(BF16), wd_ref[start : start + CHUNK, :])
    return total


def first_kernel(x_ref, gain_ref, wq_ref, qkv_ref, sums_ref):
    project_qkv(x_ref[0].astype(F32), gain_ref[...], wq_ref, qkv_ref, sums_ref)


def layer_kernel(last, *refs):
    if last:
        (x_ref, qkv_ref, sums_ref, bias_ref, gain_ref, wo_ref, wu_ref, wd_ref,
         prob_ref, o_ref, h_ref, u_ref, next_ref) = refs
    else:
        (x_ref, qkv_ref, sums_ref, bias_ref, gain_ref, wo_ref, wu_ref, wd_ref, gain_next_ref, wq_ref,
         prob_ref, o_ref, h_ref, u_ref, next_ref, qkv_next_ref, sums_next_ref) = refs
    attention_forward(qkv_ref, sums_ref, bias_ref, prob_ref, o_ref)
    hidden = x_ref[0].astype(F32) + dot(o_ref[0], wo_ref[...])
    h_ref[0] = hidden
    result = mlp_forward(hidden, gain_ref[...], wu_ref, wd_ref, u_ref)
    next_ref[0] = result.astype(next_ref.dtype)
    if not last:
        project_qkv(result, gain_next_ref[...], wq_ref, qkv_next_ref, sums_next_ref)


def accumulate(ref, index, value, first):
    @pl.when(first)
    def _():
        ref[index] = value

    @pl.when(jnp.logical_not(first))
    def _():
        ref[index] = ref[index] + value


def mlp_attention_backward(dy32, u_ref, h_ref, o_ref, prob_ref, qkv_ref, sums_ref, gain_ref,
                           wo_ref, wu_ref, wd_ref, dh_ref, dqkv_ref, dsums_ref, gd_ref, gu_ref,
                           go_ref, gg_ref):
    ddown = dy32.astype(BF16)
    unit, rstd = normed(h_ref[0])
    n_two = (unit * gain_ref[...]).astype(BF16)
    dn_two = 0.0
    for start in range(0, wu_ref.shape[1], CHUNK):
        cols = slice(start, start + CHUNK)
        dactive = dot(ddown, wd_ref[cols, :], NT)
        active, slope = gelu_both(u_ref[0, :, cols].astype(F32))
        gd_ref[cols, :] += dot(active.astype(BF16), ddown, TN)
        dupper = (dactive * slope).astype(BF16)
        gu_ref[:, cols] += dot(n_two, dupper, TN)
        dn_two = dn_two + dot(dupper, wu_ref[:, cols], NT)
    dnorm, grad_gain = norm_backward(dn_two, unit, rstd, gain_ref[...])
    gg_ref[...] += grad_gain
    dhidden = dy32 + dnorm
    dh_ref[0] = dhidden
    dattn = dhidden.astype(BF16)
    go_ref[...] += dot(o_ref[0], dattn, TN)
    dout = dot(dattn, wo_ref[...], NT).astype(BF16)
    attention_backward(qkv_ref, sums_ref, prob_ref, dout, dqkv_ref, dsums_ref)


def back_kernel(dy_ref, u_ref, h_ref, o_ref, prob_ref, qkv_ref, sums_ref, gain_ref,
                wo_ref, wu_ref, wd_ref, dh_ref, dqkv_ref, dsums_ref, gd_out, gu_out, go_out,
                gg_ref, gd_ref, gu_ref, go_ref):
    step = pl.program_id(0)

    @pl.when(step == 0)
    def _():
        gd_ref[...] = jnp.zeros_like(gd_ref)
        gu_ref[...] = jnp.zeros_like(gu_ref)
        go_ref[...] = jnp.zeros_like(go_ref)
        gg_ref[...] = jnp.zeros_like(gg_ref)

    mlp_attention_backward(dy_ref[0].astype(F32), u_ref, h_ref, o_ref, prob_ref, qkv_ref, sums_ref,
                           gain_ref, wo_ref, wu_ref, wd_ref, dh_ref, dqkv_ref, dsums_ref, gd_ref,
                           gu_ref, go_ref, gg_ref)

    @pl.when(step == pl.num_programs(0) - 1)
    def _():
        gd_out[...] = gd_ref[...].astype(BF16)
        gu_out[...] = gu_ref[...].astype(BF16)
        go_out[...] = go_ref[...].astype(BF16)


def qkv_backward(x32, gain, near_ref, dsums_ref, dh, wq_ref, gq_ref, gg_ref):
    unit, rstd = normed(x32)
    n_one = (unit * gain).astype(BF16)
    dn_one = 0.0
    tokens = x32.shape[0]
    for part in range(3):
        cols = slice(part * D, (part + 1) * D)
        block = near_ref[0, :, cols]
        if part > 0:
            pieces = []
            for span in range(tokens // SPAN):
                share = dsums_ref[0, span : span + 1, (part - 1) * D : part * D].astype(F32) * (1.0 / SPAN)
                pieces.append(block[span * SPAN : (span + 1) * SPAN].astype(F32) + share)
            block = jnp.concatenate(pieces, 0).astype(BF16)
        gq_ref[:, cols] += dot(n_one, block, TN)
        dn_one = dn_one + dot(block, wq_ref[:, cols], NT)
    dnorm, grad_gain = norm_backward(dn_one, unit, rstd, gain)
    gg_ref[...] += grad_gain
    return dh + dnorm


def last_kernel(x_ref, gain_ref, near_ref, dsums_ref, dh_ref, wq_ref, dx_ref, gq_out, gg_ref, gq_ref):
    step = pl.program_id(0)

    @pl.when(step == 0)
    def _():
        gq_ref[...] = jnp.zeros_like(gq_ref)
        gg_ref[...] = jnp.zeros_like(gg_ref)

    dx_ref[0] = qkv_backward(x_ref[0].astype(F32), gain_ref[...], near_ref, dsums_ref, dh_ref[0], wq_ref,
                             gq_ref, gg_ref)

    @pl.when(step == pl.num_programs(0) - 1)
    def _():
        gq_out[...] = gq_ref[...].astype(BF16)


def per_seq(shape):
    rest = len(shape) - 1
    return pl.BlockSpec((1,) + tuple(shape[1:]), lambda b: (b,) + (0,) * rest)


def whole(shape):
    rank = len(shape)
    return pl.BlockSpec(tuple(shape), lambda b: (0,) * rank, pipeline_mode=pl.Buffered(1))


def sds(shape, dtype):
    return jax.ShapeDtypeStruct(tuple(shape), dtype)


def params():
    return pltpu.CompilerParams(dimension_semantics=("arbitrary",), vmem_limit_bytes=VMEM_LIMIT)


def call_first(x, gain, wq):
    batch, tokens, _ = x.shape
    spans = tokens // SPAN
    outs = (sds((batch, tokens, 3 * D), BF16), sds((batch, spans, 2 * D), BF16))
    return pl.pallas_call(
        first_kernel,
        grid=(batch,),
        in_specs=[per_seq(x.shape), whole(gain.shape), whole(wq.shape)],
        out_specs=[per_seq(o.shape) for o in outs],
        out_shape=outs,
        compiler_params=params(),
        name="first",
    )(x, gain, wq)


def call_layer(x, qkv, sums, bias, gain, wo, wu, wd, gain_next=None, wq=None):
    batch, tokens, _ = x.shape
    spans = tokens // SPAN
    last = wq is None
    keys = SPAN + sums.shape[1]
    outs = [
        sds((batch, spans, PAIRS, keys, 2 * SPAN), BF16),
        sds((batch, tokens, D), BF16),
        sds((batch, tokens, D), F32),
        sds((batch, tokens, wu.shape[1]), BF16),
        sds((batch, tokens, D), BF16 if last else F32),
    ]
    args = [x, qkv, sums, bias, gain, wo, wu, wd]
    if not last:
        outs += [sds((batch, tokens, 3 * D), BF16), sds((batch, spans, 2 * D), BF16)]
        args += [gain_next, wq]
    specs = [per_seq(a.shape) for a in args[:4]] + [whole(a.shape) for a in args[4:]]
    return pl.pallas_call(
        functools.partial(layer_kernel, last),
        grid=(batch,),
        in_specs=specs,
        out_specs=[per_seq(o.shape) for o in outs],
        out_shape=outs,
        compiler_params=params(),
        name="layer",
    )(*args)


def call_back(dy, u, h, o, prob, qkv, sums, gain, wo, wu, wd):
    batch, tokens, _ = dy.shape
    args = [dy, u, h, o, prob, qkv, sums, gain, wo, wu, wd]
    specs = [per_seq(a.shape) for a in args[:7]] + [whole(a.shape) for a in args[7:]]
    outs = [sds(h.shape, F32), sds(qkv.shape, BF16), sds(sums.shape, BF16),
            sds(wd.shape, BF16), sds(wu.shape, BF16), sds(wo.shape, BF16), sds((1, D), F32)]
    return pl.pallas_call(
        back_kernel,
        grid=(batch,),
        in_specs=specs,
        out_specs=[per_seq(o.shape) for o in outs[:3]] + [whole(o.shape) for o in outs[3:]],
        out_shape=outs,
        scratch_shapes=[pltpu.VMEM(wd.shape, F32), pltpu.VMEM(wu.shape, F32), pltpu.VMEM(wo.shape, F32)],
        compiler_params=params(),
        name="back",
    )(*args)


def call_last(x, gain, near, dsums, dh, wq):
    batch, tokens, _ = x.shape
    outs = [sds((batch, tokens, D), F32), sds(wq.shape, BF16), sds((1, D), F32)]
    return pl.pallas_call(
        last_kernel,
        grid=(batch,),
        in_specs=[per_seq(x.shape), whole(gain.shape), per_seq(near.shape), per_seq(dsums.shape),
                  per_seq(dh.shape), whole(wq.shape)],
        out_specs=[per_seq(outs[0].shape), whole(outs[1].shape), whole(outs[2].shape)],
        out_shape=outs,
        scratch_shapes=[pltpu.VMEM(wq.shape, F32)],
        compiler_params=params(),
        name="last",
    )(x, gain, near, dsums, dh, wq)


def mask_bias(segments, stretch):
    batch, length = segments.shape
    rank = lax.axis_index("seq")
    own = lax.dynamic_slice_in_dim(segments, rank * stretch, stretch, 1).reshape(batch, -1, SPAN)
    ends = segments.reshape(batch, -1, SPAN)[:, :, SPAN - 1]
    spans = own.shape[1]
    pos = jnp.arange(SPAN)
    near = (own[:, :, :, None] == own[:, :, None, :]) & (pos[:, None] <= pos[None, :])
    ids = rank * spans + jnp.arange(spans)
    before = jnp.arange(ends.shape[1])[None, :] < ids[:, None]
    far = (ends[:, None, :, None] == own[:, :, None, :]) & before[None, :, :, None]
    return jnp.where(jnp.concatenate([near, far], 2), 0.0, NEG).astype(F32)

MESH = pl.DeviceIdType.MESH
CORES = 2


def place():
    nz, nseq = lax.axis_size("dp"), lax.axis_size("seq")
    z, s = lax.axis_index("dp"), lax.axis_index("seq")
    return nz, nseq // CORES, z, s // CORES, lax.rem(s, CORES)


def modulo(value, size):
    return lax.rem(value + size, size)


def peers_of():
    nz, nchip, z, chip, core = place()
    seq = chip * CORES + core
    out = [(modulo(z + d, nz), seq) for d in range(1, nz)]
    out += [(z, modulo(chip + d, nchip) * CORES + core) for d in range(1, nchip)]
    out.append((z, chip * CORES + 1 - core))
    return out


def greet(peers):
    barrier = pltpu.get_barrier_semaphore()
    for peer in peers:
        pl.semaphore_signal(barrier, inc=1, device_id=peer, device_id_type=MESH)
    pl.semaphore_wait(barrier, len(peers))


def remote(src, dst, send, recv, peer):
    return pltpu.make_async_remote_copy(
        src_ref=src, dst_ref=dst, send_sem=send, recv_sem=recv, device_id=peer, device_id_type=MESH
    )


class Gather:
    def __init__(self, shards, fulls, sems):
        self.shards, self.fulls = shards, fulls
        self.own, self.zs, self.zr, self.ps, self.pr, self.cs, self.cr = sems
        self.nz, self.nchip, self.z, self.chip, self.core = place()
        self.seq = self.chip * CORES + self.core

    @staticmethod
    def scratch(count):
        nz, nchip = lax.axis_size("dp"), lax.axis_size("seq") // CORES
        dma = pltpu.SemaphoreType.DMA
        return [dma((count,)), dma((count, nz - 1)), dma((count, nz - 1)), dma((count, nchip - 1)),
                dma((count, nchip - 1)), dma((count, nchip)), dma((count, nchip))]

    def local(self, t):
        return pltpu.make_async_copy(self.shards[t], self.fulls[t].at[self.z, self.seq], self.own.at[t])

    def line(self, t, d):
        peer = (modulo(self.z + d, self.nz), self.seq)
        return remote(self.shards[t], self.fulls[t].at[self.z, self.seq], self.zs.at[t, d - 1],
                      self.zr.at[t, d - 1], peer)

    def plane(self, t, d):
        block = self.fulls[t].at[:, self.seq]
        peer = (self.z, modulo(self.chip + d, self.nchip) * CORES + self.core)
        return remote(block, block, self.ps.at[t, d - 1], self.pr.at[t, d - 1], peer)

    def cross(self, t, d):
        block = self.fulls[t].at[:, modulo(self.chip - d, self.nchip) * CORES + self.core]
        peer = (self.z, self.chip * CORES + 1 - self.core)
        return remote(block, block, self.cs.at[t, d], self.cr.at[t, d], peer)

    def start(self, t):
        self.local(t).start()
        for d in range(1, self.nz):
            self.line(t, d).start()

    def spread(self, t):
        self.local(t).wait()
        for d in range(1, self.nz):
            self.line(t, d).wait_recv()
        for d in range(1, self.nchip):
            self.plane(t, d).start()
        self.cross(t, 0).start()

    def share(self, t):
        for d in range(1, self.nchip):
            self.plane(t, d).wait_recv()
            self.cross(t, d).start()

    def finish(self, t):
        for d in range(self.nchip):
            self.cross(t, d).wait_recv()

    def drain(self, t):
        for d in range(1, self.nz):
            self.line(t, d).wait_send()
        for d in range(1, self.nchip):
            self.plane(t, d).wait_send()
        for d in range(self.nchip):
            self.cross(t, d).wait_send()


def gather_kernel(count, *refs):
    work = Gather(refs[:count], refs[count : 2 * count], refs[2 * count :])
    greet(peers_of())
    for stage in (work.start, work.spread, work.share, work.finish, work.drain):
        for t in range(count):
            stage(t)


def call_gather(shards, collective_id):
    nz, nseq = lax.axis_size("dp"), lax.axis_size("seq")
    count = len(shards)
    outs = [sds((nz, nseq) + a.shape, a.dtype) for a in shards]
    return pl.pallas_call(
        functools.partial(gather_kernel, count),
        in_specs=[pl.BlockSpec(memory_space=pltpu.VMEM)] * count,
        out_specs=[pl.BlockSpec(memory_space=pl.ANY)] * count,
        out_shape=outs,
        scratch_shapes=Gather.scratch(count),
        compiler_params=pltpu.CompilerParams(
            collective_id=collective_id, has_side_effects=True, vmem_limit_bytes=VMEM_LIMIT
        ),
        name="gather",
    )(*shards)


class Reduce:
    def __init__(self, parts, outs, bufs, sems):
        self.parts, self.outs = parts, outs
        count = len(parts)
        self.mine, self.cross_in, self.plane_in, self.col, self.line_in = (
            bufs[i * count : (i + 1) * count] for i in range(5)
        )
        self.own, self.cs, self.cr, self.ps, self.pr, self.zs, self.zr = sems
        self.nz, self.nchip, self.z, self.chip, self.core = place()
        self.seq = self.chip * CORES + self.core

    @staticmethod
    def scratch(parts):
        nz, nchip = lax.axis_size("dp"), lax.axis_size("seq") // CORES
        dma = pltpu.SemaphoreType.DMA
        count = len(parts)
        bufs = []
        for lead in ((nchip, nz), (nchip, nz), (nchip - 1, nz), (nz,), (nz - 1,)):
            bufs += [pltpu.VMEM(lead + a.shape[3:], a.dtype) for a in parts]
        return bufs + [dma((count, nchip)), dma((count, nchip)), dma((count, nchip)), dma((count, nchip - 1)),
                       dma((count, nchip - 1)), dma((count, nz - 1)), dma((count, nz - 1))]

    def local(self, t, d):
        chip = modulo(self.chip + d, self.nchip)
        return pltpu.make_async_copy(self.parts[t].at[:, chip, self.core], self.mine[t].at[d], self.own.at[t, d])

    def cross(self, t, d):
        chip = modulo(self.chip + d, self.nchip)
        peer = (self.z, self.chip * CORES + 1 - self.core)
        return remote(self.parts[t].at[:, chip, 1 - self.core], self.cross_in[t].at[d], self.cs.at[t, d],
                      self.cr.at[t, d], peer)

    def plane(self, t, d):
        peer = (self.z, modulo(self.chip + d, self.nchip) * CORES + self.core)
        return remote(self.mine[t].at[d], self.plane_in[t].at[d - 1], self.ps.at[t, d - 1],
                      self.pr.at[t, d - 1], peer)

    def line(self, t, d):
        z = modulo(self.z + d, self.nz)
        return remote(self.col[t].at[z], self.line_in[t].at[d - 1], self.zs.at[t, d - 1],
                      self.zr.at[t, d - 1], (z, self.seq))

    def order(self):
        return list(range(1, self.nchip)) + [0]

    def start(self, t):
        for d in self.order():
            self.cross(t, d).start()
            self.local(t, d).start()

    def combine(self, t):
        for d in self.order():
            self.local(t, d).wait()
            self.cross(t, d).wait_recv()

            def add(i, carry):
                total = self.mine[t][d, i].astype(F32) + self.cross_in[t][d, i].astype(F32)
                self.mine[t][d, i] = total.astype(self.mine[t].dtype)
                return carry

            lax.fori_loop(0, self.nz, add, 0)
            if d > 0:
                self.plane(t, d).start()

    def column(self, t):
        for d in range(1, self.nchip):
            self.plane(t, d).wait_recv()

        def add(i, carry):
            total = self.mine[t][0, i].astype(F32)
            for d in range(self.nchip - 1):
                total = total + self.plane_in[t][d, i].astype(F32)
            self.col[t][i] = total.astype(self.col[t].dtype)
            return carry

        lax.fori_loop(0, self.nz, add, 0)
        for d in range(1, self.nz):
            self.line(t, d).start()

    def finish(self, t):
        total = self.col[t][self.z].astype(F32)
        for d in range(1, self.nz):
            self.line(t, d).wait_recv()
        for d in range(self.nz - 1):
            total = total + self.line_in[t][d].astype(F32)
        self.outs[t][...] = total

    def drain(self, t):
        for d in self.order():
            self.cross(t, d).wait_send()
        for d in range(1, self.nchip):
            self.plane(t, d).wait_send()
        for d in range(1, self.nz):
            self.line(t, d).wait_send()


def reduce_kernel(count, *refs):
    work = Reduce(refs[:count], refs[count : 2 * count], refs[2 * count : 7 * count], refs[7 * count :])
    greet(peers_of())
    for stage in (work.start, work.combine, work.column, work.finish, work.drain):
        for t in range(count):
            stage(t)


def call_reduce(parts, collective_id):
    nz, nseq = lax.axis_size("dp"), lax.axis_size("seq")
    count = len(parts)
    parts = [a.reshape((nz, nseq // CORES, CORES, a.shape[0] // (nz * nseq)) + a.shape[1:]) for a in parts]
    outs = [sds(a.shape[3:], F32) for a in parts]
    return pl.pallas_call(
        functools.partial(reduce_kernel, count),
        in_specs=[pl.BlockSpec(memory_space=pl.ANY)] * count,
        out_specs=[pl.BlockSpec(memory_space=pltpu.VMEM)] * count,
        out_shape=outs,
        scratch_shapes=Reduce.scratch(parts),
        compiler_params=pltpu.CompilerParams(
            collective_id=collective_id, has_side_effects=True, vmem_limit_bytes=VMEM_LIMIT
        ),
        name="reduce",
    )(*parts)


def seq_peers():
    nseq = lax.axis_size("seq")
    z, s = lax.axis_index("dp"), lax.axis_index("seq")
    return [(d, (z, modulo(s + d, nseq))) for d in range(1, nseq)]


def spread_kernel(own_ref, all_ref, send, recv):
    s = lax.axis_index("seq")
    peers = seq_peers()
    greet([peer for _, peer in peers])
    copies = [remote(own_ref, all_ref.at[s], send.at[d - 1], recv.at[d - 1], peer) for d, peer in peers]
    for copy in copies:
        copy.start()
    all_ref[s] = own_ref[...]
    for copy in copies:
        copy.wait()


def call_spread(own, collective_id):
    nseq = lax.axis_size("seq")
    return pl.pallas_call(
        spread_kernel,
        in_specs=[pl.BlockSpec(memory_space=pltpu.VMEM)],
        out_specs=pl.BlockSpec(memory_space=pltpu.VMEM),
        out_shape=sds((nseq,) + own.shape, own.dtype),
        scratch_shapes=[pltpu.SemaphoreType.DMA((nseq - 1,)),
                        pltpu.SemaphoreType.DMA((nseq - 1,))],
        compiler_params=pltpu.CompilerParams(
            collective_id=collective_id, has_side_effects=True, vmem_limit_bytes=VMEM_LIMIT
        ),
        name="spread",
    )(own)


def collect_kernel(part_ref, out_ref, slots, send, recv):
    s = lax.axis_index("seq")
    nseq = lax.axis_size("seq")
    peers = seq_peers()
    greet([peer for _, peer in peers])
    copies = [remote(part_ref.at[modulo(s + d, nseq)], slots.at[d - 1], send.at[d - 1], recv.at[d - 1], peer)
              for d, peer in peers]
    for copy in copies:
        copy.start()
    total = part_ref[s].astype(F32)
    for d, _ in peers:
        copies[d - 1].wait()
    for d in range(nseq - 1):
        total = total + slots[d].astype(F32)
    out_ref[...] = total


def call_collect(part, collective_id):
    nseq = part.shape[0]
    return pl.pallas_call(
        collect_kernel,
        in_specs=[pl.BlockSpec(memory_space=pltpu.VMEM)],
        out_specs=pl.BlockSpec(memory_space=pltpu.VMEM),
        out_shape=sds(part.shape[1:], F32),
        scratch_shapes=[pltpu.VMEM((nseq - 1,) + part.shape[1:], part.dtype),
                        pltpu.SemaphoreType.DMA((nseq - 1,)), pltpu.SemaphoreType.DMA((nseq - 1,))],
        compiler_params=pltpu.CompilerParams(
            collective_id=collective_id, has_side_effects=True, vmem_limit_bytes=VMEM_LIMIT
        ),
        name="collect",
    )(part)


def on_device(inputs, segments, w_qkv, w_out, w_up, w_down, gain_attn, gain_mlp, cotangent):
    layers = w_qkv.shape[0]
    batch, stretch, _ = inputs.shape
    nz, nseq = lax.axis_size("dp"), lax.axis_size("seq")
    spans = stretch // SPAN
    slots = gain_attn.shape[1]
    gain_shard = jnp.pad(
        jnp.concatenate([gain_attn, gain_mlp], 0).astype(F32), ((0, 8 - 2 * layers), (0, 128 - slots))
    )
    shards = []
    for l in range(layers):
        shards += [w_qkv[l], w_out[l], w_up[l], w_down[l]]
    fulls = call_gather(shards + [gain_shard], 0)
    gains = fulls[-1][:, :, : 2 * layers, :slots].transpose(2, 0, 1, 3).reshape(2 * layers, D)
    g_one = [gains[l : l + 1] for l in range(layers)]
    g_two = [gains[layers + l : layers + l + 1] for l in range(layers)]
    flat = [a.reshape((-1, a.shape[-1])) for a in fulls[:-1]]
    wq, wo, wu, wd = (flat[m::4] for m in range(4))
    bias = mask_bias(segments, stretch)

    def spread(sums, index):
        return call_spread(sums, index).transpose(1, 0, 2, 3).reshape(batch, nseq * spans, 2 * D)

    def collect(dsums, index):
        return call_collect(dsums.reshape(batch, nseq, spans, 2 * D).transpose(1, 0, 2, 3), index)

    x = inputs
    qkv, own = call_first(x, g_one[0], wq[0])
    kept = []
    for l in range(layers):
        sums = spread(own, 1)
        if l + 1 < layers:
            prob, o, h, u, x_next, qkv_next, own = call_layer(
                x, qkv, sums, bias, g_two[l], wo[l], wu[l], wd[l], g_one[l + 1], wq[l + 1]
            )
        else:
            prob, o, h, u, x_next = call_layer(x, qkv, sums, bias, g_two[l], wo[l], wu[l], wd[l])
            qkv_next = None
        kept.append((x, qkv, sums, prob, o, h, u))
        x, qkv = x_next, qkv_next
    outputs = x
    dy = cotangent
    grads = [None] * layers
    for l in reversed(range(layers)):
        x, qkv, sums, prob, o, h, u = kept[l]
        dh, near, dsums, gd, gu, go, gg_two = call_back(
            dy, u, h, o, prob, qkv, sums, g_two[l], wo[l], wu[l], wd[l]
        )
        dy, gq, gg_one = call_last(x, g_one[l], near, collect(dsums, 2), dh, wq[l])
        grads[l] = (gq, go, gu, gd, gg_one, gg_two)
    gain_grads = jnp.concatenate([grads[l][4] for l in range(layers)] + [grads[l][5] for l in range(layers)], 0)
    gain_grads = jnp.pad(
        gain_grads.reshape(2 * layers, nz * nseq, slots).transpose(1, 0, 2),
        ((0, 0), (0, 8 - 2 * layers), (0, 128 - slots)),
    ).reshape(-1, 128)
    parts = []
    for l in range(layers):
        parts += list(grads[l][:4])
    shares = call_reduce(parts + [gain_grads], 3)
    stacked = [jnp.stack(shares[m : 4 * layers : 4]) for m in range(4)]
    gain_share = shares[-1][: 2 * layers, :slots]
    return (outputs, dy, *stacked, gain_share[:layers], gain_share[layers:])


def solution(mesh):
    weights = P(None, ("dp", "seq"), None)
    gains = P(None, ("dp", "seq"))
    rows = P("dp", "seq", None)
    return jax.shard_map(
        on_device,
        mesh=mesh,
        in_specs=(rows, P("dp", None), weights, weights, weights, weights, gains, gains, rows),
        out_specs=(rows, rows, weights, weights, weights, weights, gains, gains),
        check_vma=False,
    )
```

```python
import functools

import jax
import jax.numpy as jnp
from jax import lax
from jax.experimental import pallas as pl
from jax.experimental.pallas import tpu as pltpu
from jax.sharding import PartitionSpec as P

D = 512
HEADS = 8
HEAD = 64
SPAN = 128
PAIRS = HEADS // 2
EPS = 1e-05
NEG = -1000000000.0
SCALE = HEAD ** (-0.5)
F32 = jnp.float32
BF16 = jnp.bfloat16
CHUNK = 512
VMEM_LIMIT = 60 * 1024 * 1024

NN = (((1,), (0,)), ((), ()))
NT = (((1,), (1,)), ((), ()))
TN = (((0,), (0,)), ((), ()))


def dot(left, right, dims=NN):
    return lax.dot_general(left, right, dims, preferred_element_type=F32)


def normed(values):
    mean = jnp.mean(values, -1, keepdims=True)
    centred = values - mean
    var = jnp.mean(centred * centred, -1, keepdims=True)
    rstd = lax.rsqrt(var + EPS)
    return centred * rstd, rstd


def norm_backward(dnorm, unit, rstd, gain):
    grad_gain = jnp.sum(dnorm * unit, 0, keepdims=True)
    scaled = dnorm * gain
    first = jnp.mean(scaled, -1, keepdims=True)
    second = jnp.mean(scaled * unit, -1, keepdims=True)
    return rstd * (scaled - first - unit * second), grad_gain


def project_qkv(x32, gain, wq_ref, qkv_ref, sums_ref):
    unit, _ = normed(x32)
    n_one = (unit * gain).astype(BF16)
    spans = x32.shape[0] // SPAN
    for part in range(3):
        block = dot(n_one, wq_ref[:, part * D : (part + 1) * D]).astype(BF16)
        qkv_ref[0, :, part * D : (part + 1) * D] = block
        if part > 0:
            wide = block.astype(F32)
            for span in range(spans):
                mean = jnp.sum(wide[span * SPAN : (span + 1) * SPAN], 0, keepdims=True) * (1.0 / SPAN)
                sums_ref[0, span : span + 1, (part - 1) * D : part * D] = mean.astype(BF16)


def lane_halves():
    lane = lax.broadcasted_iota(jnp.int32, (1, 2 * HEAD), 1)
    low = lane < HEAD
    return low


def head_stack(block, low, factor):
    one = jnp.where(low, factor, 0.0).astype(BF16)
    two = jnp.where(low, 0.0, factor).astype(BF16)
    return jnp.concatenate([block * one, block * two], 0)


def pair_operands(qkv_ref, sums_ref, span, pair):
    rows = slice(span * SPAN, (span + 1) * SPAN)
    lanes = slice(pair * 128, (pair + 1) * 128)
    keys = jnp.concatenate(
        [qkv_ref[0, rows, D + pair * 128 : D + (pair + 1) * 128], sums_ref[0, :, lanes]], 0
    )
    values = jnp.concatenate(
        [
            qkv_ref[0, rows, 2 * D + pair * 128 : 2 * D + (pair + 1) * 128],
            sums_ref[0, :, D + pair * 128 : D + (pair + 1) * 128],
        ],
        0,
    )
    query = qkv_ref[0, rows, lanes]
    return query, keys, values


def attention_forward(qkv_ref, sums_ref, bias_ref, prob_ref, o_ref):
    low = lane_halves()
    spans = qkv_ref.shape[1] // SPAN
    for span in range(spans):
        bias = bias_ref[0, span]
        bias = jnp.concatenate([bias, bias], 1)
        for pair in range(PAIRS):
            query, keys, values = pair_operands(qkv_ref, sums_ref, span, pair)
            scores = dot(keys, head_stack(query, low, SCALE), NT) + bias
            top = jnp.max(scores, 0, keepdims=True)
            exps = jnp.exp(scores - top)
            total = jnp.sum(exps, 0, keepdims=True)
            prob = (exps * (1.0 / total)).astype(BF16)
            prob_ref[0, span, pair] = prob
            both = dot(prob, values, TN)
            o_ref[0, span * SPAN : (span + 1) * SPAN, pair * 128 : (pair + 1) * 128] = jnp.where(
                low, both[:SPAN], both[SPAN:]
            ).astype(BF16)


def attention_backward(qkv_ref, sums_ref, prob_ref, dout, dqkv_ref, dsums_ref):
    low = lane_halves()
    spans = qkv_ref.shape[1] // SPAN
    for pair in range(PAIRS):
        lanes = slice(pair * 128, (pair + 1) * 128)
        klanes = slice(D + pair * 128, D + (pair + 1) * 128)
        vlanes = slice(2 * D + pair * 128, 2 * D + (pair + 1) * 128)
        dksum = dvsum = 0.0
        for span in range(spans):
            rows = slice(span * SPAN, (span + 1) * SPAN)
            query, keys, values = pair_operands(qkv_ref, sums_ref, span, pair)
            q_stack = head_stack(query, low, SCALE)
            do_stack = head_stack(dout[rows, lanes], low, 1.0)
            prob = prob_ref[0, span, pair]
            wide = prob.astype(F32)
            dprob = dot(values, do_stack, NT)
            rowdot = jnp.sum(wide * dprob, 0, keepdims=True)
            dscore = (wide * (dprob - rowdot)).astype(BF16)
            dboth = dot(dscore, keys, TN)
            dquery = jnp.where(low, dboth[:SPAN], dboth[SPAN:]) * SCALE
            dkeys = dot(dscore, q_stack)
            dvalues = dot(prob, do_stack)
            dqkv_ref[0, rows, lanes] = dquery.astype(BF16)
            dqkv_ref[0, rows, klanes] = dkeys[:SPAN].astype(BF16)
            dqkv_ref[0, rows, vlanes] = dvalues[:SPAN].astype(BF16)
            dksum = dksum + dkeys[SPAN:]
            dvsum = dvsum + dvalues[SPAN:]
        dsums_ref[0, :, pair * 128 : (pair + 1) * 128] = dksum.astype(BF16)
        dsums_ref[0, :, D + pair * 128 : D + (pair + 1) * 128] = dvsum.astype(BF16)


G0 = 0.7978845608
G1 = 0.7978845608 * 0.044715


def gelu(values):
    squared = values * values
    slope = jnp.tanh(values * (G0 + G1 * squared))
    half = 0.5 * values
    return half + half * slope


def gelu_both(values):
    squared = values * values
    slope = jnp.tanh(values * (G0 + G1 * squared))
    half = 0.5 * values
    rise = 0.5 + 0.5 * slope
    inner = G0 + (3.0 * G1) * squared
    return values * rise, rise + half * (1.0 - slope * slope) * inner


def mlp_forward(h32, gain, wu_ref, wd_ref, u_ref):
    unit, _ = normed(h32)
    n_two = (unit * gain).astype(BF16)
    total = h32
    for start in range(0, wu_ref.shape[1], CHUNK):
        upper = dot(n_two, wu_ref[:, start : start + CHUNK])
        u_ref[0, :, start : start + CHUNK] = upper.astype(BF16)
        total = total + dot(gelu(upper).astype(BF16), wd_ref[start : start + CHUNK, :])
    return total


def first_kernel(x_ref, gain_ref, wq_ref, qkv_ref, sums_ref):
    project_qkv(x_ref[0].astype(F32), gain_ref[...], wq_ref, qkv_ref, sums_ref)


def layer_kernel(last, *refs):
    if last:
        (x_ref, qkv_ref, sums_ref, bias_ref, gain_ref, wo_ref, wu_ref, wd_ref,
         prob_ref, o_ref, h_ref, u_ref, next_ref) = refs
    else:
        (x_ref, qkv_ref, sums_ref, bias_ref, gain_ref, wo_ref, wu_ref, wd_ref, gain_next_ref, wq_ref,
         prob_ref, o_ref, h_ref, u_ref, next_ref, qkv_next_ref, sums_next_ref) = refs
    attention_forward(qkv_ref, sums_ref, bias_ref, prob_ref, o_ref)
    hidden = x_ref[0].astype(F32) + dot(o_ref[0], wo_ref[...])
    h_ref[0] = hidden
    result = mlp_forward(hidden, gain_ref[...], wu_ref, wd_ref, u_ref)
    next_ref[0] = result.astype(next_ref.dtype)
    if not last:
        project_qkv(result, gain_next_ref[...], wq_ref, qkv_next_ref, sums_next_ref)


def accumulate(ref, index, value, first):
    @pl.when(first)
    def _():
        ref[index] = value

    @pl.when(jnp.logical_not(first))
    def _():
        ref[index] = ref[index] + value


def mlp_attention_backward(dy32, u_ref, h_ref, o_ref, prob_ref, qkv_ref, sums_ref, gain_ref,
                           wo_ref, wu_ref, wd_ref, dh_ref, dqkv_ref, dsums_ref, gd_ref, gu_ref,
                           go_ref, gg_ref):
    ddown = dy32.astype(BF16)
    unit, rstd = normed(h_ref[0])
    n_two = (unit * gain_ref[...]).astype(BF16)
    dn_two = 0.0
    for start in range(0, wu_ref.shape[1], CHUNK):
        cols = slice(start, start + CHUNK)
        dactive = dot(ddown, wd_ref[cols, :], NT)
        active, slope = gelu_both(u_ref[0, :, cols].astype(F32))
        gd_ref[cols, :] += dot(active.astype(BF16), ddown, TN)
        dupper = (dactive * slope).astype(BF16)
        gu_ref[:, cols] += dot(n_two, dupper, TN)
        dn_two = dn_two + dot(dupper, wu_ref[:, cols], NT)
    dnorm, grad_gain = norm_backward(dn_two, unit, rstd, gain_ref[...])
    gg_ref[...] += grad_gain
    dhidden = dy32 + dnorm
    dh_ref[0] = dhidden
    dattn = dhidden.astype(BF16)
    go_ref[...] += dot(o_ref[0], dattn, TN)
    dout = dot(dattn, wo_ref[...], NT).astype(BF16)
    attention_backward(qkv_ref, sums_ref, prob_ref, dout, dqkv_ref, dsums_ref)


def back_kernel(dy_ref, u_ref, h_ref, o_ref, prob_ref, qkv_ref, sums_ref, gain_ref,
                wo_ref, wu_ref, wd_ref, dh_ref, dqkv_ref, dsums_ref, gd_out, gu_out, go_out,
                gg_ref, gd_ref, gu_ref, go_ref):
    step = pl.program_id(0)

    @pl.when(step == 0)
    def _():
        gd_ref[...] = jnp.zeros_like(gd_ref)
        gu_ref[...] = jnp.zeros_like(gu_ref)
        go_ref[...] = jnp.zeros_like(go_ref)
        gg_ref[...] = jnp.zeros_like(gg_ref)

    mlp_attention_backward(dy_ref[0].astype(F32), u_ref, h_ref, o_ref, prob_ref, qkv_ref, sums_ref,
                           gain_ref, wo_ref, wu_ref, wd_ref, dh_ref, dqkv_ref, dsums_ref, gd_ref,
                           gu_ref, go_ref, gg_ref)

    @pl.when(step == pl.num_programs(0) - 1)
    def _():
        gd_out[...] = gd_ref[...].astype(BF16)
        gu_out[...] = gu_ref[...].astype(BF16)
        go_out[...] = go_ref[...].astype(BF16)


def qkv_backward(x32, gain, near_ref, dsums_ref, dh, wq_ref, gq_ref, gg_ref):
    unit, rstd = normed(x32)
    n_one = (unit * gain).astype(BF16)
    dn_one = 0.0
    tokens = x32.shape[0]
    for part in range(3):
        cols = slice(part * D, (part + 1) * D)
        block = near_ref[0, :, cols]
        if part > 0:
            pieces = []
            for span in range(tokens // SPAN):
                share = dsums_ref[0, span : span + 1, (part - 1) * D : part * D].astype(F32) * (1.0 / SPAN)
                pieces.append(block[span * SPAN : (span + 1) * SPAN].astype(F32) + share)
            block = jnp.concatenate(pieces, 0).astype(BF16)
        gq_ref[:, cols] += dot(n_one, block, TN)
        dn_one = dn_one + dot(block, wq_ref[:, cols], NT)
    dnorm, grad_gain = norm_backward(dn_one, unit, rstd, gain)
    gg_ref[...] += grad_gain
    return dh + dnorm


def last_kernel(x_ref, gain_ref, near_ref, dsums_ref, dh_ref, wq_ref, dx_ref, gq_out, gg_ref, gq_ref):
    step = pl.program_id(0)

    @pl.when(step == 0)
    def _():
        gq_ref[...] = jnp.zeros_like(gq_ref)
        gg_ref[...] = jnp.zeros_like(gg_ref)

    dx_ref[0] = qkv_backward(x_ref[0].astype(F32), gain_ref[...], near_ref, dsums_ref, dh_ref[0], wq_ref,
                             gq_ref, gg_ref)

    @pl.when(step == pl.num_programs(0) - 1)
    def _():
        gq_out[...] = gq_ref[...].astype(BF16)


def per_seq(shape):
    rest = len(shape) - 1
    return pl.BlockSpec((1,) + tuple(shape[1:]), lambda b: (b,) + (0,) * rest)


def whole(shape):
    rank = len(shape)
    return pl.BlockSpec(tuple(shape), lambda b: (0,) * rank, pipeline_mode=pl.Buffered(1))


def sds(shape, dtype):
    return jax.ShapeDtypeStruct(tuple(shape), dtype)


def params():
    return pltpu.CompilerParams(dimension_semantics=("arbitrary",), vmem_limit_bytes=VMEM_LIMIT)


def call_first(x, gain, wq):
    batch, tokens, _ = x.shape
    spans = tokens // SPAN
    outs = (sds((batch, tokens, 3 * D), BF16), sds((batch, spans, 2 * D), BF16))
    return pl.pallas_call(
        first_kernel,
        grid=(batch,),
        in_specs=[per_seq(x.shape), whole(gain.shape), whole(wq.shape)],
        out_specs=[per_seq(o.shape) for o in outs],
        out_shape=outs,
        compiler_params=params(),
        name="first",
    )(x, gain, wq)


def call_layer(x, qkv, sums, bias, gain, wo, wu, wd, gain_next=None, wq=None):
    batch, tokens, _ = x.shape
    spans = tokens // SPAN
    last = wq is None
    keys = SPAN + sums.shape[1]
    outs = [
        sds((batch, spans, PAIRS, keys, 2 * SPAN), BF16),
        sds((batch, tokens, D), BF16),
        sds((batch, tokens, D), F32),
        sds((batch, tokens, wu.shape[1]), BF16),
        sds((batch, tokens, D), BF16 if last else F32),
    ]
    args = [x, qkv, sums, bias, gain, wo, wu, wd]
    if not last:
        outs += [sds((batch, tokens, 3 * D), BF16), sds((batch, spans, 2 * D), BF16)]
        args += [gain_next, wq]
    specs = [per_seq(a.shape) for a in args[:4]] + [whole(a.shape) for a in args[4:]]
    return pl.pallas_call(
        functools.partial(layer_kernel, last),
        grid=(batch,),
        in_specs=specs,
        out_specs=[per_seq(o.shape) for o in outs],
        out_shape=outs,
        compiler_params=params(),
        name="layer",
    )(*args)


def call_back(dy, u, h, o, prob, qkv, sums, gain, wo, wu, wd):
    batch, tokens, _ = dy.shape
    args = [dy, u, h, o, prob, qkv, sums, gain, wo, wu, wd]
    specs = [per_seq(a.shape) for a in args[:7]] + [whole(a.shape) for a in args[7:]]
    outs = [sds(h.shape, F32), sds(qkv.shape, BF16), sds(sums.shape, BF16),
            sds(wd.shape, BF16), sds(wu.shape, BF16), sds(wo.shape, BF16), sds((1, D), F32)]
    return pl.pallas_call(
        back_kernel,
        grid=(batch,),
        in_specs=specs,
        out_specs=[per_seq(o.shape) for o in outs[:3]] + [whole(o.shape) for o in outs[3:]],
        out_shape=outs,
        scratch_shapes=[pltpu.VMEM(wd.shape, F32), pltpu.VMEM(wu.shape, F32), pltpu.VMEM(wo.shape, F32)],
        compiler_params=params(),
        name="back",
    )(*args)


def call_last(x, gain, near, dsums, dh, wq):
    batch, tokens, _ = x.shape
    outs = [sds((batch, tokens, D), F32), sds(wq.shape, BF16), sds((1, D), F32)]
    return pl.pallas_call(
        last_kernel,
        grid=(batch,),
        in_specs=[per_seq(x.shape), whole(gain.shape), per_seq(near.shape), per_seq(dsums.shape),
                  per_seq(dh.shape), whole(wq.shape)],
        out_specs=[per_seq(outs[0].shape), whole(outs[1].shape), whole(outs[2].shape)],
        out_shape=outs,
        scratch_shapes=[pltpu.VMEM(wq.shape, F32)],
        compiler_params=params(),
        name="last",
    )(x, gain, near, dsums, dh, wq)


def mask_bias(segments, stretch):
    batch, length = segments.shape
    rank = lax.axis_index("seq")
    own = lax.dynamic_slice_in_dim(segments, rank * stretch, stretch, 1).reshape(batch, -1, SPAN)
    ends = segments.reshape(batch, -1, SPAN)[:, :, SPAN - 1]
    spans = own.shape[1]
    pos = jnp.arange(SPAN)
    near = (own[:, :, :, None] == own[:, :, None, :]) & (pos[:, None] <= pos[None, :])
    ids = rank * spans + jnp.arange(spans)
    before = jnp.arange(ends.shape[1])[None, :] < ids[:, None]
    far = (ends[:, None, :, None] == own[:, :, None, :]) & before[None, :, :, None]
    return jnp.where(jnp.concatenate([near, far], 2), 0.0, NEG).astype(F32)

MESH = pl.DeviceIdType.MESH
CORES = 2


def place():
    nz, nseq = lax.axis_size("dp"), lax.axis_size("seq")
    z, s = lax.axis_index("dp"), lax.axis_index("seq")
    return nz, nseq // CORES, z, s // CORES, lax.rem(s, CORES)


def modulo(value, size):
    return lax.rem(value + size, size)


def peers_of():
    nz, nchip, z, chip, core = place()
    seq = chip * CORES + core
    out = [(modulo(z + d, nz), seq) for d in range(1, nz)]
    out += [(z, modulo(chip + d, nchip) * CORES + core) for d in range(1, nchip)]
    out.append((z, chip * CORES + 1 - core))
    return out


def greet(peers):
    barrier = pltpu.get_barrier_semaphore()
    for peer in peers:
        pl.semaphore_signal(barrier, inc=1, device_id=peer, device_id_type=MESH)
    pl.semaphore_wait(barrier, len(peers))


def remote(src, dst, send, recv, peer):
    return pltpu.make_async_remote_copy(
        src_ref=src, dst_ref=dst, send_sem=send, recv_sem=recv, device_id=peer, device_id_type=MESH
    )


class Gather:
    def __init__(self, shards, fulls, sems):
        self.shards, self.fulls = shards, fulls
        self.own, self.zs, self.zr, self.ps, self.pr, self.cs, self.cr = sems
        self.nz, self.nchip, self.z, self.chip, self.core = place()
        self.seq = self.chip * CORES + self.core

    @staticmethod
    def scratch(count):
        nz, nchip = lax.axis_size("dp"), lax.axis_size("seq") // CORES
        dma = pltpu.SemaphoreType.DMA
        return [dma((count,)), dma((count, nz - 1)), dma((count, nz - 1)), dma((count, nchip - 1)),
                dma((count, nchip - 1)), dma((count, nchip)), dma((count, nchip))]

    def local(self, t):
        return pltpu.make_async_copy(self.shards[t], self.fulls[t].at[self.z, self.seq], self.own.at[t])

    def line(self, t, d):
        peer = (modulo(self.z + d, self.nz), self.seq)
        return remote(self.shards[t], self.fulls[t].at[self.z, self.seq], self.zs.at[t, d - 1],
                      self.zr.at[t, d - 1], peer)

    def plane(self, t, d):
        block = self.fulls[t].at[:, self.seq]
        peer = (self.z, modulo(self.chip + d, self.nchip) * CORES + self.core)
        return remote(block, block, self.ps.at[t, d - 1], self.pr.at[t, d - 1], peer)

    def cross(self, t, d):
        block = self.fulls[t].at[:, modulo(self.chip - d, self.nchip) * CORES + self.core]
        peer = (self.z, self.chip * CORES + 1 - self.core)
        return remote(block, block, self.cs.at[t, d], self.cr.at[t, d], peer)

    def start(self, t):
        self.local(t).start()
        for d in range(1, self.nz):
            self.line(t, d).start()

    def spread(self, t):
        self.local(t).wait()
        for d in range(1, self.nz):
            self.line(t, d).wait_recv()
        for d in range(1, self.nchip):
            self.plane(t, d).start()
        self.cross(t, 0).start()

    def share(self, t):
        for d in range(1, self.nchip):
            self.plane(t, d).wait_recv()
            self.cross(t, d).start()

    def finish(self, t):
        for d in range(self.nchip):
            self.cross(t, d).wait_recv()

    def drain(self, t):
        for d in range(1, self.nz):
            self.line(t, d).wait_send()
        for d in range(1, self.nchip):
            self.plane(t, d).wait_send()
        for d in range(self.nchip):
            self.cross(t, d).wait_send()


def gather_kernel(count, *refs):
    work = Gather(refs[:count], refs[count : 2 * count], refs[2 * count :])
    greet(peers_of())
    for stage in (work.start, work.spread, work.share, work.finish, work.drain):
        for t in range(count):
            stage(t)


def call_gather(shards, collective_id):
    nz, nseq = lax.axis_size("dp"), lax.axis_size("seq")
    count = len(shards)
    outs = [sds((nz, nseq) + a.shape, a.dtype) for a in shards]
    return pl.pallas_call(
        functools.partial(gather_kernel, count),
        in_specs=[pl.BlockSpec(memory_space=pltpu.VMEM)] * count,
        out_specs=[pl.BlockSpec(memory_space=pl.ANY)] * count,
        out_shape=outs,
        scratch_shapes=Gather.scratch(count),
        compiler_params=pltpu.CompilerParams(
            collective_id=collective_id, has_side_effects=True, vmem_limit_bytes=VMEM_LIMIT
        ),
        name="gather",
    )(*shards)


class Reduce:
    def __init__(self, parts, outs, bufs, sems):
        self.parts, self.outs = parts, outs
        count = len(parts)
        self.mine, self.cross_in, self.plane_in, self.col, self.line_in = (
            bufs[i * count : (i + 1) * count] for i in range(5)
        )
        self.own, self.cs, self.cr, self.ps, self.pr, self.zs, self.zr = sems
        self.nz, self.nchip, self.z, self.chip, self.core = place()
        self.seq = self.chip * CORES + self.core

    @staticmethod
    def scratch(parts):
        nz, nchip = lax.axis_size("dp"), lax.axis_size("seq") // CORES
        dma = pltpu.SemaphoreType.DMA
        count = len(parts)
        bufs = []
        for lead in ((nchip, nz), (nchip, nz), (nchip - 1, nz), (nz,), (nz - 1,)):
            bufs += [pltpu.VMEM(lead + a.shape[3:], a.dtype) for a in parts]
        return bufs + [dma((count, nchip)), dma((count, nchip)), dma((count, nchip)), dma((count, nchip - 1)),
                       dma((count, nchip - 1)), dma((count, nz - 1)), dma((count, nz - 1))]

    def local(self, t, d):
        chip = modulo(self.chip + d, self.nchip)
        return pltpu.make_async_copy(self.parts[t].at[:, chip, self.core], self.mine[t].at[d], self.own.at[t, d])

    def cross(self, t, d):
        chip = modulo(self.chip + d, self.nchip)
        peer = (self.z, self.chip * CORES + 1 - self.core)
        return remote(self.parts[t].at[:, chip, 1 - self.core], self.cross_in[t].at[d], self.cs.at[t, d],
                      self.cr.at[t, d], peer)

    def plane(self, t, d):
        peer = (self.z, modulo(self.chip + d, self.nchip) * CORES + self.core)
        return remote(self.mine[t].at[d], self.plane_in[t].at[d - 1], self.ps.at[t, d - 1],
                      self.pr.at[t, d - 1], peer)

    def line(self, t, d):
        z = modulo(self.z + d, self.nz)
        return remote(self.col[t].at[z], self.line_in[t].at[d - 1], self.zs.at[t, d - 1],
                      self.zr.at[t, d - 1], (z, self.seq))

    def order(self):
        return list(range(1, self.nchip)) + [0]

    def start(self, t):
        for d in self.order():
            self.cross(t, d).start()
            self.local(t, d).start()

    def combine(self, t):
        for d in self.order():
            self.local(t, d).wait()
            self.cross(t, d).wait_recv()

            def add(i, carry):
                total = self.mine[t][d, i].astype(F32) + self.cross_in[t][d, i].astype(F32)
                self.mine[t][d, i] = total.astype(self.mine[t].dtype)
                return carry

            lax.fori_loop(0, self.nz, add, 0)
            if d > 0:
                self.plane(t, d).start()

    def column(self, t):
        for d in range(1, self.nchip):
            self.plane(t, d).wait_recv()

        def add(i, carry):
            total = self.mine[t][0, i].astype(F32)
            for d in range(self.nchip - 1):
                total = total + self.plane_in[t][d, i].astype(F32)
            self.col[t][i] = total.astype(self.col[t].dtype)
            return carry

        lax.fori_loop(0, self.nz, add, 0)
        for d in range(1, self.nz):
            self.line(t, d).start()

    def finish(self, t):
        total = self.col[t][self.z].astype(F32)
        for d in range(1, self.nz):
            self.line(t, d).wait_recv()
        for d in range(self.nz - 1):
            total = total + self.line_in[t][d].astype(F32)
        self.outs[t][...] = total

    def drain(self, t):
        for d in self.order():
            self.cross(t, d).wait_send()
        for d in range(1, self.nchip):
            self.plane(t, d).wait_send()
        for d in range(1, self.nz):
            self.line(t, d).wait_send()


def reduce_kernel(count, *refs):
    work = Reduce(refs[:count], refs[count : 2 * count], refs[2 * count : 7 * count], refs[7 * count :])
    greet(peers_of())
    for stage in (work.start, work.combine, work.column, work.finish, work.drain):
        for t in range(count):
            stage(t)


def call_reduce(parts, collective_id):
    nz, nseq = lax.axis_size("dp"), lax.axis_size("seq")
    count = len(parts)
    parts = [a.reshape((nz, nseq // CORES, CORES, a.shape[0] // (nz * nseq)) + a.shape[1:]) for a in parts]
    outs = [sds(a.shape[3:], F32) for a in parts]
    return pl.pallas_call(
        functools.partial(reduce_kernel, count),
        in_specs=[pl.BlockSpec(memory_space=pl.ANY)] * count,
        out_specs=[pl.BlockSpec(memory_space=pltpu.VMEM)] * count,
        out_shape=outs,
        scratch_shapes=Reduce.scratch(parts),
        compiler_params=pltpu.CompilerParams(
            collective_id=collective_id, has_side_effects=True, vmem_limit_bytes=VMEM_LIMIT
        ),
        name="reduce",
    )(*parts)


def seq_peers():
    nseq = lax.axis_size("seq")
    z, s = lax.axis_index("dp"), lax.axis_index("seq")
    return [(d, (z, modulo(s + d, nseq))) for d in range(1, nseq)]


def spread_kernel(own_ref, all_ref, send, recv):
    s = lax.axis_index("seq")
    peers = seq_peers()
    greet([peer for _, peer in peers])
    copies = [remote(own_ref, all_ref.at[s], send.at[d - 1], recv.at[d - 1], peer) for d, peer in peers]
    for copy in copies:
        copy.start()
    all_ref[s] = own_ref[...]
    for copy in copies:
        copy.wait()


def call_spread(own, collective_id):
    nseq = lax.axis_size("seq")
    return pl.pallas_call(
        spread_kernel,
        in_specs=[pl.BlockSpec(memory_space=pltpu.VMEM)],
        out_specs=pl.BlockSpec(memory_space=pltpu.VMEM),
        out_shape=sds((nseq,) + own.shape, own.dtype),
        scratch_shapes=[pltpu.SemaphoreType.DMA((nseq - 1,)),
                        pltpu.SemaphoreType.DMA((nseq - 1,))],
        compiler_params=pltpu.CompilerParams(
            collective_id=collective_id, has_side_effects=True, vmem_limit_bytes=VMEM_LIMIT
        ),
        name="spread",
    )(own)


def collect_kernel(part_ref, out_ref, slots, send, recv):
    s = lax.axis_index("seq")
    nseq = lax.axis_size("seq")
    peers = seq_peers()
    greet([peer for _, peer in peers])
    copies = [remote(part_ref.at[modulo(s + d, nseq)], slots.at[d - 1], send.at[d - 1], recv.at[d - 1], peer)
              for d, peer in peers]
    for copy in copies:
        copy.start()
    total = part_ref[s].astype(F32)
    for d, _ in peers:
        copies[d - 1].wait()
    for d in range(nseq - 1):
        total = total + slots[d].astype(F32)
    out_ref[...] = total


def call_collect(part, collective_id):
    nseq = part.shape[0]
    return pl.pallas_call(
        collect_kernel,
        in_specs=[pl.BlockSpec(memory_space=pltpu.VMEM)],
        out_specs=pl.BlockSpec(memory_space=pltpu.VMEM),
        out_shape=sds(part.shape[1:], F32),
        scratch_shapes=[pltpu.VMEM((nseq - 1,) + part.shape[1:], part.dtype),
                        pltpu.SemaphoreType.DMA((nseq - 1,)), pltpu.SemaphoreType.DMA((nseq - 1,))],
        compiler_params=pltpu.CompilerParams(
            collective_id=collective_id, has_side_effects=True, vmem_limit_bytes=VMEM_LIMIT
        ),
        name="collect",
    )(part)


def on_device(inputs, segments, w_qkv, w_out, w_up, w_down, gain_attn, gain_mlp, cotangent):
    layers = w_qkv.shape[0]
    batch, stretch, _ = inputs.shape
    nz, nseq = lax.axis_size("dp"), lax.axis_size("seq")
    spans = stretch // SPAN
    slots = gain_attn.shape[1]
    gain_shard = jnp.pad(
        jnp.concatenate([gain_attn, gain_mlp], 0).astype(F32), ((0, 8 - 2 * layers), (0, 128 - slots))
    )
    shards = []
    for l in range(layers):
        shards += [w_qkv[l], w_out[l], w_up[l], w_down[l]]
    fulls = call_gather(shards + [gain_shard], 0)
    gains = fulls[-1][:, :, : 2 * layers, :slots].transpose(2, 0, 1, 3).reshape(2 * layers, D)
    g_one = [gains[l : l + 1] for l in range(layers)]
    g_two = [gains[layers + l : layers + l + 1] for l in range(layers)]
    flat = [a.reshape((-1, a.shape[-1])) for a in fulls[:-1]]
    wq, wo, wu, wd = (flat[m::4] for m in range(4))
    bias = mask_bias(segments, stretch)

    def spread(sums, index):
        return call_spread(sums, index).transpose(1, 0, 2, 3).reshape(batch, nseq * spans, 2 * D)

    def collect(dsums, index):
        return call_collect(dsums.reshape(batch, nseq, spans, 2 * D).transpose(1, 0, 2, 3), index)

    x = inputs
    qkv, own = call_first(x, g_one[0], wq[0])
    kept = []
    for l in range(layers):
        sums = spread(own, 1)
        if l + 1 < layers:
            prob, o, h, u, x_next, qkv_next, own = call_layer(
                x, qkv, sums, bias, g_two[l], wo[l], wu[l], wd[l], g_one[l + 1], wq[l + 1]
            )
        else:
            prob, o, h, u, x_next = call_layer(x, qkv, sums, bias, g_two[l], wo[l], wu[l], wd[l])
            qkv_next = None
        kept.append((x, qkv, sums, prob, o, h, u))
        x, qkv = x_next, qkv_next
    outputs = x
    dy = cotangent
    grads = [None] * layers
    for l in reversed(range(layers)):
        x, qkv, sums, prob, o, h, u = kept[l]
        dh, near, dsums, gd, gu, go, gg_two = call_back(
            dy, u, h, o, prob, qkv, sums, g_two[l], wo[l], wu[l], wd[l]
        )
        dy, gq, gg_one = call_last(x, g_one[l], near, collect(dsums, 2), dh, wq[l])
        grads[l] = (gq, go, gu, gd, gg_one, gg_two)
    gain_grads = jnp.concatenate([grads[l][4] for l in range(layers)] + [grads[l][5] for l in range(layers)], 0)
    gain_grads = jnp.pad(
        gain_grads.reshape(2 * layers, nz * nseq, slots).transpose(1, 0, 2),
        ((0, 0), (0, 8 - 2 * layers), (0, 128 - slots)),
    ).reshape(-1, 128)
    parts = []
    for l in range(layers):
        parts += list(grads[l][:4])
    shares = call_reduce(parts + [gain_grads], 3)
    stacked = [jnp.stack(shares[m : 4 * layers : 4]) for m in range(4)]
    gain_share = shares[-1][: 2 * layers, :slots]
    return (outputs, dy, *stacked, gain_share[:layers], gain_share[layers:])


class Spot:
    def __init__(self):
        self.nz, self.nseq = lax.axis_size("dp"), lax.axis_size("seq")
        self.z, self.seq = lax.axis_index("dp"), lax.axis_index("seq")
        self.chip, self.core = lax.div(self.seq, CORES), lax.rem(self.seq, CORES)
        row, col = lax.div(self.chip, 2), lax.rem(self.chip, 2)
        across, along = row * 2 + 1 - col, (1 - row) * 2 + col
        self.first = (1 - self.core) * across + self.core * along
        self.second = (1 - self.core) * along + self.core * across
        self.diagonal = (1 - row) * 2 + 1 - col

    def at_chip(self, chip):
        return (self.z, chip * CORES + self.core)

    def twin(self):
        return (self.z, self.chip * CORES + 1 - self.core)

    def on_line(self, d):
        return (modulo(self.z + d, self.nz), self.seq)

    def signal(self):
        barrier = pltpu.get_barrier_semaphore()
        for peer in self.peers():
            pl.semaphore_signal(barrier, inc=1, device_id=peer, device_id_type=MESH)

    def meet(self):
        pl.semaphore_wait(pltpu.get_barrier_semaphore(), len(self.peers()))

    def peers(self):
        out = [self.on_line(d) for d in range(1, self.nz)]
        return out + [(self.z, modulo(self.seq + d, self.nseq)) for d in range(1, self.nseq)]


def dma(*shape):
    return pltpu.SemaphoreType.DMA(shape)


class Fetch:
    def __init__(self, spot, shards, fulls, sems):
        self.spot, self.shards, self.fulls = spot, shards, fulls
        self.own, self.zs, self.zr, self.hs, self.hr, self.cs, self.cr = sems

    @staticmethod
    def scratch(count, nz):
        return [dma(count), dma(count, nz - 1), dma(count, nz - 1), dma(count, 3), dma(count, 3),
                dma(count, 4), dma(count, 4)]

    def local(self, t):
        return pltpu.make_async_copy(
            self.shards[t], self.fulls[t].at[self.spot.z, self.spot.seq], self.own.at[t])

    def line(self, t, d):
        return remote(self.shards[t], self.fulls[t].at[self.spot.z, self.spot.seq], self.zs.at[t, d - 1],
                      self.zr.at[t, d - 1], self.spot.on_line(d))

    def hop(self, t, k):
        spot = self.spot
        chip = (spot.chip, spot.chip, spot.first)[k]
        target = (spot.first, spot.second, spot.second)[k]
        block = self.fulls[t].at[:, chip * CORES + spot.core]
        return remote(block, block, self.hs.at[t, k], self.hr.at[t, k], spot.at_chip(target))

    def cross(self, t, k):
        spot = self.spot
        chip = (spot.chip, spot.first, spot.second, spot.diagonal)[k]
        block = self.fulls[t].at[:, chip * CORES + spot.core]
        return remote(block, block, self.cs.at[t, k], self.cr.at[t, k], spot.twin())

    def start(self, t):
        self.local(t).start()
        for d in range(1, self.spot.nz):
            self.line(t, d).start()

    def spread(self, t):
        self.local(t).wait()
        for d in range(1, self.spot.nz):
            self.line(t, d).wait_recv()
        self.hop(t, 0).start()
        self.hop(t, 1).start()
        self.cross(t, 0).start()

    def relay(self, t):
        self.hop(t, 0).wait_recv()
        self.hop(t, 2).start()
        self.cross(t, 1).start()

    def share(self, t):
        self.hop(t, 1).wait_recv()
        self.cross(t, 2).start()

    def close(self, t):
        self.hop(t, 2).wait_recv()
        self.cross(t, 3).start()

    def finish(self, t):
        for k in range(4):
            self.cross(t, k).wait_recv()

    def drain(self, t):
        for d in range(1, self.spot.nz):
            self.line(t, d).wait_send()
        for k in range(3):
            self.hop(t, k).wait_send()
        for k in range(4):
            self.cross(t, k).wait_send()


class Fold:
    def __init__(self, spot, parts, outs, bufs, sems):
        self.spot, self.parts, self.outs = spot, parts, outs
        count = len(parts)
        self.mine, self.twin_in, self.first_in, self.second_in, self.col, self.line_in = (
            bufs[i * count : (i + 1) * count] for i in range(6)
        )
        self.own, self.cs, self.cr, self.hs, self.hr, self.zs, self.zr = sems

    @staticmethod
    def buffers(shapes, nz):
        out = []
        for lead in ((4, nz), (4, nz), (2, nz), (nz,), (nz,), (nz - 1,)):
            out += [pltpu.VMEM(lead + tuple(shape), BF16) for shape in shapes]
        return out

    @staticmethod
    def sems(count, nz):
        return [dma(count, 4), dma(count, 4), dma(count, 4), dma(count, 3), dma(count, 3),
                dma(count, nz - 1), dma(count, nz - 1)]

    def local(self, t, k):
        spot = self.spot
        chip = (spot.chip, spot.first, spot.second, spot.diagonal)[k]
        return pltpu.make_async_copy(self.parts[t].at[:, chip, spot.core], self.mine[t].at[k], self.own.at[t, k])

    def cross(self, t, k):
        spot = self.spot
        chip = (spot.chip, spot.second, spot.first, spot.diagonal)[k]
        return remote(self.parts[t].at[:, chip, 1 - spot.core], self.twin_in[t].at[k], self.cs.at[t, k],
                      self.cr.at[t, k], spot.twin())

    def hop(self, t, k):
        spot = self.spot
        source = self.mine[t].at[(1, 3, 2)[k]]
        target = (self.first_in[t].at[0], self.first_in[t].at[1], self.second_in[t])[k]
        chip = (spot.first, spot.first, spot.second)[k]
        return remote(source, target, self.hs.at[t, k], self.hr.at[t, k], spot.at_chip(chip))

    def line(self, t, d):
        z = modulo(self.spot.z + d, self.spot.nz)
        return remote(self.col[t].at[z], self.line_in[t].at[d - 1], self.zs.at[t, d - 1], self.zr.at[t, d - 1],
                      self.spot.on_line(d))

    def start(self, t):
        for k in (3, 1, 2, 0):
            self.cross(t, k).start()
            self.local(t, k).start()

    def combine(self, t):
        mine, twin_in = self.mine[t], self.twin_in[t]
        for k in (3, 1, 2, 0):
            self.local(t, k).wait()
            self.cross(t, k).wait_recv()

            def add(i, carry):
                mine[k, i] = (mine[k, i].astype(F32) + twin_in[k, i].astype(F32)).astype(BF16)
                return carry

            lax.fori_loop(0, self.spot.nz, add, 0)
            if k == 3:
                self.hop(t, 1).start()
            elif k == 1:
                self.hop(t, 0).start()

    def middle(self, t):
        mine, first_in = self.mine[t], self.first_in[t]
        self.hop(t, 1).wait_recv()

        def add(i, carry):
            mine[2, i] = (mine[2, i].astype(F32) + first_in[1, i].astype(F32)).astype(BF16)
            return carry

        lax.fori_loop(0, self.spot.nz, add, 0)
        self.hop(t, 2).start()

    def column(self, t):
        mine, first_in, second_in, col = self.mine[t], self.first_in[t], self.second_in[t], self.col[t]
        self.hop(t, 0).wait_recv()
        self.hop(t, 2).wait_recv()

        def add(i, carry):
            total = mine[0, i].astype(F32) + first_in[0, i].astype(F32) + second_in[i].astype(F32)
            col[i] = total.astype(BF16)
            return carry

        lax.fori_loop(0, self.spot.nz, add, 0)
        for d in range(1, self.spot.nz):
            self.line(t, d).start()

    def finish(self, t):
        total = self.col[t][self.spot.z].astype(F32)
        for d in range(1, self.spot.nz):
            self.line(t, d).wait_recv()
        for d in range(self.spot.nz - 1):
            total = total + self.line_in[t][d].astype(F32)
        self.outs[t][...] = total

    def drain(self, t):
        for k in range(4):
            self.cross(t, k).wait_send()
        for k in range(3):
            self.hop(t, k).wait_send()
        for d in range(1, self.spot.nz):
            self.line(t, d).wait_send()


class AllSum:
    def __init__(self, spot, source, bufs):
        self.spot, self.source = spot, source
        self.twin_in, self.pair, self.plane_in, self.col, self.line_in, self.ss, self.rs = bufs

    @staticmethod
    def scratch(shape, nz):
        return [pltpu.VMEM(shape, F32), pltpu.VMEM(shape, F32), pltpu.VMEM((3,) + shape, F32),
                pltpu.VMEM(shape, F32), pltpu.VMEM((nz - 1,) + shape, F32), dma(3 + nz), dma(3 + nz)]

    def cross(self):
        return remote(self.source, self.twin_in, self.ss.at[0], self.rs.at[0], self.spot.twin())

    def hop(self, k):
        chip = (self.spot.first, self.spot.second, self.spot.diagonal)[k]
        return remote(self.pair, self.plane_in.at[k], self.ss.at[1 + k], self.rs.at[1 + k],
                      self.spot.at_chip(chip))

    def line(self, d):
        return remote(self.col, self.line_in.at[d - 1], self.ss.at[3 + d], self.rs.at[3 + d],
                      self.spot.on_line(d))

    def start(self):
        self.cross().start()

    def plane(self):
        self.cross().wait_recv()
        self.pair[...] = self.source[...] + self.twin_in[...]
        for k in range(3):
            self.hop(k).start()

    def column(self):
        for k in range(3):
            self.hop(k).wait_recv()
        self.col[...] = self.pair[...] + self.plane_in[0] + self.plane_in[1] + self.plane_in[2]
        for d in range(1, self.spot.nz):
            self.line(d).start()

    def total(self):
        out = self.col[...]
        for d in range(1, self.spot.nz):
            self.line(d).wait_recv()
        for d in range(self.spot.nz - 1):
            out = out + self.line_in[d]
        return out

    def drain(self):
        self.cross().wait_send()
        for k in range(3):
            self.hop(k).wait_send()
        for d in range(1, self.spot.nz):
            self.line(d).wait_send()


class Exchange:
    def __init__(self, spot, ss, rs):
        self.spot, self.ss, self.rs = spot, ss, rs

    def copies(self, source, target):
        spot = self.spot
        out = []
        for d in range(1, spot.nseq):
            s = modulo(spot.seq + d, spot.nseq)
            out.append(remote(source(s), target(d), self.ss.at[d - 1], self.rs.at[d - 1], (spot.z, s)))
        return out

    def spread(self, own, land):
        return self.copies(lambda s: own, lambda d: land.at[self.spot.seq])

    def collect(self, parts, land):
        return self.copies(lambda s: parts.at[s], lambda d: land.at[d - 1])


def begin(copies):
    for copy in copies:
        copy.start()


def complete(copies):
    for copy in copies:
        copy.wait()


def when(condition, *actions):
    @pl.when(condition)
    def _():
        for action in actions:
            action()


def does(method, *args):
    return lambda: method(*args)


def log2(value):
    assert value & (value - 1) == 0
    return value.bit_length() - 1


def row_picker(b, batch, spans, nseq):
    shape = (nseq * spans, nseq * batch * spans)
    r = lax.broadcasted_iota(jnp.int32, shape, 0)
    c = lax.broadcasted_iota(jnp.int32, shape, 1)
    shift = log2(spans)
    place_of = (r >> shift) * (batch * spans) + b * spans + (r & (spans - 1))
    return jnp.where(c == place_of, 1.0, 0.0).astype(BF16)


def span_adder(b, batch, spans, tokens):
    shape = (batch * spans, tokens)
    r = lax.broadcasted_iota(jnp.int32, shape, 0)
    t = lax.broadcasted_iota(jnp.int32, shape, 1)
    return jnp.where(r == b * spans + (t >> log2(SPAN)), 1.0, 0.0).astype(BF16)


def whole_weight(ref, cols):
    block = ref[:, :, :, cols]
    return block.reshape((-1, block.shape[-1]))


def enter_kernel(counts, *refs):
    batch, spans = counts
    (x_ref, bias_ref, gain_own, wq_sh, wo_sh, wu_sh, wd_sh,
     qkv_ref, sums_ref, prob_ref, o_ref, gains_ref, fq, fo, fu, fd, fq_next,
     qkv_all, own_acc, own_low, land, wq_in, wq_sem, ex_s, ex_r) = refs[:25]
    rest = refs[25:]
    spot = Spot()
    fetch = Fetch(spot, [wq_sh.at[0], wo_sh.at[0], wu_sh.at[0], wd_sh.at[0], wq_sh.at[1]],
                  [fq, fo, fu, fd, fq_next], rest[:7])
    adder = AllSum(spot, gain_own, rest[7:])
    exchange = Exchange(spot, ex_s, ex_r).spread(own_low, land)
    q0, o0, u0, d0, q1 = range(5)
    step = pl.program_id(0)
    tokens = x_ref.shape[1]

    @pl.when(step == 0)
    def _():
        spot.signal()
        own_acc[...] = jnp.zeros_like(own_acc)
        spot.meet()
        adder.start()
        for t in range(5):
            fetch.start(t)
        fetch.spread(q0)
        adder.plane()
        fetch.spread(o0)
        adder.column()
        fetch.relay(q0)
        gains_ref[...] = adder.total()
        fetch.share(q0)
        fetch.spread(u0)
        fetch.close(q0)
        fetch.relay(o0)
        fetch.finish(q0)
        copy = pltpu.make_async_copy(fq, wq_in, wq_sem)
        copy.start()
        copy.wait()

    when(step == 1, does(fetch.share, o0), does(fetch.spread, d0))
    when(step == 3, does(fetch.close, o0))
    when(step == 4, does(fetch.relay, u0), does(fetch.finish, o0))
    when(step == 5, does(fetch.share, u0))
    when(step == 6, does(fetch.spread, q1))

    @pl.when(step < batch)
    def _():
        unit, _ = normed(x_ref[0].astype(F32))
        n_one = (unit * gains_ref[0:1]).astype(BF16)
        pick = span_adder(step, batch, spans, tokens)
        for part in range(3):
            cols = slice(part * D, (part + 1) * D)
            block = dot(n_one, whole_weight(wq_in, cols)).astype(BF16)
            qkv_ref[0, :, cols] = block
            qkv_all[step, :, cols] = block
            if part > 0:
                own_acc[:, (part - 1) * D : part * D] += dot(pick, block)

    @pl.when(step == batch - 1)
    def _():
        own_low[...] = (own_acc[...] * (1.0 / SPAN)).astype(BF16)
        begin(exchange)
        land[spot.seq] = own_low[...]

    when(step == batch, does(complete, exchange))
    when(step == batch + 1, does(fetch.close, u0), does(fetch.relay, d0))
    when(step == batch + 2, does(fetch.share, d0))
    when(step == batch + 3, does(fetch.finish, u0))
    when(step == batch + 4, does(fetch.relay, q1))
    when(step == batch + 5, does(fetch.close, d0), does(fetch.share, q1))
    when(step == batch + 6, does(fetch.finish, d0))
    when(step == batch + 7, does(fetch.close, q1))

    @pl.when(step >= batch)
    def _():
        b = step - batch
        every = land[...].reshape((-1, land.shape[-1]))
        sums_ref[0] = dot(row_picker(b, batch, spans, spot.nseq), every).astype(BF16)
        attention_forward(qkv_all.at[pl.ds(b, 1)], sums_ref, bias_ref, prob_ref, o_ref)

    @pl.when(step == 2 * batch - 1)
    def _():
        fetch.finish(q1)
        for t in range(5):
            fetch.drain(t)
        adder.drain()


def phased(shape, start, count):
    rest = len(shape) - 1
    return pl.BlockSpec((1,) + tuple(shape[1:]),
                        lambda i: (jnp.clip(i - start, 0, count - 1),) + (0,) * rest)


def anywhere():
    return pl.BlockSpec(memory_space=pl.ANY)


def fused_params(collective_id):
    return pltpu.CompilerParams(dimension_semantics=("arbitrary",), vmem_limit_bytes=VMEM_LIMIT,
                                collective_id=collective_id, has_side_effects=True)


def full_shape(weights):
    return sds((lax.axis_size("dp"), lax.axis_size("seq")) + weights.shape[1:], weights.dtype)


def call_enter(x, bias, gain_own, wq, wo, wu, wd):
    batch, tokens, _ = x.shape
    spans = tokens // SPAN
    nz, nseq = lax.axis_size("dp"), lax.axis_size("seq")
    rows = batch * spans
    keys = SPAN + nseq * spans
    outs = [sds((batch, tokens, 3 * D), BF16), sds((batch, nseq * spans, 2 * D), BF16),
            sds((batch, spans, PAIRS, keys, 2 * SPAN), BF16), sds((batch, tokens, D), BF16),
            sds(gain_own.shape, F32)] + [full_shape(w) for w in (wq, wo, wu, wd, wq)]
    return pl.pallas_call(
        functools.partial(enter_kernel, (batch, spans)),
        grid=(2 * batch,),
        in_specs=[phased(x.shape, 0, batch), phased(bias.shape, batch, batch)]
        + [whole(a.shape) for a in (gain_own, wq, wo, wu, wd)],
        out_specs=[phased(outs[0].shape, 0, batch)] + [phased(o.shape, batch, batch) for o in outs[1:4]]
        + [whole(gain_own.shape)] + [anywhere()] * 5,
        out_shape=outs,
        scratch_shapes=[pltpu.VMEM((batch, tokens, 3 * D), BF16), pltpu.VMEM((rows, 2 * D), F32),
                        pltpu.VMEM((rows, 2 * D), BF16), pltpu.VMEM((nseq, rows, 2 * D), BF16),
                        pltpu.VMEM(outs[5].shape, BF16), pltpu.SemaphoreType.DMA, dma(nseq - 1), dma(nseq - 1)]
        + Fetch.scratch(5, nz) + AllSum.scratch(gain_own.shape, nz),
        compiler_params=fused_params(0),
        name="enter",
    )(x, bias, gain_own, wq, wo, wu, wd)


def mid_kernel(counts, *refs):
    batch, spans = counts
    (x_ref, o_ref, gains_ref, wo_ref, wu_ref, wd_ref, wq_ref, wo_sh, wu_sh, wd_sh,
     h_ref, u_ref, next_ref, qkv_ref, raw_ref, fo, fu, fd,
     own_acc, own_low, land, ex_s, ex_r) = refs[:23]
    spot = Spot()
    fetch = Fetch(spot, [wu_sh.at[1], wd_sh.at[1], wo_sh.at[1]], [fu, fd, fo], refs[23:])
    exchange = Exchange(spot, ex_s, ex_r).spread(own_low, land)
    u1, d1, o1 = range(3)
    step = pl.program_id(0)

    @pl.when(step == 0)
    def _():
        spot.signal()
        own_acc[...] = jnp.zeros_like(own_acc)

    hidden = x_ref[0].astype(F32) + dot(o_ref[0], wo_ref[...])
    h_ref[0] = hidden

    @pl.when(step == 0)
    def _():
        spot.meet()
        for t in range(3):
            fetch.start(t)

    when(step == 2, does(fetch.spread, u1))
    when(step == 3, does(fetch.spread, d1), does(fetch.spread, o1))
    when(step == 4, does(fetch.relay, u1), does(fetch.share, u1))
    when(step == 5, does(fetch.relay, d1), does(fetch.share, d1), does(fetch.relay, o1))
    when(step == 6, does(fetch.close, u1), does(fetch.share, o1))
    when(step == 7, does(fetch.close, d1), does(fetch.close, o1), does(fetch.finish, u1))

    result = mlp_forward(hidden, gains_ref[2:3], wu_ref, wd_ref, u_ref)
    next_ref[0] = result
    unit, _ = normed(result)
    n_one = (unit * gains_ref[1:2]).astype(BF16)
    pick = span_adder(step, batch, spans, x_ref.shape[1])
    for part in range(3):
        cols = slice(part * D, (part + 1) * D)
        block = dot(n_one, wq_ref[:, cols]).astype(BF16)
        qkv_ref[0, :, cols] = block
        if part > 0:
            own_acc[:, (part - 1) * D : part * D] += dot(pick, block)

    @pl.when(step == batch - 1)
    def _():
        own_low[...] = (own_acc[...] * (1.0 / SPAN)).astype(BF16)
        begin(exchange)
        land[spot.seq] = own_low[...]
        fetch.finish(d1)
        fetch.finish(o1)
        complete(exchange)
        raw_ref[...] = land[...]
        for t in range(3):
            fetch.drain(t)


def call_mid(x, o, gains, wo, wu, wd, wq_next, wo_sh, wu_sh, wd_sh):
    batch, tokens, _ = x.shape
    spans = tokens // SPAN
    nz, nseq = lax.axis_size("dp"), lax.axis_size("seq")
    rows = batch * spans
    outs = [sds((batch, tokens, D), F32), sds((batch, tokens, wu.shape[1]), BF16), sds((batch, tokens, D), F32),
            sds((batch, tokens, 3 * D), BF16), sds((nseq, rows, 2 * D), BF16)]
    outs += [full_shape(w) for w in (wo_sh, wu_sh, wd_sh)]
    args = [x, o, gains, wo, wu, wd, wq_next, wo_sh, wu_sh, wd_sh]
    return pl.pallas_call(
        functools.partial(mid_kernel, (batch, spans)),
        grid=(batch,),
        in_specs=[per_seq(a.shape) for a in args[:2]] + [whole(a.shape) for a in args[2:]],
        out_specs=[per_seq(a.shape) for a in outs[:4]] + [whole(outs[4].shape)] + [anywhere()] * 3,
        out_shape=outs,
        scratch_shapes=[pltpu.VMEM((rows, 2 * D), F32), pltpu.VMEM((rows, 2 * D), BF16),
                        pltpu.VMEM((nseq, rows, 2 * D), BF16), dma(nseq - 1), dma(nseq - 1)]
        + Fetch.scratch(3, nz),
        compiler_params=fused_params(1),
        name="mid",
    )(*args)


def top_kernel(counts, x_ref, qkv_ref, bias_ref, raw_ref, gains_ref, wo_ref, wu_ref, wd_ref,
               sums_ref, prob_ref, o_ref, h_ref, u_ref, next_ref):
    batch, spans, nseq = counts
    every = raw_ref[...].reshape((-1, raw_ref.shape[-1]))
    sums_ref[0] = dot(row_picker(pl.program_id(0), batch, spans, nseq), every).astype(BF16)
    attention_forward(qkv_ref, sums_ref, bias_ref, prob_ref, o_ref)
    hidden = x_ref[0] + dot(o_ref[0], wo_ref[...])
    h_ref[0] = hidden
    result = mlp_forward(hidden, gains_ref[3:4], wu_ref, wd_ref, u_ref)
    next_ref[0] = result.astype(next_ref.dtype)


def call_top(x, qkv, bias, raw, gains, wo, wu, wd):
    batch, tokens, _ = x.shape
    spans = tokens // SPAN
    nseq = raw.shape[0]
    outs = [sds((batch, nseq * spans, 2 * D), BF16),
            sds((batch, spans, PAIRS, SPAN + nseq * spans, 2 * SPAN), BF16), sds((batch, tokens, D), BF16),
            sds((batch, tokens, D), F32), sds((batch, tokens, wu.shape[1]), BF16), sds((batch, tokens, D), BF16)]
    args = [x, qkv, bias, raw, gains, wo, wu, wd]
    return pl.pallas_call(
        functools.partial(top_kernel, (batch, spans, nseq)),
        grid=(batch,),
        in_specs=[per_seq(a.shape) for a in args[:3]] + [whole(a.shape) for a in args[3:]],
        out_specs=[per_seq(a.shape) for a in outs],
        out_shape=outs,
        compiler_params=params(),
        name="top",
    )(*args)


def mlp_back(dy32, u_ref, h_ref, o_ref, gain, wo_ref, wu_ref, wd_ref, dh_ref, gd_ref, gu_ref, go_ref, gg_ref):
    ddown = dy32.astype(BF16)
    unit, rstd = normed(h_ref[0])
    n_two = (unit * gain).astype(BF16)
    dn_two = 0.0
    for start in range(0, wu_ref.shape[1], CHUNK):
        cols = slice(start, start + CHUNK)
        dactive = dot(ddown, wd_ref[cols, :], NT)
        active, slope = gelu_both(u_ref[0, :, cols].astype(F32))
        gd_ref[cols, :] += dot(active.astype(BF16), ddown, TN)
        dupper = (dactive * slope).astype(BF16)
        gu_ref[:, cols] += dot(n_two, dupper, TN)
        dn_two = dn_two + dot(dupper, wu_ref[:, cols], NT)
    dnorm, grad_gain = norm_backward(dn_two, unit, rstd, gain)
    gg_ref[...] += grad_gain
    dhidden = dy32 + dnorm
    dh_ref[0] = dhidden
    dattn = dhidden.astype(BF16)
    go_ref[...] += dot(o_ref[0], dattn, TN)
    return dot(dattn, wo_ref[...], NT).astype(BF16)


def pile(b, batch, spans, nseq, dsums_ref, part_acc):
    part_acc[...] += dot(row_picker(b, batch, spans, nseq), dsums_ref[0], TN)


def ship(spot, part_acc, part_low, copies):
    part_low[...] = part_acc[...].astype(BF16).reshape(part_low.shape)
    begin(copies)


def gathered(spot, part_low, land, copies):
    total = part_low[spot.seq].astype(F32)
    complete(copies)
    for d in range(spot.nseq - 1):
        total = total + land[d].astype(F32)
    return total


def zero(*refs):
    for ref in refs:
        ref[...] = jnp.zeros_like(ref)


def base_kernel(counts, *refs):
    batch, spans = counts
    (dy_ref, u_ref, h_ref, o_ref, prob_ref, qkv_ref, sums_ref, gains_ref, wo_ref, wu_ref, wd_ref,
     dh_ref, dqkv_ref, total_ref, gd_out, gu_out, go_out, gg_ref,
     gd_ref, gu_ref, go_ref, dsums, part_acc, part_low, land, ex_s, ex_r) = refs
    spot = Spot()
    exchange = Exchange(spot, ex_s, ex_r).collect(part_low, land)
    step = pl.program_id(0)

    @pl.when(step == 0)
    def _():
        spot.signal()
        zero(gd_ref, gu_ref, go_ref, gg_ref, part_acc)

    dout = mlp_back(dy_ref[0].astype(F32), u_ref, h_ref, o_ref, gains_ref[3:4], wo_ref, wu_ref, wd_ref,
                    dh_ref, gd_ref, gu_ref, go_ref, gg_ref)
    attention_backward(qkv_ref, sums_ref, prob_ref, dout, dqkv_ref, dsums)
    pile(step, batch, spans, spot.nseq, dsums, part_acc)

    @pl.when(step == batch - 1)
    def _():
        spot.meet()
        ship(spot, part_acc, part_low, exchange)
        gd_out[...] = gd_ref[...].astype(BF16)
        gu_out[...] = gu_ref[...].astype(BF16)
        go_out[...] = go_ref[...].astype(BF16)
        total_ref[...] = gathered(spot, part_low, land, exchange)


def call_base(dy, u, h, o, prob, qkv, sums, gains, wo, wu, wd):
    batch, tokens, _ = dy.shape
    spans = tokens // SPAN
    nseq = lax.axis_size("seq")
    rows = batch * spans
    args = [dy, u, h, o, prob, qkv, sums, gains, wo, wu, wd]
    outs = [sds(h.shape, F32), sds(qkv.shape, BF16), sds((rows, 2 * D), F32), sds(wd.shape, BF16),
            sds(wu.shape, BF16), sds(wo.shape, BF16), sds((1, D), F32)]
    return pl.pallas_call(
        functools.partial(base_kernel, (batch, spans)),
        grid=(batch,),
        in_specs=[per_seq(a.shape) for a in args[:7]] + [whole(a.shape) for a in args[7:]],
        out_specs=[per_seq(a.shape) for a in outs[:2]] + [whole(a.shape) for a in outs[2:]],
        out_shape=outs,
        scratch_shapes=[pltpu.VMEM(wd.shape, F32), pltpu.VMEM(wu.shape, F32), pltpu.VMEM(wo.shape, F32),
                        pltpu.VMEM((1, nseq * spans, 2 * D), BF16), pltpu.VMEM((nseq * rows, 2 * D), F32),
                        pltpu.VMEM((nseq, rows, 2 * D), BF16), pltpu.VMEM((nseq - 1, rows, 2 * D), BF16),
                        dma(nseq - 1), dma(nseq - 1)],
        compiler_params=fused_params(2),
        name="base",
    )(*args)


def qkv_back(x32, gain, near, share, dh, weight, gq_ref, gg_ref):
    unit, rstd = normed(x32)
    n_one = (unit * gain).astype(BF16)
    dn_one = 0.0
    for part in range(3):
        cols = slice(part * D, (part + 1) * D)
        block = near(cols)
        if part > 0:
            pieces = []
            for span in range(x32.shape[0] // SPAN):
                row = share(span, slice((part - 1) * D, part * D)) * (1.0 / SPAN)
                pieces.append(block[span * SPAN : (span + 1) * SPAN].astype(F32) + row)
            block = jnp.concatenate(pieces, 0).astype(BF16)
        gq_ref[:, cols] += dot(n_one, block, TN)
        dn_one = dn_one + dot(block, weight(cols), NT)
    dnorm, grad_gain = norm_backward(dn_one, unit, rstd, gain)
    gg_ref[...] += grad_gain
    return dh + dnorm


def turn_kernel(counts, *refs):
    batch, spans = counts
    (x_ref, near_ref, dh_ref, u_ref, h_ref, o_ref, total_ref, gains_ref, wq_ref, wo_ref, wu_ref, wd_ref,
     pd, pu, po,
     dh_out, dout_out, gd_out, gu_out, go_out, ggq_ref, gg_ref, sd, su, so, sq,
     dx_all, gq_ref, gd_ref, gu_ref, go_ref, gq_low) = refs[:32]
    rest = refs[32:]
    spot = Spot()
    fold = Fold(spot, [pd, pu, po, gq_low], [sd, su, so, sq], rest[:24], rest[24:])
    d1, u1, o1, q1 = range(4)
    step = pl.program_id(0)

    @pl.when(step == 0)
    def _():
        spot.signal()
        zero(gq_ref, gd_ref, gu_ref, go_ref, gg_ref, ggq_ref)
        spot.meet()
        for t in range(3):
            fold.start(t)

    when(step == 2, does(fold.combine, d1))
    when(step == 3, does(fold.combine, u1))
    when(step == 4, does(fold.combine, o1))
    when(step == 6, does(fold.middle, d1))

    @pl.when(step == batch)
    def _():
        gq_low[...] = gq_ref[...].astype(BF16).reshape(gq_low.shape)
        fold.start(q1)
        fold.middle(u1)

    when(step == batch + 1, does(fold.middle, o1), does(fold.column, d1), does(fold.combine, q1))
    when(step == batch + 2, does(fold.column, u1), does(fold.column, o1))
    when(step == batch + 3, does(fold.middle, q1), does(fold.finish, d1))
    when(step == batch + 4, does(fold.finish, u1), does(fold.finish, o1))
    when(step == batch + 5, does(fold.column, q1))
    when(step == batch + 7, does(fold.finish, q1))

    @pl.when(step < batch)
    def _():
        dx_all[step] = qkv_back(
            x_ref[0], gains_ref[1:2], lambda cols: near_ref[0, :, cols],
            lambda span, cols: total_ref[pl.ds(step * spans + span, 1), cols], dh_ref[0],
            lambda cols: wq_ref[:, cols], gq_ref, ggq_ref)

    @pl.when(step >= batch)
    def _():
        dout_out[0] = mlp_back(dx_all[step - batch], u_ref, h_ref, o_ref, gains_ref[2:3], wo_ref, wu_ref, wd_ref,
                               dh_out, gd_ref, gu_ref, go_ref, gg_ref)

    @pl.when(step == 2 * batch - 1)
    def _():
        gd_out[...] = gd_ref[...].astype(BF16)
        gu_out[...] = gu_ref[...].astype(BF16)
        go_out[...] = go_ref[...].astype(BF16)
        for t in range(4):
            fold.drain(t)


def by_owner(part):
    nz, nseq = lax.axis_size("dp"), lax.axis_size("seq")
    return part.reshape((nz, nseq // CORES, CORES, part.shape[0] // (nz * nseq)) + part.shape[1:])


def call_turn(x, near, dh, u, h, o, total, gains, wq, wo, wu, wd, pd, pu, po):
    batch, tokens, _ = x.shape
    nz = lax.axis_size("dp")
    parts = [by_owner(a) for a in (pd, pu, po)]
    owned = by_owner(sds_like(wq))
    shapes = [a.shape[3:] for a in parts] + [owned.shape[3:]]
    args = [x, near, dh, u, h, o, total, gains, wq, wo, wu, wd] + parts
    outs = [sds(h.shape, F32), sds(o.shape, BF16), sds(wd.shape, BF16), sds(wu.shape, BF16), sds(wo.shape, BF16),
            sds((1, D), F32), sds((1, D), F32)] + [sds(s, F32) for s in shapes]
    return pl.pallas_call(
        functools.partial(turn_kernel, (batch, tokens // SPAN)),
        grid=(2 * batch,),
        in_specs=[phased(a.shape, 0, batch) for a in args[:3]] + [phased(a.shape, batch, batch) for a in args[3:6]]
        + [whole(a.shape) for a in args[6:12]] + [anywhere()] * 3,
        out_specs=[phased(a.shape, batch, batch) for a in outs[:2]] + [whole(a.shape) for a in outs[2:]],
        out_shape=outs,
        scratch_shapes=[pltpu.VMEM(x.shape, F32), pltpu.VMEM(wq.shape, F32), pltpu.VMEM(wd.shape, F32),
                        pltpu.VMEM(wu.shape, F32), pltpu.VMEM(wo.shape, F32), pltpu.VMEM(owned.shape, BF16)]
        + Fold.buffers(shapes, nz) + Fold.sems(4, nz),
        compiler_params=fused_params(3),
        name="turn",
    )(*args)


def sds_like(a):
    class Shaped:
        shape = a.shape

        def reshape(self, shape):
            return sds(shape, a.dtype)

    return Shaped()


def leave_kernel(counts, *refs):
    batch, spans = counts
    (prob_ref, qkv_ref, sums_ref, dout_ref, x_ref, dh_ref, gains_ref, wq_ref, g_mlp0, g_attn1, g_mlp1,
     pd, pu, po,
     dx_ref, gsum_ref, sd, su, so, sq,
     near_all, gq_ref, gq_low, gg_ref, gain_src, dsums, part_acc, part_low, land, total, ex_s, ex_r) = refs[:32]
    rest = refs[32:]
    spot = Spot()
    fold = Fold(spot, [pd, pu, po, gq_low], [sd, su, so, sq], rest[:24], rest[24:31])
    adder = AllSum(spot, gain_src, rest[31:])
    exchange = Exchange(spot, ex_s, ex_r).collect(part_low, land)
    d0, u0, o0, q0 = range(4)
    step = pl.program_id(0)

    @pl.when(step == 0)
    def _():
        spot.signal()
        zero(gq_ref, gg_ref, part_acc)
        spot.meet()
        for t in range(3):
            fold.start(t)

    when(step == 2, does(fold.combine, d0))
    when(step == 3, does(fold.combine, u0))
    when(step == 4, does(fold.combine, o0))
    when(step == 6, does(fold.middle, d0))

    @pl.when(step == batch)
    def _():
        total[...] = gathered(spot, part_low, land, exchange)
        fold.middle(u0)
        fold.middle(o0)

    when(step == batch + 1, does(fold.column, d0))
    when(step == batch + 3, does(fold.column, u0), does(fold.column, o0))
    when(step == batch + 5, does(fold.finish, d0))
    when(step == batch + 6, does(fold.finish, u0), does(fold.finish, o0))

    @pl.when(step < batch)
    def _():
        attention_backward(qkv_ref, sums_ref, prob_ref, dout_ref[0], near_all.at[pl.ds(step, 1)], dsums)
        pile(step, batch, spans, spot.nseq, dsums, part_acc)

    when(step == batch - 1, does(ship, spot, part_acc, part_low, exchange))

    @pl.when(step >= batch)
    def _():
        b = step - batch
        dx_ref[0] = qkv_back(
            x_ref[0].astype(F32), gains_ref[0:1], lambda cols: near_all[b, :, cols],
            lambda span, cols: total[pl.ds(b * spans + span, 1), cols], dh_ref[0],
            lambda cols: wq_ref[:, cols], gq_ref, gg_ref)

    @pl.when(step == 2 * batch - 1)
    def _():
        gq_low[...] = gq_ref[...].astype(BF16).reshape(gq_low.shape)
        fold.start(q0)
        gain_src[...] = jnp.zeros_like(gain_src)
        gain_src[0:1] = gg_ref[...]
        gain_src[1:2] = g_attn1[...]
        gain_src[2:3] = g_mlp0[...]
        gain_src[3:4] = g_mlp1[...]
        adder.start()
        fold.combine(q0)
        adder.plane()
        fold.middle(q0)
        adder.column()
        fold.column(q0)
        gsum_ref[...] = adder.total()
        fold.finish(q0)
        for t in range(4):
            fold.drain(t)
        adder.drain()


def call_leave(prob, qkv, sums, dout, x, dh, gains, wq, g_mlp0, g_attn1, g_mlp1, pd, pu, po):
    batch, tokens, _ = x.shape
    spans = tokens // SPAN
    nz, nseq = lax.axis_size("dp"), lax.axis_size("seq")
    rows = batch * spans
    parts = [by_owner(a) for a in (pd, pu, po)]
    owned = by_owner(sds_like(wq))
    shapes = [a.shape[3:] for a in parts] + [owned.shape[3:]]
    args = [prob, qkv, sums, dout, x, dh, gains, wq, g_mlp0, g_attn1, g_mlp1] + parts
    outs = [sds(dh.shape, F32), sds(gains.shape, F32)] + [sds(s, F32) for s in shapes]
    return pl.pallas_call(
        functools.partial(leave_kernel, (batch, spans)),
        grid=(2 * batch,),
        in_specs=[phased(a.shape, 0, batch) for a in args[:4]] + [phased(a.shape, batch, batch) for a in args[4:6]]
        + [whole(a.shape) for a in args[6:11]] + [anywhere()] * 3,
        out_specs=[phased(outs[0].shape, batch, batch)] + [whole(a.shape) for a in outs[1:]],
        out_shape=outs,
        scratch_shapes=[pltpu.VMEM(qkv.shape, BF16), pltpu.VMEM(wq.shape, F32), pltpu.VMEM(owned.shape, BF16),
                        pltpu.VMEM((1, D), F32), pltpu.VMEM(gains.shape, F32),
                        pltpu.VMEM((1, nseq * spans, 2 * D), BF16), pltpu.VMEM((nseq * rows, 2 * D), F32),
                        pltpu.VMEM((nseq, rows, 2 * D), BF16), pltpu.VMEM((nseq - 1, rows, 2 * D), BF16),
                        pltpu.VMEM((rows, 2 * D), F32), dma(nseq - 1), dma(nseq - 1)]
        + Fold.buffers(shapes, nz) + Fold.sems(4, nz) + AllSum.scratch(gains.shape, nz),
        compiler_params=fused_params(4),
        name="leave",
    )(*args)


def pack_kernel(count, *refs):
    ins, outs = refs[: 2 * count], refs[2 * count :]
    for m in range(count):
        for l in range(2):
            outs[m][l] = ins[2 * m + l][...]


def call_pack(pairs):
    flat = [a for pair in pairs for a in pair]
    outs = [sds((2,) + pair[0].shape, F32) for pair in pairs]
    vmem = pl.BlockSpec(memory_space=pltpu.VMEM)
    return pl.pallas_call(
        functools.partial(pack_kernel, len(pairs)),
        in_specs=[vmem] * len(flat),
        out_specs=[vmem] * len(pairs),
        out_shape=outs,
        name="pack",
    )(*flat)


def fused(inputs, segments, w_qkv, w_out, w_up, w_down, gain_attn, gain_mlp, cotangent):
    stretch = inputs.shape[1]
    slots = gain_attn.shape[1]
    rank = lax.axis_index("dp") * lax.axis_size("seq") + lax.axis_index("seq")
    own = jnp.concatenate([gain_attn, gain_mlp], 0).astype(F32)
    own = jnp.pad(own, ((0, 4), (0, 0)))
    gain_own = lax.dynamic_update_slice(jnp.zeros((8, D), F32), own, (0, rank * slots))
    bias = mask_bias(segments, stretch)

    def flat(a):
        return a.reshape((-1, a.shape[-1]))

    qkv0, sums0, prob0, o0, gains, wq0, wo0, wu0, wd0, wq1 = call_enter(
        inputs, bias, gain_own, w_qkv, w_out, w_up, w_down)
    wq0, wo0, wu0, wd0, wq1 = (flat(a) for a in (wq0, wo0, wu0, wd0, wq1))
    h0, u0, x1, qkv1, raw1, wo1, wu1, wd1 = call_mid(
        inputs, o0, gains, wo0, wu0, wd0, wq1, w_out, w_up, w_down)
    wo1, wu1, wd1 = flat(wo1), flat(wu1), flat(wd1)
    sums1, prob1, o1, h1, u1, outputs = call_top(x1, qkv1, bias, raw1, gains, wo1, wu1, wd1)
    dh1, near1, total1, gd1, gu1, go1, g_mlp1 = call_base(
        cotangent, u1, h1, o1, prob1, qkv1, sums1, gains, wo1, wu1, wd1)
    dh0, dout0, gd0, gu0, go0, g_attn1, g_mlp0, sd1, su1, so1, sq1 = call_turn(
        x1, near1, dh1, u0, h0, o0, total1, gains, wq1, wo0, wu0, wd0, gd1, gu1, go1)
    dx, gsum, sd0, su0, so0, sq0 = call_leave(
        prob0, qkv0, sums0, dout0, inputs, dh0, gains, wq0, g_mlp0, g_attn1, g_mlp1, gd0, gu0, go0)
    gq, go, gu, gd = call_pack([(sq0, sq1), (so0, so1), (su0, su1), (sd0, sd1)])
    gain_share = lax.dynamic_slice(gsum, (0, rank * slots), (4, slots))
    return outputs, dx, gq, go, gu, gd, gain_share[:2], gain_share[2:]


def choose(*args):
    square = lax.axis_size("seq") == 4 * CORES
    if square and args[2].shape[1] % 16 == 0 and args[2].shape[0] == 2:
        return fused(*args)
    return on_device(*args)


def solution(mesh):
    weights = P(None, ("dp", "seq"), None)
    gains = P(None, ("dp", "seq"))
    rows = P("dp", "seq", None)
    return jax.shard_map(
        choose,
        mesh=mesh,
        in_specs=(rows, P("dp", None), weights, weights, weights, weights, gains, gains, rows),
        out_specs=(rows, rows, weights, weights, weights, weights, gains, gains),
        check_vma=False,
    )
```

```python
import functools

import jax
import jax.numpy as jnp
from jax import lax
from jax.experimental import pallas as pl
from jax.experimental.pallas import tpu as pltpu
from jax.sharding import PartitionSpec as P

D = 512
HEADS = 8
HEAD = 64
SPAN = 128
PAIRS = HEADS // 2
EPS = 1e-05
NEG = -1000000000.0
SCALE = HEAD ** (-0.5)
F32 = jnp.float32
BF16 = jnp.bfloat16
CHUNK = 512
VMEM_LIMIT = 60 * 1024 * 1024

NN = (((1,), (0,)), ((), ()))
NT = (((1,), (1,)), ((), ()))
TN = (((0,), (0,)), ((), ()))


def dot(left, right, dims=NN):
    return lax.dot_general(left, right, dims, preferred_element_type=F32)


def normed(values):
    mean = jnp.mean(values, -1, keepdims=True)
    centred = values - mean
    var = jnp.mean(centred * centred, -1, keepdims=True)
    rstd = lax.rsqrt(var + EPS)
    return centred * rstd, rstd


def norm_backward(dnorm, unit, rstd, gain):
    grad_gain = jnp.sum(dnorm * unit, 0, keepdims=True)
    scaled = dnorm * gain
    first = jnp.mean(scaled, -1, keepdims=True)
    second = jnp.mean(scaled * unit, -1, keepdims=True)
    return rstd * (scaled - first - unit * second), grad_gain


def project_qkv(x32, gain, wq_ref, qkv_ref, sums_ref):
    unit, _ = normed(x32)
    n_one = (unit * gain).astype(BF16)
    spans = x32.shape[0] // SPAN
    for part in range(3):
        block = dot(n_one, wq_ref[:, part * D : (part + 1) * D]).astype(BF16)
        qkv_ref[0, :, part * D : (part + 1) * D] = block
        if part > 0:
            wide = block.astype(F32)
            for span in range(spans):
                mean = jnp.sum(wide[span * SPAN : (span + 1) * SPAN], 0, keepdims=True) * (1.0 / SPAN)
                sums_ref[0, span : span + 1, (part - 1) * D : part * D] = mean.astype(BF16)


def lane_halves():
    lane = lax.broadcasted_iota(jnp.int32, (1, 2 * HEAD), 1)
    low = lane < HEAD
    return low


def head_stack(block, low, factor):
    one = jnp.where(low, factor, 0.0).astype(BF16)
    two = jnp.where(low, 0.0, factor).astype(BF16)
    return jnp.concatenate([block * one, block * two], 0)


def pair_operands(qkv_ref, sums_ref, span, pair):
    rows = slice(span * SPAN, (span + 1) * SPAN)
    lanes = slice(pair * 128, (pair + 1) * 128)
    keys = jnp.concatenate(
        [qkv_ref[0, rows, D + pair * 128 : D + (pair + 1) * 128], sums_ref[0, :, lanes]], 0
    )
    values = jnp.concatenate(
        [
            qkv_ref[0, rows, 2 * D + pair * 128 : 2 * D + (pair + 1) * 128],
            sums_ref[0, :, D + pair * 128 : D + (pair + 1) * 128],
        ],
        0,
    )
    query = qkv_ref[0, rows, lanes]
    return query, keys, values


def attention_forward(qkv_ref, sums_ref, bias_ref, prob_ref, o_ref):
    low = lane_halves()
    units = [(span, pair) for span in range(qkv_ref.shape[1] // SPAN) for pair in range(PAIRS)]
    for start in range(0, len(units), GROUP):
        group = units[start : start + GROUP]
        operands = [pair_operands(qkv_ref, sums_ref, span, pair) for span, pair in group]
        scores = []
        for (span, _), (query, keys, _) in zip(group, operands):
            bias = bias_ref[0, span]
            bias = jnp.concatenate([bias, bias], 1)
            scores.append(dot(keys, head_stack(query, low, SCALE), NT) + bias)
        exps = [jnp.exp(score - jnp.max(score, 0, keepdims=True)) for score in scores]
        probs = [(e * (1.0 / jnp.sum(e, 0, keepdims=True))).astype(BF16) for e in exps]
        both = [dot(prob, values, TN) for prob, (_, _, values) in zip(probs, operands)]
        for (span, pair), prob, out in zip(group, probs, both):
            prob_ref[0, span, pair] = prob
            o_ref[0, span * SPAN : (span + 1) * SPAN, pair * 128 : (pair + 1) * 128] = jnp.where(
                low, out[:SPAN], out[SPAN:]
            ).astype(BF16)


def attention_backward(qkv_ref, sums_ref, prob_ref, dout, dqkv_ref, dsums_ref):
    low = lane_halves()
    spans = qkv_ref.shape[1] // SPAN
    for start in range(0, PAIRS, BACK_GROUP):
        pairs = range(start, start + BACK_GROUP)
        units = [(span, pair) for pair in pairs for span in range(spans)]
        operands = [pair_operands(qkv_ref, sums_ref, span, pair) for span, pair in units]
        q_stacks = [head_stack(query, low, SCALE) for query, _, _ in operands]
        do_stacks = [
            head_stack(dout[span * SPAN : (span + 1) * SPAN, pair * 128 : (pair + 1) * 128], low, 1.0)
            for span, pair in units
        ]
        probs = [prob_ref[0, span, pair] for span, pair in units]
        dprobs = [dot(values, do_stack, NT) for (_, _, values), do_stack in zip(operands, do_stacks)]
        dvalues = [dot(prob, do_stack) for prob, do_stack in zip(probs, do_stacks)]
        dscores = []
        for prob, dprob in zip(probs, dprobs):
            wide = prob.astype(F32)
            product = wide * dprob
            dscores.append((product - wide * jnp.sum(product, 0, keepdims=True)).astype(BF16))
        dkeys = [dot(dscore, q_stack) for dscore, q_stack in zip(dscores, q_stacks)]
        dboths = [dot(dscore, keys, TN) for dscore, (_, keys, _) in zip(dscores, operands)]
        for (span, pair), dboth, dkey, dvalue in zip(units, dboths, dkeys, dvalues):
            rows = slice(span * SPAN, (span + 1) * SPAN)
            dquery = jnp.where(low, dboth[:SPAN], dboth[SPAN:]) * SCALE
            for part, block in enumerate((dquery, dkey[:SPAN], dvalue[:SPAN])):
                lanes = slice(part * D + pair * 128, part * D + (pair + 1) * 128)
                dqkv_ref[0, rows, lanes] = block.astype(BF16)
        for at, pair in enumerate(pairs):
            mine = range(at * spans, (at + 1) * spans)
            dksum = sum(dkeys[i][SPAN:] for i in mine)
            dvsum = sum(dvalues[i][SPAN:] for i in mine)
            dsums_ref[0, :, pair * 128 : (pair + 1) * 128] = dksum.astype(BF16)
            dsums_ref[0, :, D + pair * 128 : D + (pair + 1) * 128] = dvsum.astype(BF16)


GROUP = 8
BACK_GROUP = 4
G0 = 0.7978845608
G1 = 0.7978845608 * 0.044715


def gelu(values):
    squared = values * values
    slope = jnp.tanh(values * (G0 + G1 * squared))
    half = 0.5 * values
    return half + half * slope


def gelu_both(values):
    squared = values * values
    slope = jnp.tanh(values * (G0 + G1 * squared))
    half = 0.5 * values
    rise = 0.5 + 0.5 * slope
    inner = G0 + (3.0 * G1) * squared
    return values * rise, rise + half * (1.0 - slope * slope) * inner


def mlp_forward(h32, gain, wu_ref, wd_ref, u_ref):
    unit, _ = normed(h32)
    n_two = (unit * gain).astype(BF16)
    total = h32
    for start in range(0, wu_ref.shape[1], CHUNK):
        upper = dot(n_two, wu_ref[:, start : start + CHUNK])
        u_ref[0, :, start : start + CHUNK] = upper.astype(BF16)
        total = total + dot(gelu(upper).astype(BF16), wd_ref[start : start + CHUNK, :])
    return total


def first_kernel(x_ref, gain_ref, wq_ref, qkv_ref, sums_ref):
    project_qkv(x_ref[0].astype(F32), gain_ref[...], wq_ref, qkv_ref, sums_ref)


def layer_kernel(last, *refs):
    if last:
        (x_ref, qkv_ref, sums_ref, bias_ref, gain_ref, wo_ref, wu_ref, wd_ref,
         prob_ref, o_ref, h_ref, u_ref, next_ref) = refs
    else:
        (x_ref, qkv_ref, sums_ref, bias_ref, gain_ref, wo_ref, wu_ref, wd_ref, gain_next_ref, wq_ref,
         prob_ref, o_ref, h_ref, u_ref, next_ref, qkv_next_ref, sums_next_ref) = refs
    attention_forward(qkv_ref, sums_ref, bias_ref, prob_ref, o_ref)
    hidden = x_ref[0].astype(F32) + dot(o_ref[0], wo_ref[...])
    h_ref[0] = hidden
    result = mlp_forward(hidden, gain_ref[...], wu_ref, wd_ref, u_ref)
    next_ref[0] = result.astype(next_ref.dtype)
    if not last:
        project_qkv(result, gain_next_ref[...], wq_ref, qkv_next_ref, sums_next_ref)


def accumulate(ref, index, value, first):
    @pl.when(first)
    def _():
        ref[index] = value

    @pl.when(jnp.logical_not(first))
    def _():
        ref[index] = ref[index] + value


def mlp_attention_backward(dy32, u_ref, h_ref, o_ref, prob_ref, qkv_ref, sums_ref, gain_ref,
                           wo_ref, wu_ref, wd_ref, dh_ref, dqkv_ref, dsums_ref, gd_ref, gu_ref,
                           go_ref, gg_ref):
    ddown = dy32.astype(BF16)
    unit, rstd = normed(h_ref[0])
    n_two = (unit * gain_ref[...]).astype(BF16)
    dn_two = 0.0
    for start in range(0, wu_ref.shape[1], CHUNK):
        cols = slice(start, start + CHUNK)
        dactive = dot(ddown, wd_ref[cols, :], NT)
        active, slope = gelu_both(u_ref[0, :, cols].astype(F32))
        gd_ref[cols, :] += dot(active.astype(BF16), ddown, TN)
        dupper = (dactive * slope).astype(BF16)
        gu_ref[:, cols] += dot(n_two, dupper, TN)
        dn_two = dn_two + dot(dupper, wu_ref[:, cols], NT)
    dnorm, grad_gain = norm_backward(dn_two, unit, rstd, gain_ref[...])
    gg_ref[...] += grad_gain
    dhidden = dy32 + dnorm
    dh_ref[0] = dhidden
    dattn = dhidden.astype(BF16)
    go_ref[...] += dot(o_ref[0], dattn, TN)
    dout = dot(dattn, wo_ref[...], NT).astype(BF16)
    attention_backward(qkv_ref, sums_ref, prob_ref, dout, dqkv_ref, dsums_ref)


def back_kernel(dy_ref, u_ref, h_ref, o_ref, prob_ref, qkv_ref, sums_ref, gain_ref,
                wo_ref, wu_ref, wd_ref, dh_ref, dqkv_ref, dsums_ref, gd_out, gu_out, go_out,
                gg_ref, gd_ref, gu_ref, go_ref):
    step = pl.program_id(0)

    @pl.when(step == 0)
    def _():
        gd_ref[...] = jnp.zeros_like(gd_ref)
        gu_ref[...] = jnp.zeros_like(gu_ref)
        go_ref[...] = jnp.zeros_like(go_ref)
        gg_ref[...] = jnp.zeros_like(gg_ref)

    mlp_attention_backward(dy_ref[0].astype(F32), u_ref, h_ref, o_ref, prob_ref, qkv_ref, sums_ref,
                           gain_ref, wo_ref, wu_ref, wd_ref, dh_ref, dqkv_ref, dsums_ref, gd_ref,
                           gu_ref, go_ref, gg_ref)

    @pl.when(step == pl.num_programs(0) - 1)
    def _():
        gd_out[...] = gd_ref[...].astype(BF16)
        gu_out[...] = gu_ref[...].astype(BF16)
        go_out[...] = go_ref[...].astype(BF16)


def qkv_backward(x32, gain, near_ref, dsums_ref, dh, wq_ref, gq_ref, gg_ref):
    unit, rstd = normed(x32)
    n_one = (unit * gain).astype(BF16)
    dn_one = 0.0
    tokens = x32.shape[0]
    for part in range(3):
        cols = slice(part * D, (part + 1) * D)
        block = near_ref[0, :, cols]
        if part > 0:
            pieces = []
            for span in range(tokens // SPAN):
                share = dsums_ref[0, span : span + 1, (part - 1) * D : part * D].astype(F32) * (1.0 / SPAN)
                pieces.append(block[span * SPAN : (span + 1) * SPAN].astype(F32) + share)
            block = jnp.concatenate(pieces, 0).astype(BF16)
        gq_ref[:, cols] += dot(n_one, block, TN)
        dn_one = dn_one + dot(block, wq_ref[:, cols], NT)
    dnorm, grad_gain = norm_backward(dn_one, unit, rstd, gain)
    gg_ref[...] += grad_gain
    return dh + dnorm


def last_kernel(x_ref, gain_ref, near_ref, dsums_ref, dh_ref, wq_ref, dx_ref, gq_out, gg_ref, gq_ref):
    step = pl.program_id(0)

    @pl.when(step == 0)
    def _():
        gq_ref[...] = jnp.zeros_like(gq_ref)
        gg_ref[...] = jnp.zeros_like(gg_ref)

    dx_ref[0] = qkv_backward(x_ref[0].astype(F32), gain_ref[...], near_ref, dsums_ref, dh_ref[0], wq_ref,
                             gq_ref, gg_ref)

    @pl.when(step == pl.num_programs(0) - 1)
    def _():
        gq_out[...] = gq_ref[...].astype(BF16)


def per_seq(shape):
    rest = len(shape) - 1
    return pl.BlockSpec((1,) + tuple(shape[1:]), lambda b: (b,) + (0,) * rest)


def whole(shape):
    rank = len(shape)
    return pl.BlockSpec(tuple(shape), lambda b: (0,) * rank, pipeline_mode=pl.Buffered(1))


def sds(shape, dtype):
    return jax.ShapeDtypeStruct(tuple(shape), dtype)


def params():
    return pltpu.CompilerParams(dimension_semantics=("arbitrary",), vmem_limit_bytes=VMEM_LIMIT)


def call_first(x, gain, wq):
    batch, tokens, _ = x.shape
    spans = tokens // SPAN
    outs = (sds((batch, tokens, 3 * D), BF16), sds((batch, spans, 2 * D), BF16))
    return pl.pallas_call(
        first_kernel,
        grid=(batch,),
        in_specs=[per_seq(x.shape), whole(gain.shape), whole(wq.shape)],
        out_specs=[per_seq(o.shape) for o in outs],
        out_shape=outs,
        compiler_params=params(),
        name="first",
    )(x, gain, wq)


def call_layer(x, qkv, sums, bias, gain, wo, wu, wd, gain_next=None, wq=None):
    batch, tokens, _ = x.shape
    spans = tokens // SPAN
    last = wq is None
    keys = SPAN + sums.shape[1]
    outs = [
        sds((batch, spans, PAIRS, keys, 2 * SPAN), BF16),
        sds((batch, tokens, D), BF16),
        sds((batch, tokens, D), F32),
        sds((batch, tokens, wu.shape[1]), BF16),
        sds((batch, tokens, D), BF16 if last else F32),
    ]
    args = [x, qkv, sums, bias, gain, wo, wu, wd]
    if not last:
        outs += [sds((batch, tokens, 3 * D), BF16), sds((batch, spans, 2 * D), BF16)]
        args += [gain_next, wq]
    specs = [per_seq(a.shape) for a in args[:4]] + [whole(a.shape) for a in args[4:]]
    return pl.pallas_call(
        functools.partial(layer_kernel, last),
        grid=(batch,),
        in_specs=specs,
        out_specs=[per_seq(o.shape) for o in outs],
        out_shape=outs,
        compiler_params=params(),
        name="layer",
    )(*args)


def call_back(dy, u, h, o, prob, qkv, sums, gain, wo, wu, wd):
    batch, tokens, _ = dy.shape
    args = [dy, u, h, o, prob, qkv, sums, gain, wo, wu, wd]
    specs = [per_seq(a.shape) for a in args[:7]] + [whole(a.shape) for a in args[7:]]
    outs = [sds(h.shape, F32), sds(qkv.shape, BF16), sds(sums.shape, BF16),
            sds(wd.shape, BF16), sds(wu.shape, BF16), sds(wo.shape, BF16), sds((1, D), F32)]
    return pl.pallas_call(
        back_kernel,
        grid=(batch,),
        in_specs=specs,
        out_specs=[per_seq(o.shape) for o in outs[:3]] + [whole(o.shape) for o in outs[3:]],
        out_shape=outs,
        scratch_shapes=[pltpu.VMEM(wd.shape, F32), pltpu.VMEM(wu.shape, F32), pltpu.VMEM(wo.shape, F32)],
        compiler_params=params(),
        name="back",
    )(*args)


def call_last(x, gain, near, dsums, dh, wq):
    batch, tokens, _ = x.shape
    outs = [sds((batch, tokens, D), F32), sds(wq.shape, BF16), sds((1, D), F32)]
    return pl.pallas_call(
        last_kernel,
        grid=(batch,),
        in_specs=[per_seq(x.shape), whole(gain.shape), per_seq(near.shape), per_seq(dsums.shape),
                  per_seq(dh.shape), whole(wq.shape)],
        out_specs=[per_seq(outs[0].shape), whole(outs[1].shape), whole(outs[2].shape)],
        out_shape=outs,
        scratch_shapes=[pltpu.VMEM(wq.shape, F32)],
        compiler_params=params(),
        name="last",
    )(x, gain, near, dsums, dh, wq)


def mask_bias(segments, stretch):
    batch, length = segments.shape
    rank = lax.axis_index("seq")
    own = lax.dynamic_slice_in_dim(segments, rank * stretch, stretch, 1).reshape(batch, -1, SPAN)
    ends = segments.reshape(batch, -1, SPAN)[:, :, SPAN - 1]
    spans = own.shape[1]
    pos = jnp.arange(SPAN)
    near = (own[:, :, :, None] == own[:, :, None, :]) & (pos[:, None] <= pos[None, :])
    ids = rank * spans + jnp.arange(spans)
    before = jnp.arange(ends.shape[1])[None, :] < ids[:, None]
    far = (ends[:, None, :, None] == own[:, :, None, :]) & before[None, :, :, None]
    return jnp.where(jnp.concatenate([near, far], 2), 0.0, NEG).astype(F32)

MESH = pl.DeviceIdType.MESH
CORES = 2


def place():
    nz, nseq = lax.axis_size("dp"), lax.axis_size("seq")
    z, s = lax.axis_index("dp"), lax.axis_index("seq")
    return nz, nseq // CORES, z, s // CORES, lax.rem(s, CORES)


def modulo(value, size):
    return lax.rem(value + size, size)


def peers_of():
    nz, nchip, z, chip, core = place()
    seq = chip * CORES + core
    out = [(modulo(z + d, nz), seq) for d in range(1, nz)]
    out += [(z, modulo(chip + d, nchip) * CORES + core) for d in range(1, nchip)]
    out.append((z, chip * CORES + 1 - core))
    return out


def greet(peers):
    barrier = pltpu.get_barrier_semaphore()
    for peer in peers:
        pl.semaphore_signal(barrier, inc=1, device_id=peer, device_id_type=MESH)
    pl.semaphore_wait(barrier, len(peers))


def remote(src, dst, send, recv, peer):
    return pltpu.make_async_remote_copy(
        src_ref=src, dst_ref=dst, send_sem=send, recv_sem=recv, device_id=peer, device_id_type=MESH
    )


class Gather:
    def __init__(self, shards, fulls, sems):
        self.shards, self.fulls = shards, fulls
        self.own, self.zs, self.zr, self.ps, self.pr, self.cs, self.cr = sems
        self.nz, self.nchip, self.z, self.chip, self.core = place()
        self.seq = self.chip * CORES + self.core

    @staticmethod
    def scratch(count):
        nz, nchip = lax.axis_size("dp"), lax.axis_size("seq") // CORES
        dma = pltpu.SemaphoreType.DMA
        return [dma((count,)), dma((count, nz - 1)), dma((count, nz - 1)), dma((count, nchip - 1)),
                dma((count, nchip - 1)), dma((count, nchip)), dma((count, nchip))]

    def local(self, t):
        return pltpu.make_async_copy(self.shards[t], self.fulls[t].at[self.z, self.seq], self.own.at[t])

    def line(self, t, d):
        peer = (modulo(self.z + d, self.nz), self.seq)
        return remote(self.shards[t], self.fulls[t].at[self.z, self.seq], self.zs.at[t, d - 1],
                      self.zr.at[t, d - 1], peer)

    def plane(self, t, d):
        block = self.fulls[t].at[:, self.seq]
        peer = (self.z, modulo(self.chip + d, self.nchip) * CORES + self.core)
        return remote(block, block, self.ps.at[t, d - 1], self.pr.at[t, d - 1], peer)

    def cross(self, t, d):
        block = self.fulls[t].at[:, modulo(self.chip - d, self.nchip) * CORES + self.core]
        peer = (self.z, self.chip * CORES + 1 - self.core)
        return remote(block, block, self.cs.at[t, d], self.cr.at[t, d], peer)

    def start(self, t):
        self.local(t).start()
        for d in range(1, self.nz):
            self.line(t, d).start()

    def spread(self, t):
        self.local(t).wait()
        for d in range(1, self.nz):
            self.line(t, d).wait_recv()
        for d in range(1, self.nchip):
            self.plane(t, d).start()
        self.cross(t, 0).start()

    def share(self, t):
        for d in range(1, self.nchip):
            self.plane(t, d).wait_recv()
            self.cross(t, d).start()

    def finish(self, t):
        for d in range(self.nchip):
            self.cross(t, d).wait_recv()

    def drain(self, t):
        for d in range(1, self.nz):
            self.line(t, d).wait_send()
        for d in range(1, self.nchip):
            self.plane(t, d).wait_send()
        for d in range(self.nchip):
            self.cross(t, d).wait_send()


def gather_kernel(count, *refs):
    work = Gather(refs[:count], refs[count : 2 * count], refs[2 * count :])
    greet(peers_of())
    for stage in (work.start, work.spread, work.share, work.finish, work.drain):
        for t in range(count):
            stage(t)


def call_gather(shards, collective_id):
    nz, nseq = lax.axis_size("dp"), lax.axis_size("seq")
    count = len(shards)
    outs = [sds((nz, nseq) + a.shape, a.dtype) for a in shards]
    return pl.pallas_call(
        functools.partial(gather_kernel, count),
        in_specs=[pl.BlockSpec(memory_space=pltpu.VMEM)] * count,
        out_specs=[pl.BlockSpec(memory_space=pl.ANY)] * count,
        out_shape=outs,
        scratch_shapes=Gather.scratch(count),
        compiler_params=pltpu.CompilerParams(
            collective_id=collective_id, has_side_effects=True, vmem_limit_bytes=VMEM_LIMIT
        ),
        name="gather",
    )(*shards)


class Reduce:
    def __init__(self, parts, outs, bufs, sems):
        self.parts, self.outs = parts, outs
        count = len(parts)
        self.mine, self.cross_in, self.plane_in, self.col, self.line_in = (
            bufs[i * count : (i + 1) * count] for i in range(5)
        )
        self.own, self.cs, self.cr, self.ps, self.pr, self.zs, self.zr = sems
        self.nz, self.nchip, self.z, self.chip, self.core = place()
        self.seq = self.chip * CORES + self.core

    @staticmethod
    def scratch(parts):
        nz, nchip = lax.axis_size("dp"), lax.axis_size("seq") // CORES
        dma = pltpu.SemaphoreType.DMA
        count = len(parts)
        bufs = []
        for lead in ((nchip, nz), (nchip, nz), (nchip - 1, nz), (nz,), (nz - 1,)):
            bufs += [pltpu.VMEM(lead + a.shape[3:], a.dtype) for a in parts]
        return bufs + [dma((count, nchip)), dma((count, nchip)), dma((count, nchip)), dma((count, nchip - 1)),
                       dma((count, nchip - 1)), dma((count, nz - 1)), dma((count, nz - 1))]

    def local(self, t, d):
        chip = modulo(self.chip + d, self.nchip)
        return pltpu.make_async_copy(self.parts[t].at[:, chip, self.core], self.mine[t].at[d], self.own.at[t, d])

    def cross(self, t, d):
        chip = modulo(self.chip + d, self.nchip)
        peer = (self.z, self.chip * CORES + 1 - self.core)
        return remote(self.parts[t].at[:, chip, 1 - self.core], self.cross_in[t].at[d], self.cs.at[t, d],
                      self.cr.at[t, d], peer)

    def plane(self, t, d):
        peer = (self.z, modulo(self.chip + d, self.nchip) * CORES + self.core)
        return remote(self.mine[t].at[d], self.plane_in[t].at[d - 1], self.ps.at[t, d - 1],
                      self.pr.at[t, d - 1], peer)

    def line(self, t, d):
        z = modulo(self.z + d, self.nz)
        return remote(self.col[t].at[z], self.line_in[t].at[d - 1], self.zs.at[t, d - 1],
                      self.zr.at[t, d - 1], (z, self.seq))

    def order(self):
        return list(range(1, self.nchip)) + [0]

    def start(self, t):
        for d in self.order():
            self.cross(t, d).start()
            self.local(t, d).start()

    def combine(self, t):
        for d in self.order():
            self.local(t, d).wait()
            self.cross(t, d).wait_recv()

            def add(i, carry):
                total = self.mine[t][d, i].astype(F32) + self.cross_in[t][d, i].astype(F32)
                self.mine[t][d, i] = total.astype(self.mine[t].dtype)
                return carry

            lax.fori_loop(0, self.nz, add, 0)
            if d > 0:
                self.plane(t, d).start()

    def column(self, t):
        for d in range(1, self.nchip):
            self.plane(t, d).wait_recv()

        def add(i, carry):
            total = self.mine[t][0, i].astype(F32)
            for d in range(self.nchip - 1):
                total = total + self.plane_in[t][d, i].astype(F32)
            self.col[t][i] = total.astype(self.col[t].dtype)
            return carry

        lax.fori_loop(0, self.nz, add, 0)
        for d in range(1, self.nz):
            self.line(t, d).start()

    def finish(self, t):
        total = self.col[t][self.z].astype(F32)
        for d in range(1, self.nz):
            self.line(t, d).wait_recv()
        for d in range(self.nz - 1):
            total = total + self.line_in[t][d].astype(F32)
        self.outs[t][...] = total

    def drain(self, t):
        for d in self.order():
            self.cross(t, d).wait_send()
        for d in range(1, self.nchip):
            self.plane(t, d).wait_send()
        for d in range(1, self.nz):
            self.line(t, d).wait_send()


def reduce_kernel(count, *refs):
    work = Reduce(refs[:count], refs[count : 2 * count], refs[2 * count : 7 * count], refs[7 * count :])
    greet(peers_of())
    for stage in (work.start, work.combine, work.column, work.finish, work.drain):
        for t in range(count):
            stage(t)


def call_reduce(parts, collective_id):
    nz, nseq = lax.axis_size("dp"), lax.axis_size("seq")
    count = len(parts)
    parts = [a.reshape((nz, nseq // CORES, CORES, a.shape[0] // (nz * nseq)) + a.shape[1:]) for a in parts]
    outs = [sds(a.shape[3:], F32) for a in parts]
    return pl.pallas_call(
        functools.partial(reduce_kernel, count),
        in_specs=[pl.BlockSpec(memory_space=pl.ANY)] * count,
        out_specs=[pl.BlockSpec(memory_space=pltpu.VMEM)] * count,
        out_shape=outs,
        scratch_shapes=Reduce.scratch(parts),
        compiler_params=pltpu.CompilerParams(
            collective_id=collective_id, has_side_effects=True, vmem_limit_bytes=VMEM_LIMIT
        ),
        name="reduce",
    )(*parts)


def seq_peers():
    nseq = lax.axis_size("seq")
    z, s = lax.axis_index("dp"), lax.axis_index("seq")
    return [(d, (z, modulo(s + d, nseq))) for d in range(1, nseq)]


def spread_kernel(own_ref, all_ref, send, recv):
    s = lax.axis_index("seq")
    peers = seq_peers()
    greet([peer for _, peer in peers])
    copies = [remote(own_ref, all_ref.at[s], send.at[d - 1], recv.at[d - 1], peer) for d, peer in peers]
    for copy in copies:
        copy.start()
    all_ref[s] = own_ref[...]
    for copy in copies:
        copy.wait()


def call_spread(own, collective_id):
    nseq = lax.axis_size("seq")
    return pl.pallas_call(
        spread_kernel,
        in_specs=[pl.BlockSpec(memory_space=pltpu.VMEM)],
        out_specs=pl.BlockSpec(memory_space=pltpu.VMEM),
        out_shape=sds((nseq,) + own.shape, own.dtype),
        scratch_shapes=[pltpu.SemaphoreType.DMA((nseq - 1,)),
                        pltpu.SemaphoreType.DMA((nseq - 1,))],
        compiler_params=pltpu.CompilerParams(
            collective_id=collective_id, has_side_effects=True, vmem_limit_bytes=VMEM_LIMIT
        ),
        name="spread",
    )(own)


def collect_kernel(part_ref, out_ref, slots, send, recv):
    s = lax.axis_index("seq")
    nseq = lax.axis_size("seq")
    peers = seq_peers()
    greet([peer for _, peer in peers])
    copies = [remote(part_ref.at[modulo(s + d, nseq)], slots.at[d - 1], send.at[d - 1], recv.at[d - 1], peer)
              for d, peer in peers]
    for copy in copies:
        copy.start()
    total = part_ref[s].astype(F32)
    for d, _ in peers:
        copies[d - 1].wait()
    for d in range(nseq - 1):
        total = total + slots[d].astype(F32)
    out_ref[...] = total


def call_collect(part, collective_id):
    nseq = part.shape[0]
    return pl.pallas_call(
        collect_kernel,
        in_specs=[pl.BlockSpec(memory_space=pltpu.VMEM)],
        out_specs=pl.BlockSpec(memory_space=pltpu.VMEM),
        out_shape=sds(part.shape[1:], F32),
        scratch_shapes=[pltpu.VMEM((nseq - 1,) + part.shape[1:], part.dtype),
                        pltpu.SemaphoreType.DMA((nseq - 1,)), pltpu.SemaphoreType.DMA((nseq - 1,))],
        compiler_params=pltpu.CompilerParams(
            collective_id=collective_id, has_side_effects=True, vmem_limit_bytes=VMEM_LIMIT
        ),
        name="collect",
    )(part)


def on_device(inputs, segments, w_qkv, w_out, w_up, w_down, gain_attn, gain_mlp, cotangent):
    layers = w_qkv.shape[0]
    batch, stretch, _ = inputs.shape
    nz, nseq = lax.axis_size("dp"), lax.axis_size("seq")
    spans = stretch // SPAN
    slots = gain_attn.shape[1]
    gain_shard = jnp.pad(
        jnp.concatenate([gain_attn, gain_mlp], 0).astype(F32), ((0, 8 - 2 * layers), (0, 128 - slots))
    )
    shards = []
    for l in range(layers):
        shards += [w_qkv[l], w_out[l], w_up[l], w_down[l]]
    fulls = call_gather(shards + [gain_shard], 0)
    gains = fulls[-1][:, :, : 2 * layers, :slots].transpose(2, 0, 1, 3).reshape(2 * layers, D)
    g_one = [gains[l : l + 1] for l in range(layers)]
    g_two = [gains[layers + l : layers + l + 1] for l in range(layers)]
    flat = [a.reshape((-1, a.shape[-1])) for a in fulls[:-1]]
    wq, wo, wu, wd = (flat[m::4] for m in range(4))
    bias = mask_bias(segments, stretch)

    def spread(sums, index):
        return call_spread(sums, index).transpose(1, 0, 2, 3).reshape(batch, nseq * spans, 2 * D)

    def collect(dsums, index):
        return call_collect(dsums.reshape(batch, nseq, spans, 2 * D).transpose(1, 0, 2, 3), index)

    x = inputs
    qkv, own = call_first(x, g_one[0], wq[0])
    kept = []
    for l in range(layers):
        sums = spread(own, 1)
        if l + 1 < layers:
            prob, o, h, u, x_next, qkv_next, own = call_layer(
                x, qkv, sums, bias, g_two[l], wo[l], wu[l], wd[l], g_one[l + 1], wq[l + 1]
            )
        else:
            prob, o, h, u, x_next = call_layer(x, qkv, sums, bias, g_two[l], wo[l], wu[l], wd[l])
            qkv_next = None
        kept.append((x, qkv, sums, prob, o, h, u))
        x, qkv = x_next, qkv_next
    outputs = x
    dy = cotangent
    grads = [None] * layers
    for l in reversed(range(layers)):
        x, qkv, sums, prob, o, h, u = kept[l]
        dh, near, dsums, gd, gu, go, gg_two = call_back(
            dy, u, h, o, prob, qkv, sums, g_two[l], wo[l], wu[l], wd[l]
        )
        dy, gq, gg_one = call_last(x, g_one[l], near, collect(dsums, 2), dh, wq[l])
        grads[l] = (gq, go, gu, gd, gg_one, gg_two)
    gain_grads = jnp.concatenate([grads[l][4] for l in range(layers)] + [grads[l][5] for l in range(layers)], 0)
    gain_grads = jnp.pad(
        gain_grads.reshape(2 * layers, nz * nseq, slots).transpose(1, 0, 2),
        ((0, 0), (0, 8 - 2 * layers), (0, 128 - slots)),
    ).reshape(-1, 128)
    parts = []
    for l in range(layers):
        parts += list(grads[l][:4])
    shares = call_reduce(parts + [gain_grads], 3)
    stacked = [jnp.stack(shares[m : 4 * layers : 4]) for m in range(4)]
    gain_share = shares[-1][: 2 * layers, :slots]
    return (outputs, dy, *stacked, gain_share[:layers], gain_share[layers:])


class Spot:
    def __init__(self):
        self.nz, self.nseq = lax.axis_size("dp"), lax.axis_size("seq")
        self.z, self.seq = lax.axis_index("dp"), lax.axis_index("seq")
        self.chip, self.core = lax.div(self.seq, CORES), lax.rem(self.seq, CORES)
        row, col = lax.div(self.chip, 2), lax.rem(self.chip, 2)
        across, along = row * 2 + 1 - col, (1 - row) * 2 + col
        self.first = (1 - self.core) * across + self.core * along
        self.second = (1 - self.core) * along + self.core * across
        self.diagonal = (1 - row) * 2 + 1 - col

    def at_chip(self, chip):
        return (self.z, chip * CORES + self.core)

    def twin(self):
        return (self.z, self.chip * CORES + 1 - self.core)

    def on_line(self, d):
        return (modulo(self.z + d, self.nz), self.seq)

    def signal(self):
        barrier = pltpu.get_barrier_semaphore()
        for peer in self.peers():
            pl.semaphore_signal(barrier, inc=1, device_id=peer, device_id_type=MESH)

    def meet(self):
        pl.semaphore_wait(pltpu.get_barrier_semaphore(), len(self.peers()))

    def peers(self):
        out = [self.on_line(d) for d in range(1, self.nz)]
        return out + [(self.z, modulo(self.seq + d, self.nseq)) for d in range(1, self.nseq)]


def dma(*shape):
    return pltpu.SemaphoreType.DMA(shape)


class Fetch:
    def __init__(self, spot, shards, fulls, sems):
        self.spot, self.shards, self.fulls = spot, shards, fulls
        self.own, self.zs, self.zr, self.hs, self.hr, self.cs, self.cr = sems

    @staticmethod
    def scratch(count, nz):
        return [dma(count), dma(count, nz - 1), dma(count, nz - 1), dma(count, 3), dma(count, 3),
                dma(count, 4), dma(count, 4)]

    def local(self, t):
        return pltpu.make_async_copy(
            self.shards[t], self.fulls[t].at[self.spot.z, self.spot.seq], self.own.at[t])

    def line(self, t, d):
        return remote(self.shards[t], self.fulls[t].at[self.spot.z, self.spot.seq], self.zs.at[t, d - 1],
                      self.zr.at[t, d - 1], self.spot.on_line(d))

    def hop(self, t, k):
        spot = self.spot
        chip = (spot.chip, spot.chip, spot.first)[k]
        target = (spot.first, spot.second, spot.second)[k]
        block = self.fulls[t].at[:, chip * CORES + spot.core]
        return remote(block, block, self.hs.at[t, k], self.hr.at[t, k], spot.at_chip(target))

    def cross(self, t, k):
        spot = self.spot
        chip = (spot.chip, spot.first, spot.second, spot.diagonal)[k]
        block = self.fulls[t].at[:, chip * CORES + spot.core]
        return remote(block, block, self.cs.at[t, k], self.cr.at[t, k], spot.twin())

    def start(self, t):
        self.local(t).start()
        for d in range(1, self.spot.nz):
            self.line(t, d).start()

    def spread(self, t):
        self.local(t).wait()
        for d in range(1, self.spot.nz):
            self.line(t, d).wait_recv()
        self.hop(t, 0).start()
        self.hop(t, 1).start()
        self.cross(t, 0).start()

    def relay(self, t):
        self.hop(t, 0).wait_recv()
        self.hop(t, 2).start()
        self.cross(t, 1).start()

    def share(self, t):
        self.hop(t, 1).wait_recv()
        self.cross(t, 2).start()

    def close(self, t):
        self.hop(t, 2).wait_recv()
        self.cross(t, 3).start()

    def finish(self, t):
        for k in range(4):
            self.cross(t, k).wait_recv()

    def drain(self, t):
        for d in range(1, self.spot.nz):
            self.line(t, d).wait_send()
        for k in range(3):
            self.hop(t, k).wait_send()
        for k in range(4):
            self.cross(t, k).wait_send()


class Fold:
    def __init__(self, spot, parts, outs, bufs, sems):
        self.spot, self.parts, self.outs = spot, parts, outs
        count = len(parts)
        self.mine, self.twin_in, self.first_in, self.second_in, self.col, self.line_in = (
            bufs[i * count : (i + 1) * count] for i in range(6)
        )
        self.own, self.cs, self.cr, self.hs, self.hr, self.zs, self.zr = sems

    @staticmethod
    def buffers(shapes, nz):
        out = []
        for lead in ((4, nz), (4, nz), (2, nz), (nz,), (nz,), (nz - 1,)):
            out += [pltpu.VMEM(lead + tuple(shape), BF16) for shape in shapes]
        return out

    @staticmethod
    def sems(count, nz):
        return [dma(count, 4), dma(count, 4), dma(count, 4), dma(count, 3), dma(count, 3),
                dma(count, nz - 1), dma(count, nz - 1)]

    def local(self, t, k):
        spot = self.spot
        chip = (spot.chip, spot.first, spot.second, spot.diagonal)[k]
        return pltpu.make_async_copy(self.parts[t].at[:, chip, spot.core], self.mine[t].at[k], self.own.at[t, k])

    def cross(self, t, k):
        spot = self.spot
        chip = (spot.chip, spot.second, spot.first, spot.diagonal)[k]
        return remote(self.parts[t].at[:, chip, 1 - spot.core], self.twin_in[t].at[k], self.cs.at[t, k],
                      self.cr.at[t, k], spot.twin())

    def hop(self, t, k):
        spot = self.spot
        source = self.mine[t].at[(1, 3, 2)[k]]
        target = (self.first_in[t].at[0], self.first_in[t].at[1], self.second_in[t])[k]
        chip = (spot.first, spot.first, spot.second)[k]
        return remote(source, target, self.hs.at[t, k], self.hr.at[t, k], spot.at_chip(chip))

    def line(self, t, d):
        z = modulo(self.spot.z + d, self.spot.nz)
        return remote(self.col[t].at[z], self.line_in[t].at[d - 1], self.zs.at[t, d - 1], self.zr.at[t, d - 1],
                      self.spot.on_line(d))

    def start(self, t):
        for k in (3, 1, 2, 0):
            self.cross(t, k).start()
            self.local(t, k).start()

    def combine(self, t):
        mine, twin_in = self.mine[t], self.twin_in[t]
        for k in (3, 1, 2, 0):
            self.local(t, k).wait()
            self.cross(t, k).wait_recv()

            def add(i, carry):
                mine[k, i] = mine[k, i] + twin_in[k, i]
                return carry

            lax.fori_loop(0, self.spot.nz, add, 0)
            if k == 3:
                self.hop(t, 1).start()
            elif k == 1:
                self.hop(t, 0).start()

    def middle(self, t):
        mine, first_in = self.mine[t], self.first_in[t]
        self.hop(t, 1).wait_recv()

        def add(i, carry):
            mine[2, i] = mine[2, i] + first_in[1, i]
            return carry

        lax.fori_loop(0, self.spot.nz, add, 0)
        self.hop(t, 2).start()

    def column(self, t):
        mine, first_in, second_in, col = self.mine[t], self.first_in[t], self.second_in[t], self.col[t]
        self.hop(t, 0).wait_recv()
        self.hop(t, 2).wait_recv()

        def add(i, carry):
            total = mine[0, i].astype(F32) + first_in[0, i].astype(F32) + second_in[i].astype(F32)
            col[i] = total.astype(BF16)
            return carry

        lax.fori_loop(0, self.spot.nz, add, 0)
        for d in range(1, self.spot.nz):
            self.line(t, d).start()

    def finish(self, t):
        total = self.col[t][self.spot.z].astype(F32)
        for d in range(1, self.spot.nz):
            self.line(t, d).wait_recv()
        for d in range(self.spot.nz - 1):
            total = total + self.line_in[t][d].astype(F32)
        self.outs[t][...] = total

    def drain(self, t):
        for k in range(4):
            self.cross(t, k).wait_send()
        for k in range(3):
            self.hop(t, k).wait_send()
        for d in range(1, self.spot.nz):
            self.line(t, d).wait_send()


class AllSum:
    def __init__(self, spot, source, bufs):
        self.spot, self.source = spot, source
        self.twin_in, self.pair, self.plane_in, self.col, self.line_in, self.ss, self.rs = bufs

    @staticmethod
    def scratch(shape, nz):
        return [pltpu.VMEM(shape, F32), pltpu.VMEM(shape, F32), pltpu.VMEM((3,) + shape, F32),
                pltpu.VMEM(shape, F32), pltpu.VMEM((nz - 1,) + shape, F32), dma(3 + nz), dma(3 + nz)]

    def cross(self):
        return remote(self.source, self.twin_in, self.ss.at[0], self.rs.at[0], self.spot.twin())

    def hop(self, k):
        chip = (self.spot.first, self.spot.second, self.spot.diagonal)[k]
        return remote(self.pair, self.plane_in.at[k], self.ss.at[1 + k], self.rs.at[1 + k],
                      self.spot.at_chip(chip))

    def line(self, d):
        return remote(self.col, self.line_in.at[d - 1], self.ss.at[3 + d], self.rs.at[3 + d],
                      self.spot.on_line(d))

    def start(self):
        self.cross().start()

    def plane(self):
        self.cross().wait_recv()
        self.pair[...] = self.source[...] + self.twin_in[...]
        for k in range(3):
            self.hop(k).start()

    def column(self):
        for k in range(3):
            self.hop(k).wait_recv()
        self.col[...] = self.pair[...] + self.plane_in[0] + self.plane_in[1] + self.plane_in[2]
        for d in range(1, self.spot.nz):
            self.line(d).start()

    def total(self):
        out = self.col[...]
        for d in range(1, self.spot.nz):
            self.line(d).wait_recv()
        for d in range(self.spot.nz - 1):
            out = out + self.line_in[d]
        return out

    def drain(self):
        self.cross().wait_send()
        for k in range(3):
            self.hop(k).wait_send()
        for d in range(1, self.spot.nz):
            self.line(d).wait_send()


HALVES = 2


class Exchange:
    def __init__(self, spot, sources, lands, ss, rs):
        self.spot, self.sources, self.lands, self.ss, self.rs = spot, sources, lands, ss, rs

    @staticmethod
    def sems(nseq):
        return [dma(HALVES, nseq - 1), dma(HALVES, nseq - 1)]

    def copies(self, h, source, target):
        spot = self.spot
        out = []
        for d in range(1, spot.nseq):
            s = modulo(spot.seq + d, spot.nseq)
            out.append(remote(source(s), target(d), self.ss.at[h, d - 1], self.rs.at[h, d - 1], (spot.z, s)))
        return out

    def spread(self, h):
        return self.copies(h, lambda s: self.sources[h], lambda d: self.lands[h].at[self.spot.seq])

    def collect(self, h):
        return self.copies(h, lambda s: self.sources[h].at[s], lambda d: self.lands[h].at[d - 1])


def begin(copies):
    for copy in copies:
        copy.start()


def complete(copies):
    for copy in copies:
        copy.wait()


def when(condition, *actions):
    @pl.when(condition)
    def _():
        for action in actions:
            action()


def does(method, *args):
    return lambda: method(*args)


def log2(value):
    assert value & (value - 1) == 0
    return value.bit_length() - 1


def row_picker(b, batch, spans, nseq):
    shape = (nseq * spans, nseq * batch * spans)
    r = lax.broadcasted_iota(jnp.int32, shape, 0)
    c = lax.broadcasted_iota(jnp.int32, shape, 1)
    shift = log2(spans)
    place_of = (r >> shift) * (batch * spans) + b * spans + (r & (spans - 1))
    return jnp.where(c == place_of, 1.0, 0.0).astype(BF16)


def span_adder(b, batch, spans, tokens):
    shape = (batch * spans, tokens)
    r = lax.broadcasted_iota(jnp.int32, shape, 0)
    t = lax.broadcasted_iota(jnp.int32, shape, 1)
    return jnp.where(r == b * spans + (t >> log2(SPAN)), 1.0, 0.0).astype(BF16)


def whole_weight(ref, cols):
    block = ref[:, :, :, cols]
    return block.reshape((-1, block.shape[-1]))


def send_means(exchange, h, own_acc):
    rows = own_acc.shape[0] // HALVES
    exchange.sources[h][...] = (own_acc[h * rows : (h + 1) * rows] * (1.0 / SPAN)).astype(BF16)
    begin(exchange.spread(h))
    exchange.lands[h][exchange.spot.seq] = exchange.sources[h][...]


def pick_sums(b, counts, nseq, land):
    batch, spans = counts
    every = land.reshape((-1, land.shape[-1]))
    return dot(row_picker(b, batch // HALVES, spans, nseq), every).astype(BF16)


def enter_kernel(counts, *refs):
    batch, spans = counts
    (x_ref, bias_ref, gain_own, wq_sh, wo_sh, wu_sh, wd_sh,
     qkv_ref, sums_ref, prob_ref, o_ref, gains_ref, fq, fo, fu, fd,
     qkv_all, own_acc, own_a, own_b, land_a, land_b, wq_in, wq_sem, ex_s, ex_r) = refs[:26]
    rest = refs[26:]
    spot = Spot()
    fetch = Fetch(spot, [wq_sh.at[0], wo_sh.at[0], wu_sh.at[0], wd_sh.at[0]], [fq, fo, fu, fd], rest[:7])
    adder = AllSum(spot, gain_own, rest[7:])
    exchange = Exchange(spot, [own_a, own_b], [land_a, land_b], ex_s, ex_r)
    q0, o0, u0, d0 = range(4)
    step = pl.program_id(0)
    tokens = x_ref.shape[1]
    half = batch // HALVES

    @pl.when(step == 0)
    def _():
        spot.signal()
        own_acc[...] = jnp.zeros_like(own_acc)
        spot.meet()
        adder.start()
        for t in range(4):
            fetch.start(t)
        fetch.spread(q0)
        adder.plane()
        fetch.spread(o0)
        adder.column()
        fetch.relay(q0)
        gains_ref[...] = adder.total()
        fetch.share(q0)
        fetch.spread(u0)
        fetch.close(q0)
        fetch.relay(o0)
        fetch.finish(q0)
        copy = pltpu.make_async_copy(fq, wq_in, wq_sem)
        copy.start()
        copy.wait()

    when(step == 1, does(fetch.share, o0))
    when(step == 2, does(fetch.relay, u0), does(fetch.share, u0))
    when(step == 3, does(fetch.close, o0))

    @pl.when(step < batch)
    def _():
        unit, _ = normed(x_ref[0].astype(F32))
        n_one = (unit * gains_ref[0:1]).astype(BF16)
        pick = span_adder(step, batch, spans, tokens)
        for part in range(3):
            cols = slice(part * D, (part + 1) * D)
            block = dot(n_one, whole_weight(wq_in, cols)).astype(BF16)
            qkv_ref[0, :, cols] = block
            qkv_all[step, :, cols] = block
            if part > 0:
                own_acc[:, (part - 1) * D : part * D] += dot(pick, block)

    when(step == half - 1, does(send_means, exchange, 0, own_acc))
    when(step == half, does(fetch.spread, d0))
    when(step == half + 1, does(fetch.close, u0))
    when(step == batch - 1, does(send_means, exchange, 1, own_acc))

    @pl.when(step == batch)
    def _():
        complete(exchange.spread(0))
        fetch.finish(o0)
        fetch.finish(u0)

    when(step == batch + half - 1, does(fetch.relay, d0), does(fetch.share, d0))

    @pl.when(step == batch + half)
    def _():
        complete(exchange.spread(1))

    when(step == 2 * batch - 2, does(fetch.close, d0))

    @pl.when(jnp.logical_and(step >= batch, step < batch + half))
    def _():
        sums_ref[0] = pick_sums(step - batch, counts, spot.nseq, land_a[...])

    @pl.when(step >= batch + half)
    def _():
        sums_ref[0] = pick_sums(step - batch - half, counts, spot.nseq, land_b[...])

    @pl.when(step >= batch)
    def _():
        attention_forward(qkv_all.at[pl.ds(step - batch, 1)], sums_ref, bias_ref, prob_ref, o_ref)

    @pl.when(step == 2 * batch - 1)
    def _():
        fetch.finish(d0)
        for t in range(4):
            fetch.drain(t)
        adder.drain()


def phased(shape, start, count):
    rest = len(shape) - 1
    return pl.BlockSpec((1,) + tuple(shape[1:]),
                        lambda i: (jnp.clip(i - start, 0, count - 1),) + (0,) * rest)


def anywhere():
    return pl.BlockSpec(memory_space=pl.ANY)


def fused_params(collective_id):
    return pltpu.CompilerParams(dimension_semantics=("arbitrary",), vmem_limit_bytes=VMEM_LIMIT,
                                collective_id=collective_id, has_side_effects=True)


def full_shape(weights):
    return sds((lax.axis_size("dp"), lax.axis_size("seq")) + weights.shape[1:], weights.dtype)


def exchange_buffers(nseq, rows):
    own = pltpu.VMEM((rows // HALVES, 2 * D), BF16)
    land = pltpu.VMEM((nseq, rows // HALVES, 2 * D), BF16)
    return [own, own, land, land]


def call_enter(x, bias, gain_own, wq, wo, wu, wd):
    batch, tokens, _ = x.shape
    spans = tokens // SPAN
    nz, nseq = lax.axis_size("dp"), lax.axis_size("seq")
    rows = batch * spans
    keys = SPAN + nseq * spans
    outs = [sds((batch, tokens, 3 * D), BF16), sds((batch, nseq * spans, 2 * D), BF16),
            sds((batch, spans, PAIRS, keys, 2 * SPAN), BF16), sds((batch, tokens, D), BF16),
            sds(gain_own.shape, F32)] + [full_shape(w) for w in (wq, wo, wu, wd)]
    return pl.pallas_call(
        functools.partial(enter_kernel, (batch, spans)),
        grid=(2 * batch,),
        in_specs=[phased(x.shape, 0, batch), phased(bias.shape, batch, batch)]
        + [whole(a.shape) for a in (gain_own, wq, wo, wu, wd)],
        out_specs=[phased(outs[0].shape, 0, batch)] + [phased(o.shape, batch, batch) for o in outs[1:4]]
        + [whole(gain_own.shape)] + [anywhere()] * 4,
        out_shape=outs,
        scratch_shapes=[pltpu.VMEM((batch, tokens, 3 * D), BF16), pltpu.VMEM((rows, 2 * D), F32)]
        + exchange_buffers(nseq, rows)
        + [pltpu.VMEM(outs[5].shape, BF16), pltpu.SemaphoreType.DMA] + Exchange.sems(nseq)
        + Fetch.scratch(4, nz) + AllSum.scratch(gain_own.shape, nz),
        compiler_params=fused_params(0),
        name="enter",
    )(x, bias, gain_own, wq, wo, wu, wd)


def mid_kernel(counts, *refs):
    batch, spans = counts
    (x_ref, o_ref, gains_ref, wo_ref, wu_ref, wd_ref, wq_sh, wo_sh, wu_sh, wd_sh,
     h_ref, u_ref, next_ref, qkv_ref, raw_ref, fq, fo, fu, fd,
     next_all, own_acc, own_a, own_b, land_a, land_b, wq_in, wq_sem, ex_s, ex_r) = refs[:29]
    spot = Spot()
    fetch = Fetch(spot, [wq_sh.at[1], wu_sh.at[1], wd_sh.at[1], wo_sh.at[1]], [fq, fu, fd, fo], refs[29:])
    exchange = Exchange(spot, [own_a, own_b], [land_a, land_b], ex_s, ex_r)
    q1, u1, d1, o1 = range(4)
    step = pl.program_id(0)

    @pl.when(step == 0)
    def _():
        spot.signal()
        own_acc[...] = jnp.zeros_like(own_acc)

    @pl.when(step < batch)
    def _():
        hidden = x_ref[0].astype(F32) + dot(o_ref[0], wo_ref[...])
        h_ref[0] = hidden

        @pl.when(step == 0)
        def _():
            spot.meet()
            for t in range(4):
                fetch.start(t)

        when(step == 2, does(fetch.spread, q1))
        when(step == 4, does(fetch.relay, q1), does(fetch.share, q1), does(fetch.spread, u1))
        when(step == 5, does(fetch.close, q1))
        when(step == 6, does(fetch.spread, d1))
        when(step == 7, does(fetch.relay, u1), does(fetch.share, u1), does(fetch.spread, o1), does(fetch.finish, q1))
        result = mlp_forward(hidden, gains_ref[2:3], wu_ref, wd_ref, u_ref)
        next_ref[0] = result
        next_all[step] = result

    @pl.when(step == batch)
    def _():
        copy = pltpu.make_async_copy(fq, wq_in, wq_sem)
        copy.start()
        copy.wait()

    when(step == batch + 2, does(fetch.close, u1), does(fetch.relay, d1), does(fetch.share, d1))
    when(step == batch + 4, does(fetch.relay, o1), does(fetch.share, o1), does(fetch.close, d1))
    when(step == batch + 6, does(fetch.close, o1), does(fetch.finish, u1))
    when(step == batch + 7, does(fetch.finish, d1))

    @pl.when(step >= batch)
    def _():
        unit, _ = normed(next_all[step - batch])
        n_one = (unit * gains_ref[1:2]).astype(BF16)
        pick = span_adder(step - batch, batch, spans, x_ref.shape[1])
        for part in (1, 2, 0):
            cols = slice(part * D, (part + 1) * D)
            block = dot(n_one, whole_weight(wq_in, cols)).astype(BF16)
            qkv_ref[0, :, cols] = block
            if part > 0:
                own_acc[:, (part - 1) * D : part * D] += dot(pick, block)

    when(step == batch + batch // HALVES - 1, does(send_means, exchange, 0, own_acc))

    @pl.when(step == 2 * batch - 1)
    def _():
        send_means(exchange, 1, own_acc)
        fetch.finish(o1)
        for t in range(4):
            fetch.drain(t)
        complete(exchange.spread(0))
        raw_ref[0] = land_a[...]
        complete(exchange.spread(1))
        raw_ref[1] = land_b[...]


def call_mid(x, o, gains, wo, wu, wd, wq_sh, wo_sh, wu_sh, wd_sh):
    batch, tokens, _ = x.shape
    spans = tokens // SPAN
    nz, nseq = lax.axis_size("dp"), lax.axis_size("seq")
    rows = batch * spans
    outs = [sds((batch, tokens, D), F32), sds((batch, tokens, wu.shape[1]), BF16), sds((batch, tokens, D), F32),
            sds((batch, tokens, 3 * D), BF16), sds((HALVES, nseq, rows // HALVES, 2 * D), BF16)]
    outs += [full_shape(w) for w in (wq_sh, wo_sh, wu_sh, wd_sh)]
    args = [x, o, gains, wo, wu, wd, wq_sh, wo_sh, wu_sh, wd_sh]
    return pl.pallas_call(
        functools.partial(mid_kernel, (batch, spans)),
        grid=(2 * batch,),
        in_specs=[phased(a.shape, 0, batch) for a in args[:2]] + [whole(a.shape) for a in args[2:]],
        out_specs=[phased(a.shape, 0, batch) for a in outs[:3]] + [phased(outs[3].shape, batch, batch)]
        + [whole(outs[4].shape)] + [anywhere()] * 4,
        out_shape=outs,
        scratch_shapes=[pltpu.VMEM(x.shape, F32), pltpu.VMEM((rows, 2 * D), F32)] + exchange_buffers(nseq, rows)
        + [pltpu.VMEM(outs[5].shape, BF16), pltpu.SemaphoreType.DMA] + Exchange.sems(nseq)
        + Fetch.scratch(4, nz),
        compiler_params=fused_params(1),
        name="mid",
    )(*args)


def top_kernel(counts, x_ref, qkv_ref, bias_ref, raw_ref, gains_ref, wo_ref, wu_ref, wd_ref,
               sums_ref, prob_ref, o_ref, h_ref, u_ref, next_ref):
    batch, spans, nseq = counts
    b, half = pl.program_id(0), batch // HALVES
    sums_ref[0] = pick_sums(lax.rem(b, half), (batch, spans), nseq, raw_ref[lax.div(b, half)])
    attention_forward(qkv_ref, sums_ref, bias_ref, prob_ref, o_ref)
    hidden = x_ref[0] + dot(o_ref[0], wo_ref[...])
    h_ref[0] = hidden
    result = mlp_forward(hidden, gains_ref[3:4], wu_ref, wd_ref, u_ref)
    next_ref[0] = result.astype(next_ref.dtype)


def call_top(x, qkv, bias, raw, gains, wo, wu, wd):
    batch, tokens, _ = x.shape
    spans = tokens // SPAN
    nseq = raw.shape[1]
    outs = [sds((batch, nseq * spans, 2 * D), BF16),
            sds((batch, spans, PAIRS, SPAN + nseq * spans, 2 * SPAN), BF16), sds((batch, tokens, D), BF16),
            sds((batch, tokens, D), F32), sds((batch, tokens, wu.shape[1]), BF16), sds((batch, tokens, D), BF16)]
    args = [x, qkv, bias, raw, gains, wo, wu, wd]
    return pl.pallas_call(
        functools.partial(top_kernel, (batch, spans, nseq)),
        grid=(batch,),
        in_specs=[per_seq(a.shape) for a in args[:3]] + [whole(a.shape) for a in args[3:]],
        out_specs=[per_seq(a.shape) for a in outs],
        out_shape=outs,
        compiler_params=params(),
        name="top",
    )(*args)


def mlp_back(dy32, u_ref, h_ref, o_ref, gain, wo_ref, wu_ref, wd_ref, dh_ref, gd_ref, gu_ref, go_ref, gg_ref):
    ddown = dy32.astype(BF16)
    unit, rstd = normed(h_ref[0])
    n_two = (unit * gain).astype(BF16)
    dn_two = 0.0
    for start in range(0, wu_ref.shape[1], CHUNK):
        cols = slice(start, start + CHUNK)
        dactive = dot(ddown, wd_ref[cols, :], NT)
        active, slope = gelu_both(u_ref[0, :, cols].astype(F32))
        gd_ref[cols, :] += dot(active.astype(BF16), ddown, TN)
        dupper = (dactive * slope).astype(BF16)
        gu_ref[:, cols] += dot(n_two, dupper, TN)
        dn_two = dn_two + dot(dupper, wu_ref[:, cols], NT)
    dnorm, grad_gain = norm_backward(dn_two, unit, rstd, gain)
    gg_ref[...] += grad_gain
    dhidden = dy32 + dnorm
    dh_ref[0] = dhidden
    dattn = dhidden.astype(BF16)
    go_ref[...] += dot(o_ref[0], dattn, TN)
    return dot(dattn, wo_ref[...], NT).astype(BF16)


def pile(b, counts, nseq, dsums_ref, part_acc):
    batch, spans = counts
    local = lax.rem(b, batch // HALVES)
    part_acc[...] += dot(row_picker(local, batch // HALVES, spans, nseq), dsums_ref[0], TN)


def ship(exchange, h, part_acc):
    source = exchange.sources[h]
    source[...] = part_acc[...].astype(BF16).reshape(source.shape)
    part_acc[...] = jnp.zeros_like(part_acc)
    begin(exchange.collect(h))


def gathered(exchange, h, total_ref):
    spot = exchange.spot
    complete(exchange.collect(h))
    total = exchange.sources[h][spot.seq].astype(F32)
    for d in range(spot.nseq - 1):
        total = total + exchange.lands[h][d].astype(F32)
    rows = total.shape[0]
    total_ref[h * rows : (h + 1) * rows] = total


def collect_buffers(nseq, rows):
    part = pltpu.VMEM((nseq, rows // HALVES, 2 * D), BF16)
    land = pltpu.VMEM((nseq - 1, rows // HALVES, 2 * D), BF16)
    return [pltpu.VMEM((nseq * rows // HALVES, 2 * D), F32), part, part, land, land]


def zero(*refs):
    for ref in refs:
        ref[...] = jnp.zeros_like(ref)


def base_kernel(counts, *refs):
    batch, spans = counts
    (dy_ref, u_ref, h_ref, o_ref, prob_ref, qkv_ref, sums_ref, gains_ref, wo_ref, wu_ref, wd_ref,
     dh_ref, dqkv_ref, total_ref, gd_out, gu_out, go_out, gg_ref,
     gd_ref, gu_ref, go_ref, dsums, part_acc, part_a, part_b, land_a, land_b, ex_s, ex_r) = refs
    spot = Spot()
    exchange = Exchange(spot, [part_a, part_b], [land_a, land_b], ex_s, ex_r)
    step = pl.program_id(0)

    @pl.when(step == 0)
    def _():
        spot.signal()
        zero(gd_ref, gu_ref, go_ref, gg_ref, part_acc)

    dout = mlp_back(dy_ref[0].astype(F32), u_ref, h_ref, o_ref, gains_ref[3:4], wo_ref, wu_ref, wd_ref,
                    dh_ref, gd_ref, gu_ref, go_ref, gg_ref)
    attention_backward(qkv_ref, sums_ref, prob_ref, dout, dqkv_ref, dsums)
    pile(step, counts, spot.nseq, dsums, part_acc)

    @pl.when(step == batch // HALVES - 1)
    def _():
        spot.meet()
        ship(exchange, 0, part_acc)

    @pl.when(step == batch - 1)
    def _():
        ship(exchange, 1, part_acc)
        gd_out[...] = gd_ref[...].astype(BF16)
        gu_out[...] = gu_ref[...].astype(BF16)
        go_out[...] = go_ref[...].astype(BF16)
        gathered(exchange, 0, total_ref)
        gathered(exchange, 1, total_ref)


def call_base(dy, u, h, o, prob, qkv, sums, gains, wo, wu, wd):
    batch, tokens, _ = dy.shape
    spans = tokens // SPAN
    nseq = lax.axis_size("seq")
    rows = batch * spans
    args = [dy, u, h, o, prob, qkv, sums, gains, wo, wu, wd]
    outs = [sds(h.shape, F32), sds(qkv.shape, BF16), sds((rows, 2 * D), F32), sds(wd.shape, BF16),
            sds(wu.shape, BF16), sds(wo.shape, BF16), sds((1, D), F32)]
    return pl.pallas_call(
        functools.partial(base_kernel, (batch, spans)),
        grid=(batch,),
        in_specs=[per_seq(a.shape) for a in args[:7]] + [whole(a.shape) for a in args[7:]],
        out_specs=[per_seq(a.shape) for a in outs[:2]] + [whole(a.shape) for a in outs[2:]],
        out_shape=outs,
        scratch_shapes=[pltpu.VMEM(wd.shape, F32), pltpu.VMEM(wu.shape, F32), pltpu.VMEM(wo.shape, F32),
                        pltpu.VMEM((1, nseq * spans, 2 * D), BF16)]
        + collect_buffers(nseq, rows) + Exchange.sems(nseq),
        compiler_params=fused_params(2),
        name="base",
    )(*args)


def qkv_back(unit, rstd, gain, near, share, dh, weight, gq, gg_ref, skip=()):
    n_one = (unit * gain).astype(BF16)
    dn_one = 0.0
    for part in range(3):
        cols = slice(part * D, (part + 1) * D)
        block = near(cols)
        if part > 0:
            pieces = []
            for span in range(unit.shape[0] // SPAN):
                row = share(span, slice((part - 1) * D, part * D)) * (1.0 / SPAN)
                pieces.append(block[span * SPAN : (span + 1) * SPAN].astype(F32) + row)
            block = jnp.concatenate(pieces, 0).astype(BF16)
        if part not in skip:
            gq[part][...] += dot(n_one, block, TN)
        dn_one = dn_one + dot(block, weight(cols), NT)
    dnorm, grad_gain = norm_backward(dn_one, unit, rstd, gain)
    gg_ref[...] += grad_gain
    return dh + dnorm


def turn_kernel(counts, *refs):
    batch, spans = counts
    (x_ref, near_ref, dh_ref, u_ref, h_ref, o_ref, total_ref, gains_ref, wq_ref, wo_ref, wu_ref, wd_ref,
     pd, pu, po,
     dh_out, dout_out, gd_out, gu_out, go_out, ggq_ref, gg_ref, sd, su, so, sq,
     dx_all, gq_ref, gd_ref, gu_ref, go_ref, gq_low) = refs[:32]
    rest = refs[32:]
    spot = Spot()
    fold = Fold(spot, [pd, pu, po, gq_low], [sd, su, so, sq], rest[:24], rest[24:])
    d1, u1, o1, q1 = range(4)
    step = pl.program_id(0)

    @pl.when(step == 0)
    def _():
        spot.signal()
        zero(gq_ref, gd_ref, gu_ref, go_ref, gg_ref, ggq_ref)

    @pl.when(step == 1)
    def _():
        spot.meet()
        for t in range(3):
            fold.start(t)

    when(step == 3, does(fold.combine, d1))
    when(step == 4, does(fold.combine, u1))
    when(step == 5, does(fold.combine, o1))
    when(step == 7, does(fold.middle, d1))

    @pl.when(step == batch)
    def _():
        gq_low[...] = gq_ref[...].astype(BF16).reshape(gq_low.shape)
        fold.start(q1)

    when(step == batch + 1, does(fold.middle, u1), does(fold.middle, o1), does(fold.combine, q1))
    when(step == batch + 2, does(fold.column, d1), does(fold.column, u1), does(fold.column, o1))
    when(step == batch + 4, does(fold.middle, q1))
    when(step == batch + 5, does(fold.finish, d1), does(fold.finish, u1), does(fold.finish, o1), does(fold.column, q1))
    when(step == batch + 7, does(fold.finish, q1))

    @pl.when(step < batch)
    def _():
        unit, rstd = normed(x_ref[0])
        dx_all[step] = qkv_back(
            unit, rstd, gains_ref[1:2], lambda cols: near_ref[0, :, cols],
            lambda span, cols: total_ref[pl.ds(step * spans + span, 1), cols], dh_ref[0],
            lambda cols: wq_ref[:, cols], [gq_ref.at[:, part * D : (part + 1) * D] for part in range(3)], ggq_ref)

    @pl.when(step >= batch)
    def _():
        dout_out[0] = mlp_back(dx_all[step - batch], u_ref, h_ref, o_ref, gains_ref[2:3], wo_ref, wu_ref, wd_ref,
                               dh_out, gd_ref, gu_ref, go_ref, gg_ref)

    @pl.when(step == 2 * batch - 1)
    def _():
        gd_out[...] = gd_ref[...].astype(BF16)
        gu_out[...] = gu_ref[...].astype(BF16)
        go_out[...] = go_ref[...].astype(BF16)
        for t in range(4):
            fold.drain(t)


def by_owner(part):
    nz, nseq = lax.axis_size("dp"), lax.axis_size("seq")
    return part.reshape((nz, nseq // CORES, CORES, part.shape[0] // (nz * nseq)) + part.shape[1:])


def call_turn(x, near, dh, u, h, o, total, gains, wq, wo, wu, wd, pd, pu, po):
    batch, tokens, _ = x.shape
    nz = lax.axis_size("dp")
    parts = [by_owner(a) for a in (pd, pu, po)]
    owned = by_owner(sds_like(wq))
    shapes = [a.shape[3:] for a in parts] + [owned.shape[3:]]
    args = [x, near, dh, u, h, o, total, gains, wq, wo, wu, wd] + parts
    outs = [sds(h.shape, F32), sds(o.shape, BF16), sds(wd.shape, BF16), sds(wu.shape, BF16), sds(wo.shape, BF16),
            sds((1, D), F32), sds((1, D), F32)] + [sds(s, F32) for s in shapes]
    return pl.pallas_call(
        functools.partial(turn_kernel, (batch, tokens // SPAN)),
        grid=(2 * batch,),
        in_specs=[phased(a.shape, 0, batch) for a in args[:3]] + [phased(a.shape, batch, batch) for a in args[3:6]]
        + [whole(a.shape) for a in args[6:12]] + [anywhere()] * 3,
        out_specs=[phased(a.shape, batch, batch) for a in outs[:2]] + [whole(a.shape) for a in outs[2:]],
        out_shape=outs,
        scratch_shapes=[pltpu.VMEM(x.shape, F32), pltpu.VMEM(wq.shape, F32), pltpu.VMEM(wd.shape, F32),
                        pltpu.VMEM(wu.shape, F32), pltpu.VMEM(wo.shape, F32), pltpu.VMEM(owned.shape, BF16)]
        + Fold.buffers(shapes, nz) + Fold.sems(4, nz),
        compiler_params=fused_params(3),
        name="turn",
    )(*args)


def sds_like(a):
    class Shaped:
        shape = a.shape

        def reshape(self, shape):
            return sds(shape, a.dtype)

    return Shaped()


def leave_kernel(counts, *refs):
    batch, spans = counts
    (prob_ref, qkv_ref, sums_ref, dout_ref, x_ref, dh_ref, gains_ref, wq_ref, g_mlp0, g_attn1, g_mlp1,
     pd, pu, po,
     dx_ref, gsum_ref, sd, su, so, s0, s1, s2,
     near_all, unit_all, rstd_all, a0, a1, a2, l0, l1, l2, gg_ref, gain_src, dsums,
     part_acc, part_a, part_b, land_a, land_b, total, ex_s, ex_r) = refs[:42]
    rest = refs[42:]
    spot = Spot()
    fold = Fold(spot, [pd, pu, po, l0, l1, l2], [sd, su, so, s0, s1, s2], rest[:36], rest[36:43])
    adder = AllSum(spot, gain_src, rest[43:])
    exchange = Exchange(spot, [part_a, part_b], [land_a, land_b], ex_s, ex_r)
    d0, u0, o0, q0, k0, v0 = range(6)
    step = pl.program_id(0)
    half = batch // HALVES

    def pour(acc, low):
        low[...] = acc[...].astype(BF16).reshape(low.shape)

    @pl.when(step == 0)
    def _():
        spot.signal()
        zero(a0, a1, a2, gg_ref, part_acc)

    @pl.when(step == 1)
    def _():
        spot.meet()
        for t in range(3):
            fold.start(t)

    when(step == 2, does(fold.combine, d0))
    when(step == half + 1, does(fold.middle, d0), does(fold.combine, u0), does(fold.combine, o0))
    when(step == batch - 1, does(fold.column, d0))

    @pl.when(step == batch)
    def _():
        pour(a0, l0)
        fold.start(q0)
        gathered(exchange, 0, total)

    when(step == batch + 2, does(fold.middle, u0), does(fold.combine, q0))
    when(step == batch + 3, does(fold.middle, o0))
    when(step == batch + half, does(gathered, exchange, 1, total))
    when(step == batch + 5, does(fold.column, u0))
    when(step == batch + 6, does(fold.column, o0), does(fold.middle, q0))
    when(step == batch + 7, does(fold.finish, d0), does(fold.column, q0))

    @pl.when(step < batch)
    def _():
        near = near_all.at[pl.ds(step, 1)]
        attention_backward(qkv_ref, sums_ref, prob_ref, dout_ref[0], near, dsums)
        pile(step, counts, spot.nseq, dsums, part_acc)
        unit, rstd = normed(x_ref[0].astype(F32))
        unit_all[step] = unit
        rstd_all[step] = rstd
        a0[...] += dot((unit * gains_ref[0:1]).astype(BF16), near_all[step, :, :D], TN)

    when(step == half - 1, does(ship, exchange, 0, part_acc))
    when(step == batch - 1, does(ship, exchange, 1, part_acc))

    @pl.when(step >= batch)
    def _():
        b = step - batch
        dx_ref[0] = qkv_back(
            unit_all[b], rstd_all[b], gains_ref[0:1], lambda cols: near_all[b, :, cols],
            lambda span, cols: total[pl.ds(b * spans + span, 1), cols], dh_ref[0],
            lambda cols: wq_ref[:, cols], [a0, a1, a2], gg_ref, (0,))

    @pl.when(step == 2 * batch - 1)
    def _():
        pour(a1, l1)
        fold.start(k0)
        pour(a2, l2)
        fold.start(v0)
        gain_src[...] = jnp.zeros_like(gain_src)
        gain_src[0:1] = gg_ref[...]
        gain_src[1:2] = g_attn1[...]
        gain_src[2:3] = g_mlp0[...]
        gain_src[3:4] = g_mlp1[...]
        adder.start()
        fold.combine(k0)
        fold.combine(v0)
        adder.plane()
        fold.finish(u0)
        fold.finish(o0)
        fold.middle(k0)
        fold.middle(v0)
        adder.column()
        fold.column(k0)
        fold.column(v0)
        fold.finish(q0)
        gsum_ref[...] = adder.total()
        fold.finish(k0)
        fold.finish(v0)
        for t in range(6):
            fold.drain(t)
        adder.drain()


def call_leave(prob, qkv, sums, dout, x, dh, gains, wq, g_mlp0, g_attn1, g_mlp1, pd, pu, po):
    batch, tokens, _ = x.shape
    spans = tokens // SPAN
    nz, nseq = lax.axis_size("dp"), lax.axis_size("seq")
    rows = batch * spans
    parts = [by_owner(a) for a in (pd, pu, po)]
    square = (D, D)
    owned = (nz, nseq // CORES, CORES, D // (nz * nseq), D)
    shapes = [a.shape[3:] for a in parts] + [owned[3:]] * 3
    args = [prob, qkv, sums, dout, x, dh, gains, wq, g_mlp0, g_attn1, g_mlp1] + parts
    outs = [sds(dh.shape, F32), sds(gains.shape, F32)] + [sds(s, F32) for s in shapes]
    return pl.pallas_call(
        functools.partial(leave_kernel, (batch, spans)),
        grid=(2 * batch,),
        in_specs=[phased(a.shape, 0, batch) for a in args[:5]] + [phased(dh.shape, batch, batch)]
        + [whole(a.shape) for a in args[6:11]] + [anywhere()] * 3,
        out_specs=[phased(outs[0].shape, batch, batch)] + [whole(a.shape) for a in outs[1:]],
        out_shape=outs,
        scratch_shapes=[pltpu.VMEM(qkv.shape, BF16), pltpu.VMEM(x.shape, F32), pltpu.VMEM((batch, tokens, 1), F32)]
        + [pltpu.VMEM(square, F32)] * 3 + [pltpu.VMEM(owned, BF16)] * 3
        + [pltpu.VMEM((1, D), F32), pltpu.VMEM(gains.shape, F32), pltpu.VMEM((1, nseq * spans, 2 * D), BF16)]
        + collect_buffers(nseq, rows) + [pltpu.VMEM((rows, 2 * D), F32)] + Exchange.sems(nseq)
        + Fold.buffers(shapes, nz) + Fold.sems(6, nz) + AllSum.scratch(gains.shape, nz),
        compiler_params=fused_params(4),
        name="leave",
    )(*args)


def pack_kernel(plan, *refs):
    ins, outs = refs[: -len(plan)], refs[-len(plan) :]
    at = 0
    for out, layers in zip(outs, plan):
        for l, pieces in enumerate(layers):
            start = 0
            for width in pieces:
                out[l, :, start : start + width] = ins[at][...]
                at, start = at + 1, start + width


def call_pack(tensors):
    flat = [a for layers in tensors for pieces in layers for a in pieces]
    plan = [[[a.shape[1] for a in pieces] for pieces in layers] for layers in tensors]
    outs = [sds((len(layers), layers[0][0].shape[0], sum(a.shape[1] for a in layers[0])), F32) for layers in tensors]
    vmem = pl.BlockSpec(memory_space=pltpu.VMEM)
    return pl.pallas_call(
        functools.partial(pack_kernel, plan),
        in_specs=[vmem] * len(flat),
        out_specs=[vmem] * len(tensors),
        out_shape=outs,
        name="pack",
    )(*flat)


def fused(inputs, segments, w_qkv, w_out, w_up, w_down, gain_attn, gain_mlp, cotangent):
    stretch = inputs.shape[1]
    slots = gain_attn.shape[1]
    rank = lax.axis_index("dp") * lax.axis_size("seq") + lax.axis_index("seq")
    own = jnp.concatenate([gain_attn, gain_mlp], 0).astype(F32)
    own = jnp.pad(own, ((0, 4), (0, 0)))
    gain_own = lax.dynamic_update_slice(jnp.zeros((8, D), F32), own, (0, rank * slots))
    bias = mask_bias(segments, stretch)

    def flat(a):
        return a.reshape((-1, a.shape[-1]))

    qkv0, sums0, prob0, o0, gains, wq0, wo0, wu0, wd0 = call_enter(
        inputs, bias, gain_own, w_qkv, w_out, w_up, w_down)
    wq0, wo0, wu0, wd0 = (flat(a) for a in (wq0, wo0, wu0, wd0))
    h0, u0, x1, qkv1, raw1, wq1, wo1, wu1, wd1 = call_mid(
        inputs, o0, gains, wo0, wu0, wd0, w_qkv, w_out, w_up, w_down)
    wq1, wo1, wu1, wd1 = (flat(a) for a in (wq1, wo1, wu1, wd1))
    sums1, prob1, o1, h1, u1, outputs = call_top(x1, qkv1, bias, raw1, gains, wo1, wu1, wd1)
    dh1, near1, total1, gd1, gu1, go1, g_mlp1 = call_base(
        cotangent, u1, h1, o1, prob1, qkv1, sums1, gains, wo1, wu1, wd1)
    dh0, dout0, gd0, gu0, go0, g_attn1, g_mlp0, sd1, su1, so1, sq1 = call_turn(
        x1, near1, dh1, u0, h0, o0, total1, gains, wq1, wo0, wu0, wd0, gd1, gu1, go1)
    dx, gsum, sd0, su0, so0, *sq0 = call_leave(
        prob0, qkv0, sums0, dout0, inputs, dh0, gains, wq0, g_mlp0, g_attn1, g_mlp1, gd0, gu0, go0)
    gq, go, gu, gd = call_pack([[sq0, [sq1]], [[so0], [so1]], [[su0], [su1]], [[sd0], [sd1]]])
    gain_share = lax.dynamic_slice(gsum, (0, rank * slots), (4, slots))
    return outputs, dx, gq, go, gu, gd, gain_share[:2], gain_share[2:]


def choose(*args):
    square = lax.axis_size("seq") == 4 * CORES
    if square and args[2].shape[1] % 16 == 0 and args[2].shape[0] == 2:
        return fused(*args)
    return on_device(*args)


def solution(mesh):
    weights = P(None, ("dp", "seq"), None)
    gains = P(None, ("dp", "seq"))
    rows = P("dp", "seq", None)
    return jax.shard_map(
        choose,
        mesh=mesh,
        in_specs=(rows, P("dp", None), weights, weights, weights, weights, gains, gains, rows),
        out_specs=(rows, rows, weights, weights, weights, weights, gains, gains),
        check_vma=False,
    )
```

```python
import functools

import jax
import jax.numpy as jnp
from jax import lax
from jax.experimental import pallas as pl
from jax.experimental.pallas import tpu as pltpu
from jax.sharding import PartitionSpec as P

D = 512
HEADS = 8
HEAD = 64
SPAN = 128
PAIRS = HEADS // 2
EPS = 1e-05
NEG = -1000000000.0
SCALE = HEAD ** (-0.5)
F32 = jnp.float32
BF16 = jnp.bfloat16
CHUNK = 512
VMEM_LIMIT = 60 * 1024 * 1024

NN = (((1,), (0,)), ((), ()))
NT = (((1,), (1,)), ((), ()))
TN = (((0,), (0,)), ((), ()))


def dot(left, right, dims=NN):
    return lax.dot_general(left, right, dims, preferred_element_type=F32)


def normed(values):
    mean = jnp.mean(values, -1, keepdims=True)
    centred = values - mean
    var = jnp.mean(centred * centred, -1, keepdims=True)
    rstd = lax.rsqrt(var + EPS)
    return centred * rstd, rstd


def norm_backward(dnorm, unit, rstd, gain):
    grad_gain = jnp.sum(dnorm * unit, 0, keepdims=True)
    scaled = dnorm * gain
    first = jnp.mean(scaled, -1, keepdims=True)
    second = jnp.mean(scaled * unit, -1, keepdims=True)
    return rstd * (scaled - first - unit * second), grad_gain


def project_qkv(x32, gain, wq_ref, qkv_ref, sums_ref):
    unit, _ = normed(x32)
    n_one = (unit * gain).astype(BF16)
    spans = x32.shape[0] // SPAN
    for part in range(3):
        block = dot(n_one, wq_ref[:, part * D : (part + 1) * D]).astype(BF16)
        qkv_ref[0, :, part * D : (part + 1) * D] = block
        if part > 0:
            wide = block.astype(F32)
            for span in range(spans):
                mean = jnp.sum(wide[span * SPAN : (span + 1) * SPAN], 0, keepdims=True) * (1.0 / SPAN)
                sums_ref[0, span : span + 1, (part - 1) * D : part * D] = mean.astype(BF16)


def lane_halves():
    lane = lax.broadcasted_iota(jnp.int32, (1, 2 * HEAD), 1)
    low = lane < HEAD
    return low


def head_stack(block, low, factor):
    one = jnp.where(low, factor, 0.0).astype(BF16)
    two = jnp.where(low, 0.0, factor).astype(BF16)
    return jnp.concatenate([block * one, block * two], 0)


def pair_operands(qkv_ref, sums_ref, span, pair):
    rows = slice(span * SPAN, (span + 1) * SPAN)
    lanes = slice(pair * 128, (pair + 1) * 128)
    keys = jnp.concatenate(
        [qkv_ref[0, rows, D + pair * 128 : D + (pair + 1) * 128], sums_ref[0, :, lanes]], 0
    )
    values = jnp.concatenate(
        [
            qkv_ref[0, rows, 2 * D + pair * 128 : 2 * D + (pair + 1) * 128],
            sums_ref[0, :, D + pair * 128 : D + (pair + 1) * 128],
        ],
        0,
    )
    query = qkv_ref[0, rows, lanes]
    return query, keys, values


def attention_forward(qkv_ref, sums_ref, bias_ref, prob_ref, o_ref):
    low = lane_halves()
    units = [(span, pair) for span in range(qkv_ref.shape[1] // SPAN) for pair in range(PAIRS)]
    for start in range(0, len(units), GROUP):
        group = units[start : start + GROUP]
        operands = [pair_operands(qkv_ref, sums_ref, span, pair) for span, pair in group]
        scores = []
        for (span, _), (query, keys, _) in zip(group, operands):
            bias = bias_ref[0, span]
            bias = jnp.concatenate([bias, bias], 1)
            scores.append(dot(keys, head_stack(query, low, SCALE), NT) + bias)
        exps = [jnp.exp(score - jnp.max(score, 0, keepdims=True)) for score in scores]
        probs = [(e * (1.0 / jnp.sum(e, 0, keepdims=True))).astype(BF16) for e in exps]
        both = [dot(prob, values, TN) for prob, (_, _, values) in zip(probs, operands)]
        for (span, pair), prob, out in zip(group, probs, both):
            prob_ref[0, span, pair] = prob
            o_ref[0, span * SPAN : (span + 1) * SPAN, pair * 128 : (pair + 1) * 128] = jnp.where(
                low, out[:SPAN], out[SPAN:]
            ).astype(BF16)


def attention_backward(qkv_ref, sums_ref, prob_ref, dout, dqkv_ref, dsums_ref):
    low = lane_halves()
    spans = qkv_ref.shape[1] // SPAN
    for start in range(0, PAIRS, BACK_GROUP):
        pairs = range(start, start + BACK_GROUP)
        units = [(span, pair) for pair in pairs for span in range(spans)]
        operands = [pair_operands(qkv_ref, sums_ref, span, pair) for span, pair in units]
        q_stacks = [head_stack(query, low, SCALE) for query, _, _ in operands]
        do_stacks = [
            head_stack(dout[span * SPAN : (span + 1) * SPAN, pair * 128 : (pair + 1) * 128], low, 1.0)
            for span, pair in units
        ]
        probs = [prob_ref[0, span, pair] for span, pair in units]
        dprobs = [dot(values, do_stack, NT) for (_, _, values), do_stack in zip(operands, do_stacks)]
        dvalues = [dot(prob, do_stack) for prob, do_stack in zip(probs, do_stacks)]
        dscores = []
        for prob, dprob in zip(probs, dprobs):
            wide = prob.astype(F32)
            product = wide * dprob
            dscores.append((product - wide * jnp.sum(product, 0, keepdims=True)).astype(BF16))
        dkeys = [dot(dscore, q_stack) for dscore, q_stack in zip(dscores, q_stacks)]
        dboths = [dot(dscore, keys, TN) for dscore, (_, keys, _) in zip(dscores, operands)]
        for (span, pair), dboth, dkey, dvalue in zip(units, dboths, dkeys, dvalues):
            rows = slice(span * SPAN, (span + 1) * SPAN)
            dquery = jnp.where(low, dboth[:SPAN], dboth[SPAN:]) * SCALE
            for part, block in enumerate((dquery, dkey[:SPAN], dvalue[:SPAN])):
                lanes = slice(part * D + pair * 128, part * D + (pair + 1) * 128)
                dqkv_ref[0, rows, lanes] = block.astype(BF16)
        for at, pair in enumerate(pairs):
            mine = range(at * spans, (at + 1) * spans)
            dksum = sum(dkeys[i][SPAN:] for i in mine)
            dvsum = sum(dvalues[i][SPAN:] for i in mine)
            dsums_ref[0, :, pair * 128 : (pair + 1) * 128] = dksum.astype(BF16)
            dsums_ref[0, :, D + pair * 128 : D + (pair + 1) * 128] = dvsum.astype(BF16)


GROUP = 8
BACK_GROUP = 4
G0 = 0.7978845608
G1 = 0.7978845608 * 0.044715


def gelu(values):
    squared = values * values
    slope = jnp.tanh(values * (G0 + G1 * squared))
    half = 0.5 * values
    return half + half * slope


def gelu_both(values):
    squared = values * values
    slope = jnp.tanh(values * (G0 + G1 * squared))
    half = 0.5 * values
    rise = 0.5 + 0.5 * slope
    inner = G0 + (3.0 * G1) * squared
    return values * rise, rise + half * (1.0 - slope * slope) * inner


def mlp_forward(h32, gain, wu_ref, wd_ref, u_ref):
    unit, _ = normed(h32)
    n_two = (unit * gain).astype(BF16)
    total = h32
    for start in range(0, wu_ref.shape[1], CHUNK):
        upper = dot(n_two, wu_ref[:, start : start + CHUNK])
        u_ref[:, :, start : start + CHUNK] = upper.astype(BF16).reshape((u_ref.shape[0], -1, CHUNK))
        total = total + dot(gelu(upper).astype(BF16), wd_ref[start : start + CHUNK, :])
    return total


def first_kernel(x_ref, gain_ref, wq_ref, qkv_ref, sums_ref):
    project_qkv(x_ref[0].astype(F32), gain_ref[...], wq_ref, qkv_ref, sums_ref)


def layer_kernel(last, *refs):
    if last:
        (x_ref, qkv_ref, sums_ref, bias_ref, gain_ref, wo_ref, wu_ref, wd_ref,
         prob_ref, o_ref, h_ref, u_ref, next_ref) = refs
    else:
        (x_ref, qkv_ref, sums_ref, bias_ref, gain_ref, wo_ref, wu_ref, wd_ref, gain_next_ref, wq_ref,
         prob_ref, o_ref, h_ref, u_ref, next_ref, qkv_next_ref, sums_next_ref) = refs
    attention_forward(qkv_ref, sums_ref, bias_ref, prob_ref, o_ref)
    hidden = x_ref[0].astype(F32) + dot(o_ref[0], wo_ref[...])
    h_ref[0] = hidden
    result = mlp_forward(hidden, gain_ref[...], wu_ref, wd_ref, u_ref)
    next_ref[0] = result.astype(next_ref.dtype)
    if not last:
        project_qkv(result, gain_next_ref[...], wq_ref, qkv_next_ref, sums_next_ref)


def accumulate(ref, index, value, first):
    @pl.when(first)
    def _():
        ref[index] = value

    @pl.when(jnp.logical_not(first))
    def _():
        ref[index] = ref[index] + value


def mlp_attention_backward(dy32, u_ref, h_ref, o_ref, prob_ref, qkv_ref, sums_ref, gain_ref,
                           wo_ref, wu_ref, wd_ref, dh_ref, dqkv_ref, dsums_ref, gd_ref, gu_ref,
                           go_ref, gg_ref):
    ddown = dy32.astype(BF16)
    unit, rstd = normed(h_ref[0])
    n_two = (unit * gain_ref[...]).astype(BF16)
    dn_two = 0.0
    for start in range(0, wu_ref.shape[1], CHUNK):
        cols = slice(start, start + CHUNK)
        dactive = dot(ddown, wd_ref[cols, :], NT)
        active, slope = gelu_both(u_ref[0, :, cols].astype(F32))
        gd_ref[cols, :] += dot(active.astype(BF16), ddown, TN)
        dupper = (dactive * slope).astype(BF16)
        gu_ref[:, cols] += dot(n_two, dupper, TN)
        dn_two = dn_two + dot(dupper, wu_ref[:, cols], NT)
    dnorm, grad_gain = norm_backward(dn_two, unit, rstd, gain_ref[...])
    gg_ref[...] += grad_gain
    dhidden = dy32 + dnorm
    dh_ref[0] = dhidden
    dattn = dhidden.astype(BF16)
    go_ref[...] += dot(o_ref[0], dattn, TN)
    dout = dot(dattn, wo_ref[...], NT).astype(BF16)
    attention_backward(qkv_ref, sums_ref, prob_ref, dout, dqkv_ref, dsums_ref)


def back_kernel(dy_ref, u_ref, h_ref, o_ref, prob_ref, qkv_ref, sums_ref, gain_ref,
                wo_ref, wu_ref, wd_ref, dh_ref, dqkv_ref, dsums_ref, gd_out, gu_out, go_out,
                gg_ref, gd_ref, gu_ref, go_ref):
    step = pl.program_id(0)

    @pl.when(step == 0)
    def _():
        gd_ref[...] = jnp.zeros_like(gd_ref)
        gu_ref[...] = jnp.zeros_like(gu_ref)
        go_ref[...] = jnp.zeros_like(go_ref)
        gg_ref[...] = jnp.zeros_like(gg_ref)

    mlp_attention_backward(dy_ref[0].astype(F32), u_ref, h_ref, o_ref, prob_ref, qkv_ref, sums_ref,
                           gain_ref, wo_ref, wu_ref, wd_ref, dh_ref, dqkv_ref, dsums_ref, gd_ref,
                           gu_ref, go_ref, gg_ref)

    @pl.when(step == pl.num_programs(0) - 1)
    def _():
        gd_out[...] = gd_ref[...].astype(BF16)
        gu_out[...] = gu_ref[...].astype(BF16)
        go_out[...] = go_ref[...].astype(BF16)


def qkv_backward(x32, gain, near_ref, dsums_ref, dh, wq_ref, gq_ref, gg_ref):
    unit, rstd = normed(x32)
    n_one = (unit * gain).astype(BF16)
    dn_one = 0.0
    tokens = x32.shape[0]
    for part in range(3):
        cols = slice(part * D, (part + 1) * D)
        block = near_ref[0, :, cols]
        if part > 0:
            pieces = []
            for span in range(tokens // SPAN):
                share = dsums_ref[0, span : span + 1, (part - 1) * D : part * D].astype(F32) * (1.0 / SPAN)
                pieces.append(block[span * SPAN : (span + 1) * SPAN].astype(F32) + share)
            block = jnp.concatenate(pieces, 0).astype(BF16)
        gq_ref[:, cols] += dot(n_one, block, TN)
        dn_one = dn_one + dot(block, wq_ref[:, cols], NT)
    dnorm, grad_gain = norm_backward(dn_one, unit, rstd, gain)
    gg_ref[...] += grad_gain
    return dh + dnorm


def last_kernel(x_ref, gain_ref, near_ref, dsums_ref, dh_ref, wq_ref, dx_ref, gq_out, gg_ref, gq_ref):
    step = pl.program_id(0)

    @pl.when(step == 0)
    def _():
        gq_ref[...] = jnp.zeros_like(gq_ref)
        gg_ref[...] = jnp.zeros_like(gg_ref)

    dx_ref[0] = qkv_backward(x_ref[0].astype(F32), gain_ref[...], near_ref, dsums_ref, dh_ref[0], wq_ref,
                             gq_ref, gg_ref)

    @pl.when(step == pl.num_programs(0) - 1)
    def _():
        gq_out[...] = gq_ref[...].astype(BF16)


def per_seq(shape):
    rest = len(shape) - 1
    return pl.BlockSpec((1,) + tuple(shape[1:]), lambda b: (b,) + (0,) * rest)


def whole(shape):
    rank = len(shape)
    return pl.BlockSpec(tuple(shape), lambda b: (0,) * rank, pipeline_mode=pl.Buffered(1))


def sds(shape, dtype):
    return jax.ShapeDtypeStruct(tuple(shape), dtype)


def params():
    return pltpu.CompilerParams(dimension_semantics=("arbitrary",), vmem_limit_bytes=VMEM_LIMIT)


def call_first(x, gain, wq):
    batch, tokens, _ = x.shape
    spans = tokens // SPAN
    outs = (sds((batch, tokens, 3 * D), BF16), sds((batch, spans, 2 * D), BF16))
    return pl.pallas_call(
        first_kernel,
        grid=(batch,),
        in_specs=[per_seq(x.shape), whole(gain.shape), whole(wq.shape)],
        out_specs=[per_seq(o.shape) for o in outs],
        out_shape=outs,
        compiler_params=params(),
        name="first",
    )(x, gain, wq)


def call_layer(x, qkv, sums, bias, gain, wo, wu, wd, gain_next=None, wq=None):
    batch, tokens, _ = x.shape
    spans = tokens // SPAN
    last = wq is None
    keys = SPAN + sums.shape[1]
    outs = [
        sds((batch, spans, PAIRS, keys, 2 * SPAN), BF16),
        sds((batch, tokens, D), BF16),
        sds((batch, tokens, D), F32),
        sds((batch, tokens, wu.shape[1]), BF16),
        sds((batch, tokens, D), BF16 if last else F32),
    ]
    args = [x, qkv, sums, bias, gain, wo, wu, wd]
    if not last:
        outs += [sds((batch, tokens, 3 * D), BF16), sds((batch, spans, 2 * D), BF16)]
        args += [gain_next, wq]
    specs = [per_seq(a.shape) for a in args[:4]] + [whole(a.shape) for a in args[4:]]
    return pl.pallas_call(
        functools.partial(layer_kernel, last),
        grid=(batch,),
        in_specs=specs,
        out_specs=[per_seq(o.shape) for o in outs],
        out_shape=outs,
        compiler_params=params(),
        name="layer",
    )(*args)


def call_back(dy, u, h, o, prob, qkv, sums, gain, wo, wu, wd):
    batch, tokens, _ = dy.shape
    args = [dy, u, h, o, prob, qkv, sums, gain, wo, wu, wd]
    specs = [per_seq(a.shape) for a in args[:7]] + [whole(a.shape) for a in args[7:]]
    outs = [sds(h.shape, F32), sds(qkv.shape, BF16), sds(sums.shape, BF16),
            sds(wd.shape, BF16), sds(wu.shape, BF16), sds(wo.shape, BF16), sds((1, D), F32)]
    return pl.pallas_call(
        back_kernel,
        grid=(batch,),
        in_specs=specs,
        out_specs=[per_seq(o.shape) for o in outs[:3]] + [whole(o.shape) for o in outs[3:]],
        out_shape=outs,
        scratch_shapes=[pltpu.VMEM(wd.shape, F32), pltpu.VMEM(wu.shape, F32), pltpu.VMEM(wo.shape, F32)],
        compiler_params=params(),
        name="back",
    )(*args)


def call_last(x, gain, near, dsums, dh, wq):
    batch, tokens, _ = x.shape
    outs = [sds((batch, tokens, D), F32), sds(wq.shape, BF16), sds((1, D), F32)]
    return pl.pallas_call(
        last_kernel,
        grid=(batch,),
        in_specs=[per_seq(x.shape), whole(gain.shape), per_seq(near.shape), per_seq(dsums.shape),
                  per_seq(dh.shape), whole(wq.shape)],
        out_specs=[per_seq(outs[0].shape), whole(outs[1].shape), whole(outs[2].shape)],
        out_shape=outs,
        scratch_shapes=[pltpu.VMEM(wq.shape, F32)],
        compiler_params=params(),
        name="last",
    )(x, gain, near, dsums, dh, wq)


def mask_bias(segments, stretch):
    batch, length = segments.shape
    rank = lax.axis_index("seq")
    own = lax.dynamic_slice_in_dim(segments, rank * stretch, stretch, 1).reshape(batch, -1, SPAN)
    ends = segments.reshape(batch, -1, SPAN)[:, :, SPAN - 1]
    spans = own.shape[1]
    pos = jnp.arange(SPAN)
    near = (own[:, :, :, None] == own[:, :, None, :]) & (pos[:, None] <= pos[None, :])
    ids = rank * spans + jnp.arange(spans)
    before = jnp.arange(ends.shape[1])[None, :] < ids[:, None]
    far = (ends[:, None, :, None] == own[:, :, None, :]) & before[None, :, :, None]
    return jnp.where(jnp.concatenate([near, far], 2), 0.0, NEG).astype(F32)

MESH = pl.DeviceIdType.MESH
CORES = 2


def place():
    nz, nseq = lax.axis_size("dp"), lax.axis_size("seq")
    z, s = lax.axis_index("dp"), lax.axis_index("seq")
    return nz, nseq // CORES, z, s // CORES, lax.rem(s, CORES)


def modulo(value, size):
    return lax.rem(value + size, size)


def peers_of():
    nz, nchip, z, chip, core = place()
    seq = chip * CORES + core
    out = [(modulo(z + d, nz), seq) for d in range(1, nz)]
    out += [(z, modulo(chip + d, nchip) * CORES + core) for d in range(1, nchip)]
    out.append((z, chip * CORES + 1 - core))
    return out


def greet(peers):
    barrier = pltpu.get_barrier_semaphore()
    for peer in peers:
        pl.semaphore_signal(barrier, inc=1, device_id=peer, device_id_type=MESH)
    pl.semaphore_wait(barrier, len(peers))


def remote(src, dst, send, recv, peer):
    return pltpu.make_async_remote_copy(
        src_ref=src, dst_ref=dst, send_sem=send, recv_sem=recv, device_id=peer, device_id_type=MESH
    )


class Gather:
    def __init__(self, shards, fulls, sems):
        self.shards, self.fulls = shards, fulls
        self.own, self.zs, self.zr, self.ps, self.pr, self.cs, self.cr = sems
        self.nz, self.nchip, self.z, self.chip, self.core = place()
        self.seq = self.chip * CORES + self.core

    @staticmethod
    def scratch(count):
        nz, nchip = lax.axis_size("dp"), lax.axis_size("seq") // CORES
        dma = pltpu.SemaphoreType.DMA
        return [dma((count,)), dma((count, nz - 1)), dma((count, nz - 1)), dma((count, nchip - 1)),
                dma((count, nchip - 1)), dma((count, nchip)), dma((count, nchip))]

    def local(self, t):
        return pltpu.make_async_copy(self.shards[t], self.fulls[t].at[self.z, self.seq], self.own.at[t])

    def line(self, t, d):
        peer = (modulo(self.z + d, self.nz), self.seq)
        return remote(self.shards[t], self.fulls[t].at[self.z, self.seq], self.zs.at[t, d - 1],
                      self.zr.at[t, d - 1], peer)

    def plane(self, t, d):
        block = self.fulls[t].at[:, self.seq]
        peer = (self.z, modulo(self.chip + d, self.nchip) * CORES + self.core)
        return remote(block, block, self.ps.at[t, d - 1], self.pr.at[t, d - 1], peer)

    def cross(self, t, d):
        block = self.fulls[t].at[:, modulo(self.chip - d, self.nchip) * CORES + self.core]
        peer = (self.z, self.chip * CORES + 1 - self.core)
        return remote(block, block, self.cs.at[t, d], self.cr.at[t, d], peer)

    def start(self, t):
        self.local(t).start()
        for d in range(1, self.nz):
            self.line(t, d).start()

    def spread(self, t):
        self.local(t).wait()
        for d in range(1, self.nz):
            self.line(t, d).wait_recv()
        for d in range(1, self.nchip):
            self.plane(t, d).start()
        self.cross(t, 0).start()

    def share(self, t):
        for d in range(1, self.nchip):
            self.plane(t, d).wait_recv()
            self.cross(t, d).start()

    def finish(self, t):
        for d in range(self.nchip):
            self.cross(t, d).wait_recv()

    def drain(self, t):
        for d in range(1, self.nz):
            self.line(t, d).wait_send()
        for d in range(1, self.nchip):
            self.plane(t, d).wait_send()
        for d in range(self.nchip):
            self.cross(t, d).wait_send()


def gather_kernel(count, *refs):
    work = Gather(refs[:count], refs[count : 2 * count], refs[2 * count :])
    greet(peers_of())
    for stage in (work.start, work.spread, work.share, work.finish, work.drain):
        for t in range(count):
            stage(t)


def call_gather(shards, collective_id):
    nz, nseq = lax.axis_size("dp"), lax.axis_size("seq")
    count = len(shards)
    outs = [sds((nz, nseq) + a.shape, a.dtype) for a in shards]
    return pl.pallas_call(
        functools.partial(gather_kernel, count),
        in_specs=[pl.BlockSpec(memory_space=pltpu.VMEM)] * count,
        out_specs=[pl.BlockSpec(memory_space=pl.ANY)] * count,
        out_shape=outs,
        scratch_shapes=Gather.scratch(count),
        compiler_params=pltpu.CompilerParams(
            collective_id=collective_id, has_side_effects=True, vmem_limit_bytes=VMEM_LIMIT
        ),
        name="gather",
    )(*shards)


class Reduce:
    def __init__(self, parts, outs, bufs, sems):
        self.parts, self.outs = parts, outs
        count = len(parts)
        self.mine, self.cross_in, self.plane_in, self.col, self.line_in = (
            bufs[i * count : (i + 1) * count] for i in range(5)
        )
        self.own, self.cs, self.cr, self.ps, self.pr, self.zs, self.zr = sems
        self.nz, self.nchip, self.z, self.chip, self.core = place()
        self.seq = self.chip * CORES + self.core

    @staticmethod
    def scratch(parts):
        nz, nchip = lax.axis_size("dp"), lax.axis_size("seq") // CORES
        dma = pltpu.SemaphoreType.DMA
        count = len(parts)
        bufs = []
        for lead in ((nchip, nz), (nchip, nz), (nchip - 1, nz), (nz,), (nz - 1,)):
            bufs += [pltpu.VMEM(lead + a.shape[3:], a.dtype) for a in parts]
        return bufs + [dma((count, nchip)), dma((count, nchip)), dma((count, nchip)), dma((count, nchip - 1)),
                       dma((count, nchip - 1)), dma((count, nz - 1)), dma((count, nz - 1))]

    def local(self, t, d):
        chip = modulo(self.chip + d, self.nchip)
        return pltpu.make_async_copy(self.parts[t].at[:, chip, self.core], self.mine[t].at[d], self.own.at[t, d])

    def cross(self, t, d):
        chip = modulo(self.chip + d, self.nchip)
        peer = (self.z, self.chip * CORES + 1 - self.core)
        return remote(self.parts[t].at[:, chip, 1 - self.core], self.cross_in[t].at[d], self.cs.at[t, d],
                      self.cr.at[t, d], peer)

    def plane(self, t, d):
        peer = (self.z, modulo(self.chip + d, self.nchip) * CORES + self.core)
        return remote(self.mine[t].at[d], self.plane_in[t].at[d - 1], self.ps.at[t, d - 1],
                      self.pr.at[t, d - 1], peer)

    def line(self, t, d):
        z = modulo(self.z + d, self.nz)
        return remote(self.col[t].at[z], self.line_in[t].at[d - 1], self.zs.at[t, d - 1],
                      self.zr.at[t, d - 1], (z, self.seq))

    def order(self):
        return list(range(1, self.nchip)) + [0]

    def start(self, t):
        for d in self.order():
            self.cross(t, d).start()
            self.local(t, d).start()

    def combine(self, t):
        for d in self.order():
            self.local(t, d).wait()
            self.cross(t, d).wait_recv()

            def add(i, carry):
                total = self.mine[t][d, i].astype(F32) + self.cross_in[t][d, i].astype(F32)
                self.mine[t][d, i] = total.astype(self.mine[t].dtype)
                return carry

            lax.fori_loop(0, self.nz, add, 0)
            if d > 0:
                self.plane(t, d).start()

    def column(self, t):
        for d in range(1, self.nchip):
            self.plane(t, d).wait_recv()

        def add(i, carry):
            total = self.mine[t][0, i].astype(F32)
            for d in range(self.nchip - 1):
                total = total + self.plane_in[t][d, i].astype(F32)
            self.col[t][i] = total.astype(self.col[t].dtype)
            return carry

        lax.fori_loop(0, self.nz, add, 0)
        for d in range(1, self.nz):
            self.line(t, d).start()

    def finish(self, t):
        total = self.col[t][self.z].astype(F32)
        for d in range(1, self.nz):
            self.line(t, d).wait_recv()
        for d in range(self.nz - 1):
            total = total + self.line_in[t][d].astype(F32)
        self.outs[t][...] = total

    def drain(self, t):
        for d in self.order():
            self.cross(t, d).wait_send()
        for d in range(1, self.nchip):
            self.plane(t, d).wait_send()
        for d in range(1, self.nz):
            self.line(t, d).wait_send()


def reduce_kernel(count, *refs):
    work = Reduce(refs[:count], refs[count : 2 * count], refs[2 * count : 7 * count], refs[7 * count :])
    greet(peers_of())
    for stage in (work.start, work.combine, work.column, work.finish, work.drain):
        for t in range(count):
            stage(t)


def call_reduce(parts, collective_id):
    nz, nseq = lax.axis_size("dp"), lax.axis_size("seq")
    count = len(parts)
    parts = [a.reshape((nz, nseq // CORES, CORES, a.shape[0] // (nz * nseq)) + a.shape[1:]) for a in parts]
    outs = [sds(a.shape[3:], F32) for a in parts]
    return pl.pallas_call(
        functools.partial(reduce_kernel, count),
        in_specs=[pl.BlockSpec(memory_space=pl.ANY)] * count,
        out_specs=[pl.BlockSpec(memory_space=pltpu.VMEM)] * count,
        out_shape=outs,
        scratch_shapes=Reduce.scratch(parts),
        compiler_params=pltpu.CompilerParams(
            collective_id=collective_id, has_side_effects=True, vmem_limit_bytes=VMEM_LIMIT
        ),
        name="reduce",
    )(*parts)


def seq_peers():
    nseq = lax.axis_size("seq")
    z, s = lax.axis_index("dp"), lax.axis_index("seq")
    return [(d, (z, modulo(s + d, nseq))) for d in range(1, nseq)]


def spread_kernel(own_ref, all_ref, send, recv):
    s = lax.axis_index("seq")
    peers = seq_peers()
    greet([peer for _, peer in peers])
    copies = [remote(own_ref, all_ref.at[s], send.at[d - 1], recv.at[d - 1], peer) for d, peer in peers]
    for copy in copies:
        copy.start()
    all_ref[s] = own_ref[...]
    for copy in copies:
        copy.wait()


def call_spread(own, collective_id):
    nseq = lax.axis_size("seq")
    return pl.pallas_call(
        spread_kernel,
        in_specs=[pl.BlockSpec(memory_space=pltpu.VMEM)],
        out_specs=pl.BlockSpec(memory_space=pltpu.VMEM),
        out_shape=sds((nseq,) + own.shape, own.dtype),
        scratch_shapes=[pltpu.SemaphoreType.DMA((nseq - 1,)),
                        pltpu.SemaphoreType.DMA((nseq - 1,))],
        compiler_params=pltpu.CompilerParams(
            collective_id=collective_id, has_side_effects=True, vmem_limit_bytes=VMEM_LIMIT
        ),
        name="spread",
    )(own)


def collect_kernel(part_ref, out_ref, slots, send, recv):
    s = lax.axis_index("seq")
    nseq = lax.axis_size("seq")
    peers = seq_peers()
    greet([peer for _, peer in peers])
    copies = [remote(part_ref.at[modulo(s + d, nseq)], slots.at[d - 1], send.at[d - 1], recv.at[d - 1], peer)
              for d, peer in peers]
    for copy in copies:
        copy.start()
    total = part_ref[s].astype(F32)
    for d, _ in peers:
        copies[d - 1].wait()
    for d in range(nseq - 1):
        total = total + slots[d].astype(F32)
    out_ref[...] = total


def call_collect(part, collective_id):
    nseq = part.shape[0]
    return pl.pallas_call(
        collect_kernel,
        in_specs=[pl.BlockSpec(memory_space=pltpu.VMEM)],
        out_specs=pl.BlockSpec(memory_space=pltpu.VMEM),
        out_shape=sds(part.shape[1:], F32),
        scratch_shapes=[pltpu.VMEM((nseq - 1,) + part.shape[1:], part.dtype),
                        pltpu.SemaphoreType.DMA((nseq - 1,)), pltpu.SemaphoreType.DMA((nseq - 1,))],
        compiler_params=pltpu.CompilerParams(
            collective_id=collective_id, has_side_effects=True, vmem_limit_bytes=VMEM_LIMIT
        ),
        name="collect",
    )(part)


def on_device(inputs, segments, w_qkv, w_out, w_up, w_down, gain_attn, gain_mlp, cotangent):
    layers = w_qkv.shape[0]
    batch, stretch, _ = inputs.shape
    nz, nseq = lax.axis_size("dp"), lax.axis_size("seq")
    spans = stretch // SPAN
    slots = gain_attn.shape[1]
    gain_shard = jnp.pad(
        jnp.concatenate([gain_attn, gain_mlp], 0).astype(F32), ((0, 8 - 2 * layers), (0, 128 - slots))
    )
    shards = []
    for l in range(layers):
        shards += [w_qkv[l], w_out[l], w_up[l], w_down[l]]
    fulls = call_gather(shards + [gain_shard], 0)
    gains = fulls[-1][:, :, : 2 * layers, :slots].transpose(2, 0, 1, 3).reshape(2 * layers, D)
    g_one = [gains[l : l + 1] for l in range(layers)]
    g_two = [gains[layers + l : layers + l + 1] for l in range(layers)]
    flat = [a.reshape((-1, a.shape[-1])) for a in fulls[:-1]]
    wq, wo, wu, wd = (flat[m::4] for m in range(4))
    bias = mask_bias(segments, stretch)

    def spread(sums, index):
        return call_spread(sums, index).transpose(1, 0, 2, 3).reshape(batch, nseq * spans, 2 * D)

    def collect(dsums, index):
        return call_collect(dsums.reshape(batch, nseq, spans, 2 * D).transpose(1, 0, 2, 3), index)

    x = inputs
    qkv, own = call_first(x, g_one[0], wq[0])
    kept = []
    for l in range(layers):
        sums = spread(own, 1)
        if l + 1 < layers:
            prob, o, h, u, x_next, qkv_next, own = call_layer(
                x, qkv, sums, bias, g_two[l], wo[l], wu[l], wd[l], g_one[l + 1], wq[l + 1]
            )
        else:
            prob, o, h, u, x_next = call_layer(x, qkv, sums, bias, g_two[l], wo[l], wu[l], wd[l])
            qkv_next = None
        kept.append((x, qkv, sums, prob, o, h, u))
        x, qkv = x_next, qkv_next
    outputs = x
    dy = cotangent
    grads = [None] * layers
    for l in reversed(range(layers)):
        x, qkv, sums, prob, o, h, u = kept[l]
        dh, near, dsums, gd, gu, go, gg_two = call_back(
            dy, u, h, o, prob, qkv, sums, g_two[l], wo[l], wu[l], wd[l]
        )
        dy, gq, gg_one = call_last(x, g_one[l], near, collect(dsums, 2), dh, wq[l])
        grads[l] = (gq, go, gu, gd, gg_one, gg_two)
    gain_grads = jnp.concatenate([grads[l][4] for l in range(layers)] + [grads[l][5] for l in range(layers)], 0)
    gain_grads = jnp.pad(
        gain_grads.reshape(2 * layers, nz * nseq, slots).transpose(1, 0, 2),
        ((0, 0), (0, 8 - 2 * layers), (0, 128 - slots)),
    ).reshape(-1, 128)
    parts = []
    for l in range(layers):
        parts += list(grads[l][:4])
    shares = call_reduce(parts + [gain_grads], 3)
    stacked = [jnp.stack(shares[m : 4 * layers : 4]) for m in range(4)]
    gain_share = shares[-1][: 2 * layers, :slots]
    return (outputs, dy, *stacked, gain_share[:layers], gain_share[layers:])


class Spot:
    def __init__(self):
        self.nz, self.nseq = lax.axis_size("dp"), lax.axis_size("seq")
        self.z, self.seq = lax.axis_index("dp"), lax.axis_index("seq")
        self.chip, self.core = lax.div(self.seq, CORES), lax.rem(self.seq, CORES)
        row, col = lax.div(self.chip, 2), lax.rem(self.chip, 2)
        across, along = row * 2 + 1 - col, (1 - row) * 2 + col
        self.first = (1 - self.core) * across + self.core * along
        self.second = (1 - self.core) * along + self.core * across
        self.diagonal = (1 - row) * 2 + 1 - col

    def at_chip(self, chip):
        return (self.z, chip * CORES + self.core)

    def twin(self):
        return (self.z, self.chip * CORES + 1 - self.core)

    def on_line(self, d):
        return (modulo(self.z + d, self.nz), self.seq)

    def signal(self):
        barrier = pltpu.get_barrier_semaphore()
        for peer in self.peers():
            pl.semaphore_signal(barrier, inc=1, device_id=peer, device_id_type=MESH)

    def meet(self):
        pl.semaphore_wait(pltpu.get_barrier_semaphore(), len(self.peers()))

    def peers(self):
        out = [self.on_line(d) for d in range(1, self.nz)]
        return out + [(self.z, modulo(self.seq + d, self.nseq)) for d in range(1, self.nseq)]


def dma(*shape):
    return pltpu.SemaphoreType.DMA(shape)


class Lines:
    def __init__(self, spot, shards, cols, sems):
        self.spot, self.shards, self.cols = spot, shards, cols
        self.own, self.ss, self.rs = sems

    @staticmethod
    def sems(count, nz):
        return [dma(count), dma(count, nz - 1), dma(count, nz - 1)]

    def local(self, t):
        return pltpu.make_async_copy(self.shards[t], self.cols[t].at[self.spot.z], self.own.at[t])

    def line(self, t, d):
        return remote(self.shards[t], self.cols[t].at[self.spot.z], self.ss.at[t, d - 1], self.rs.at[t, d - 1],
                      self.spot.on_line(d))

    def start(self, t):
        self.local(t).start()
        for d in range(1, self.spot.nz):
            self.line(t, d).start()

    def arrive(self, t):
        self.local(t).wait()
        for d in range(1, self.spot.nz):
            self.line(t, d).wait_recv()

    def drain(self, t):
        for d in range(1, self.spot.nz):
            self.line(t, d).wait_send()


class Plane:
    def __init__(self, spot, cols, fulls, sems):
        self.spot, self.cols, self.fulls = spot, cols, fulls
        self.own, self.hs, self.hr, self.cs, self.cr = sems

    @staticmethod
    def sems(count):
        return [dma(count), dma(count, 3), dma(count, 3), dma(count, 4), dma(count, 4)]

    def block(self, t, chip):
        return self.fulls[t].at[:, chip * CORES + self.spot.core]

    def local(self, t):
        return pltpu.make_async_copy(self.cols[t], self.block(t, self.spot.chip), self.own.at[t])

    def hop(self, t, k):
        spot = self.spot
        target = (spot.first, spot.second, spot.second)[k]
        source = self.cols[t] if k < 2 else self.block(t, spot.first)
        land = self.block(t, (spot.chip, spot.chip, spot.first)[k])
        return remote(source, land, self.hs.at[t, k], self.hr.at[t, k], spot.at_chip(target))

    def cross(self, t, k):
        spot = self.spot
        land = self.block(t, (spot.chip, spot.first, spot.second, spot.diagonal)[k])
        return remote(land if k else self.cols[t], land, self.cs.at[t, k], self.cr.at[t, k], spot.twin())

    def spread(self, t):
        self.hop(t, 0).start()
        self.hop(t, 1).start()
        self.cross(t, 0).start()
        self.local(t).start()

    def relay(self, t):
        self.hop(t, 0).wait_recv()
        self.hop(t, 2).start()
        self.cross(t, 1).start()
        self.hop(t, 1).wait_recv()
        self.cross(t, 2).start()

    def close(self, t):
        self.hop(t, 2).wait_recv()
        self.cross(t, 3).start()

    def finish(self, t):
        self.local(t).wait()
        for k in range(4):
            self.cross(t, k).wait_recv()

    def drain(self, t):
        for k in range(3):
            self.hop(t, k).wait_send()
        for k in range(4):
            self.cross(t, k).wait_send()


class Fold:
    def __init__(self, spot, parts, outs, bufs, sems):
        self.spot, self.parts, self.outs = spot, parts, outs
        count = len(parts)
        self.mine, self.twin_in, self.first_in, self.second_in, self.col, self.line_in = (
            bufs[i * count : (i + 1) * count] for i in range(6)
        )
        self.own, self.cs, self.cr, self.hs, self.hr, self.zs, self.zr = sems

    @staticmethod
    def buffers(shapes, nz):
        out = []
        for lead in ((4, nz), (4, nz), (2, nz), (nz,), (nz,), (nz - 1,)):
            out += [pltpu.VMEM(lead + tuple(shape), BF16) for shape in shapes]
        return out

    @staticmethod
    def sems(count, nz):
        return [dma(count, 4), dma(count, 4), dma(count, 4), dma(count, 3), dma(count, 3),
                dma(count, nz - 1), dma(count, nz - 1)]

    def local(self, t, k):
        spot = self.spot
        chip = (spot.chip, spot.first, spot.second, spot.diagonal)[k]
        return pltpu.make_async_copy(self.parts[t].at[:, chip, spot.core], self.mine[t].at[k], self.own.at[t, k])

    def cross(self, t, k):
        spot = self.spot
        chip = (spot.chip, spot.second, spot.first, spot.diagonal)[k]
        return remote(self.parts[t].at[:, chip, 1 - spot.core], self.twin_in[t].at[k], self.cs.at[t, k],
                      self.cr.at[t, k], spot.twin())

    def hop(self, t, k):
        spot = self.spot
        source = self.mine[t].at[(1, 3, 2)[k]]
        target = (self.first_in[t].at[0], self.first_in[t].at[1], self.second_in[t])[k]
        chip = (spot.first, spot.first, spot.second)[k]
        return remote(source, target, self.hs.at[t, k], self.hr.at[t, k], spot.at_chip(chip))

    def line(self, t, d):
        z = modulo(self.spot.z + d, self.spot.nz)
        return remote(self.col[t].at[z], self.line_in[t].at[d - 1], self.zs.at[t, d - 1], self.zr.at[t, d - 1],
                      self.spot.on_line(d))

    def start(self, t):
        for k in (3, 1, 2, 0):
            self.cross(t, k).start()
            self.local(t, k).start()

    def combine(self, t):
        mine, twin_in = self.mine[t], self.twin_in[t]
        for k in (3, 1, 2, 0):
            self.local(t, k).wait()
            self.cross(t, k).wait_recv()

            def add(i, carry):
                mine[k, i] = mine[k, i] + twin_in[k, i]
                return carry

            lax.fori_loop(0, self.spot.nz, add, 0)
            if k == 3:
                self.hop(t, 1).start()
            elif k == 1:
                self.hop(t, 0).start()

    def middle(self, t):
        mine, first_in = self.mine[t], self.first_in[t]
        self.hop(t, 1).wait_recv()

        def add(i, carry):
            mine[2, i] = mine[2, i] + first_in[1, i]
            return carry

        lax.fori_loop(0, self.spot.nz, add, 0)
        self.hop(t, 2).start()

    def column(self, t):
        mine, first_in, second_in, col = self.mine[t], self.first_in[t], self.second_in[t], self.col[t]
        self.hop(t, 0).wait_recv()
        self.hop(t, 2).wait_recv()

        def add(i, carry):
            total = mine[0, i].astype(F32) + first_in[0, i].astype(F32) + second_in[i].astype(F32)
            col[i] = total.astype(BF16)
            return carry

        lax.fori_loop(0, self.spot.nz, add, 0)
        for d in range(1, self.spot.nz):
            self.line(t, d).start()

    def finish(self, t):
        total = self.col[t][self.spot.z].astype(F32)
        for d in range(1, self.spot.nz):
            self.line(t, d).wait_recv()
        for d in range(self.spot.nz - 1):
            total = total + self.line_in[t][d].astype(F32)
        self.outs[t][...] = total

    def drain(self, t):
        for k in range(4):
            self.cross(t, k).wait_send()
        for k in range(3):
            self.hop(t, k).wait_send()
        for d in range(1, self.spot.nz):
            self.line(t, d).wait_send()


class AllSum:
    def __init__(self, spot, source, bufs):
        self.spot, self.source = spot, source
        self.line_in, self.col, self.plane_in, self.pair, self.twin_in, self.ss, self.rs = bufs

    @staticmethod
    def scratch(shape, nz):
        return [pltpu.VMEM((nz - 1,) + shape, F32), pltpu.VMEM(shape, F32), pltpu.VMEM((3,) + shape, F32),
                pltpu.VMEM(shape, F32), pltpu.VMEM(shape, F32), dma(3 + nz), dma(3 + nz)]

    def cross(self):
        return remote(self.pair, self.twin_in, self.ss.at[0], self.rs.at[0], self.spot.twin())

    def hop(self, k):
        chip = (self.spot.first, self.spot.second, self.spot.diagonal)[k]
        return remote(self.col, self.plane_in.at[k], self.ss.at[1 + k], self.rs.at[1 + k],
                      self.spot.at_chip(chip))

    def line(self, d):
        return remote(self.source, self.line_in.at[d - 1], self.ss.at[3 + d], self.rs.at[3 + d],
                      self.spot.on_line(d))

    def start(self):
        for d in range(1, self.spot.nz):
            self.line(d).start()

    def plane(self):
        out = self.source[...]
        for d in range(1, self.spot.nz):
            self.line(d).wait_recv()
        for d in range(self.spot.nz - 1):
            out = out + self.line_in[d]
        self.col[...] = out
        for k in range(3):
            self.hop(k).start()

    def column(self):
        for k in range(3):
            self.hop(k).wait_recv()
        self.pair[...] = self.col[...] + self.plane_in[0] + self.plane_in[1] + self.plane_in[2]
        self.cross().start()

    def total(self):
        self.cross().wait_recv()
        return self.pair[...] + self.twin_in[...]

    def drain(self):
        self.cross().wait_send()
        for k in range(3):
            self.hop(k).wait_send()
        for d in range(1, self.spot.nz):
            self.line(d).wait_send()


HALVES = 2


class Exchange:
    def __init__(self, spot, sources, lands, ss, rs):
        self.spot, self.sources, self.lands, self.ss, self.rs = spot, sources, lands, ss, rs

    @staticmethod
    def sems(nseq):
        return [dma(HALVES, nseq - 1), dma(HALVES, nseq - 1)]

    def copies(self, h, source, target):
        spot = self.spot
        out = []
        for d in range(1, spot.nseq):
            s = modulo(spot.seq + d, spot.nseq)
            out.append(remote(source(s), target(d), self.ss.at[h, d - 1], self.rs.at[h, d - 1], (spot.z, s)))
        return out

    def spread(self, h):
        return self.copies(h, lambda s: self.sources[h], lambda d: self.lands[h].at[self.spot.seq])

    def collect(self, h):
        return self.copies(h, lambda s: self.sources[h].at[s], lambda d: self.lands[h].at[d - 1])


def begin(copies):
    for copy in copies:
        copy.start()


def complete(copies):
    for copy in copies:
        copy.wait()


def when(condition, *actions):
    @pl.when(condition)
    def _():
        for action in actions:
            action()


def does(method, *args):
    return lambda: method(*args)


def log2(value):
    assert value & (value - 1) == 0
    return value.bit_length() - 1


def row_picker(b, batch, spans, nseq):
    shape = (nseq * spans, nseq * batch * spans)
    r = lax.broadcasted_iota(jnp.int32, shape, 0)
    c = lax.broadcasted_iota(jnp.int32, shape, 1)
    shift = log2(spans)
    place_of = (r >> shift) * (batch * spans) + b * spans + (r & (spans - 1))
    return jnp.where(c == place_of, 1.0, 0.0).astype(BF16)


def span_adder(b, batch, spans, tokens):
    shape = (batch * spans, tokens)
    r = lax.broadcasted_iota(jnp.int32, shape, 0)
    t = lax.broadcasted_iota(jnp.int32, shape, 1)
    return jnp.where(r == b * spans + (t >> log2(SPAN)), 1.0, 0.0).astype(BF16)


def whole_weight(ref, cols):
    block = ref[:, :, :, cols]
    return block.reshape((-1, block.shape[-1]))


def send_means(exchange, h, own_acc):
    rows = own_acc.shape[0] // HALVES
    exchange.sources[h][...] = (own_acc[h * rows : (h + 1) * rows] * (1.0 / SPAN)).astype(BF16)
    begin(exchange.spread(h))
    exchange.lands[h][exchange.spot.seq] = exchange.sources[h][...]


def pick_sums(b, counts, nseq, land):
    batch, spans = counts
    every = land.reshape((-1, land.shape[-1]))
    return dot(row_picker(b, batch // HALVES, spans, nseq), every).astype(BF16)


QKV_ORDER = (1, 2, 0)
PARTS = len(QKV_ORDER)
U_CUTS = 2


def enter_kernel(counts, *refs):
    batch, spans = counts
    (x_ref, bias_ref, gain_own, wq_sh, wo_sh, wu_sh, wd_sh,
     qkv_ref, sums_ref, prob_ref, o_ref, gains_ref, fk, fv, fq, fo, fu, fd, cq, cu, cd, co,
     n_all, qkv_all, own_acc, own_a, own_b, land_a, land_b, ik, iv, iq, out_sem, qkv_sem, ex_s, ex_r) = refs[:36]
    rest = refs[36:]
    spot = Spot()
    wide = wu_sh.shape[-1] // U_CUTS
    cuts = [slice(i * wide, (i + 1) * wide) for i in range(U_CUTS)]
    shards = [wq_sh.at[0, :, part * D : (part + 1) * D] for part in QKV_ORDER]
    shards += [wo_sh.at[0]] + [wu_sh.at[0, :, cols] for cols in cuts] + [wd_sh.at[0]]
    cols = list(rest[:7])
    lines = Lines(spot, shards + [wq_sh.at[1], wu_sh.at[1], wd_sh.at[1], wo_sh.at[1]], cols + [cq, cu, cd, co],
                  rest[7:10])
    plane = Plane(spot, cols, [ik, iv, iq, fo] + [fu.at[:, :, :, c] for c in cuts] + [fd], rest[10:15])
    adder = AllSum(spot, gain_own, rest[15:])
    exchange = Exchange(spot, [own_a, own_b], [land_a, land_b], ex_s, ex_r)
    k0, v0, q0, o0, ua, ub, d0 = range(7)
    inner, outer = (ik, iv, iq), (fk, fv, fq)
    step = pl.program_id(0)
    tokens = x_ref.shape[1]
    half = batch // HALVES
    first = PARTS + 1

    def keep(t):
        return pltpu.make_async_copy(inner[t], outer[t], out_sem.at[t])

    def record(b):
        return pltpu.make_async_copy(qkv_all.at[b], qkv_ref.at[b], qkv_sem.at[b])

    def spread(t):
        lines.arrive(t)
        plane.spread(t)

    def settle(t):
        plane.close(t)
        plane.finish(t)
        keep(t).start()

    @pl.when(step == 0)
    def _():
        spot.signal()
        own_acc[...] = jnp.zeros_like(own_acc)
        spot.meet()
        adder.start()
        for t in range(11):
            lines.start(t)
        adder.plane()
        spread(k0)
        spread(v0)
        adder.column()
        spread(q0)
        plane.relay(k0)
        spread(o0)
        plane.relay(v0)
        gains_ref[...] = adder.total()

        def norm(b, carry):
            unit, _ = normed(x_ref[b].astype(F32))
            n_all[b] = (unit * gains_ref[0:1]).astype(BF16)
            return carry

        lax.fori_loop(0, batch // 2, norm, 0)
        plane.relay(q0)
        lax.fori_loop(batch // 2, batch, norm, 0)
        settle(k0)

    @pl.when(step == 2)
    def _():
        plane.relay(o0)
        spread(ua)
        settle(v0)

    @pl.when(step == 3)
    def _():
        spread(ub)
        plane.relay(ua)
        settle(q0)

    for at, part in enumerate(QKV_ORDER):

        @pl.when(step == 1 + at)
        def _(at=at, part=part):
            weight = inner[at]

            def project(b, carry):
                block = dot(n_all[b], weight[...].reshape((D, D))).astype(BF16)
                qkv_all[b, :, part * D : (part + 1) * D] = block
                if part > 0:
                    pick = span_adder(b, batch, spans, tokens)
                    own_acc[:, (part - 1) * D : part * D] += dot(pick, block)
                return carry

            lax.fori_loop(0, batch, project, 0)

    @pl.when(step == 2)
    def _():
        send_means(exchange, 0, own_acc)
        send_means(exchange, 1, own_acc)

    @pl.when(step == first)
    def _():
        complete(exchange.spread(0))
        complete(exchange.spread(1))
        for b in range(batch):
            record(b).start()
        spread(d0)
        plane.close(o0)

    when(step == first + 2, does(plane.relay, ub), does(plane.finish, o0))
    when(step == first + 3, does(plane.close, ua))
    when(step == first + 6, does(plane.relay, d0), does(plane.finish, ua))
    when(step == first + 7, does(plane.close, ub))

    @pl.when(jnp.logical_and(step >= first, step < first + half))
    def _():
        sums_ref[0] = pick_sums(step - first, counts, spot.nseq, land_a[...])

    @pl.when(step >= first + half)
    def _():
        sums_ref[0] = pick_sums(step - first - half, counts, spot.nseq, land_b[...])

    @pl.when(step >= first)
    def _():
        attention_forward(qkv_all.at[pl.ds(step - first, 1)], sums_ref, bias_ref, prob_ref, o_ref)

    @pl.when(step == first + batch - 1)
    def _():
        plane.close(d0)
        plane.finish(ub)
        for t in range(7, 11):
            lines.arrive(t)
        plane.finish(d0)
        for t in range(PARTS):
            keep(t).wait()
        for b in range(batch):
            record(b).wait()
        for t in range(11):
            lines.drain(t)
        for t in range(7):
            plane.drain(t)
        adder.drain()


def phased(shape, start, count):
    rest = len(shape) - 1
    return pl.BlockSpec((1,) + tuple(shape[1:]),
                        lambda i: (jnp.clip(i - start, 0, count - 1),) + (0,) * rest)


def anywhere():
    return pl.BlockSpec(memory_space=pl.ANY)


def fused_params(collective_id):
    return pltpu.CompilerParams(dimension_semantics=("arbitrary",), vmem_limit_bytes=VMEM_LIMIT,
                                collective_id=collective_id, has_side_effects=True)


def full_shape(shape):
    return sds((lax.axis_size("dp"), lax.axis_size("seq")) + tuple(shape), BF16)


def col_shape(weights):
    return sds((lax.axis_size("dp"),) + weights.shape[1:], BF16)


def exchange_buffers(nseq, rows):
    own = pltpu.VMEM((rows // HALVES, 2 * D), BF16)
    land = pltpu.VMEM((nseq, rows // HALVES, 2 * D), BF16)
    return [own, own, land, land]


def call_enter(x, bias, gain_own, wq, wo, wu, wd):
    batch, tokens, _ = x.shape
    spans = tokens // SPAN
    nz, nseq = lax.axis_size("dp"), lax.axis_size("seq")
    rows = batch * spans
    keys = SPAN + nseq * spans
    own_rows = wq.shape[1]
    square = full_shape((own_rows, D))
    outs = [sds((batch, tokens, 3 * D), BF16), sds((batch, nseq * spans, 2 * D), BF16),
            sds((batch, spans, PAIRS, keys, 2 * SPAN), BF16), sds((batch, tokens, D), BF16),
            sds(gain_own.shape, F32)] + [square] * PARTS + [full_shape(w.shape[1:]) for w in (wo, wu, wd)]
    outs += [col_shape(w) for w in (wq, wu, wd, wo)]
    cols = [(own_rows, D)] * (PARTS + 1) + [(own_rows, wu.shape[2] // U_CUTS)] * U_CUTS + [wd.shape[1:]]
    first = PARTS + 1
    return pl.pallas_call(
        functools.partial(enter_kernel, (batch, spans)),
        grid=(first + batch,),
        in_specs=[whole(x.shape), phased(bias.shape, first, batch)]
        + [whole(a.shape) for a in (gain_own, wq, wo, wu, wd)],
        out_specs=[anywhere()] + [phased(o.shape, first, batch) for o in outs[1:4]]
        + [whole(gain_own.shape)] + [anywhere()] * (PARTS + 7),
        out_shape=outs,
        scratch_shapes=[pltpu.VMEM(x.shape, BF16), pltpu.VMEM((batch, tokens, 3 * D), BF16),
                        pltpu.VMEM((rows, 2 * D), F32)]
        + exchange_buffers(nseq, rows) + [pltpu.VMEM(square.shape, BF16)] * PARTS
        + [dma(PARTS), dma(batch)] + Exchange.sems(nseq)
        + [pltpu.VMEM((nz,) + tuple(c), BF16) for c in cols]
        + Lines.sems(11, nz) + Plane.sems(7) + AllSum.scratch(gain_own.shape, nz),
        compiler_params=fused_params(0),
        name="enter",
    )(x, bias, gain_own, wq, wo, wu, wd)


def mid_kernel(counts, *refs):
    batch, spans = counts
    (x_ref, o_ref, gains_ref, wo_ref, wu_ref, wd_ref, cq, cu, cd, co,
     h_ref, u_ref, next_ref, qkv_ref, raw_ref, fq, fo, fu, fd,
     next_all, own_acc, own_a, own_b, land_a, land_b, wq_in, wq_sem, ex_s, ex_r) = refs[:29]
    spot = Spot()
    plane = Plane(spot, [cq, cu, cd, co], [wq_in, fu, fd, fo], refs[29:])
    exchange = Exchange(spot, [own_a, own_b], [land_a, land_b], ex_s, ex_r)
    q1, u1, d1, o1 = range(4)
    step = pl.program_id(0)
    keep = pltpu.make_async_copy(wq_in, fq, wq_sem)

    @pl.when(step == 0)
    def _():
        spot.signal()
        own_acc[...] = jnp.zeros_like(own_acc)

    @pl.when(step < batch)
    def _():
        hidden = x_ref[0].astype(F32) + dot(o_ref[0], wo_ref[...])
        h_ref[0] = hidden
        when(step == 0, does(spot.meet), does(plane.spread, q1), does(plane.spread, u1))
        result = mlp_forward(hidden, gains_ref[2:3], wu_ref, wd_ref, u_ref)
        next_ref[0] = result
        next_all[step] = result

    when(step == 3, does(plane.relay, q1), does(plane.spread, d1))
    when(step == 5, does(plane.relay, u1), does(plane.spread, o1))
    when(step == 6, does(plane.close, q1))
    when(step == batch, does(plane.finish, q1), does(keep.start), does(plane.relay, d1))
    when(step == batch + 1, does(plane.close, u1))
    when(step == batch + 2, does(plane.relay, o1))
    when(step == batch + 5, does(plane.close, d1), does(plane.finish, u1))
    when(step == batch + 6, does(plane.close, o1))

    @pl.when(step >= batch)
    def _():
        unit, _ = normed(next_all[step - batch])
        n_one = (unit * gains_ref[1:2]).astype(BF16)
        pick = span_adder(step - batch, batch, spans, x_ref.shape[1])
        for part in (1, 2, 0):
            cols = slice(part * D, (part + 1) * D)
            block = dot(n_one, whole_weight(wq_in, cols)).astype(BF16)
            qkv_ref[0, :, cols] = block
            if part > 0:
                own_acc[:, (part - 1) * D : part * D] += dot(pick, block)

    when(step == batch + batch // HALVES - 1, does(send_means, exchange, 0, own_acc))

    @pl.when(step == 2 * batch - 1)
    def _():
        send_means(exchange, 1, own_acc)
        plane.finish(d1)
        plane.finish(o1)
        keep.wait()
        for t in range(4):
            plane.drain(t)
        complete(exchange.spread(0))
        raw_ref[0] = land_a[...]
        complete(exchange.spread(1))
        raw_ref[1] = land_b[...]


def call_mid(x, o, gains, wo, wu, wd, cq, cu, cd, co):
    batch, tokens, _ = x.shape
    spans = tokens // SPAN
    nseq = lax.axis_size("seq")
    rows = batch * spans
    outs = [sds((batch, tokens, D), F32), sds((batch, tokens, wu.shape[1]), BF16), sds((batch, tokens, D), F32),
            sds((batch, tokens, 3 * D), BF16), sds((HALVES, nseq, rows // HALVES, 2 * D), BF16)]
    outs += [full_shape(c.shape[1:]) for c in (cq, co, cu, cd)]
    args = [x, o, gains, wo, wu, wd, cq, cu, cd, co]
    return pl.pallas_call(
        functools.partial(mid_kernel, (batch, spans)),
        grid=(2 * batch,),
        in_specs=[phased(a.shape, 0, batch) for a in args[:2]] + [whole(a.shape) for a in args[2:]],
        out_specs=[phased(a.shape, 0, batch) for a in outs[:3]] + [phased(outs[3].shape, batch, batch)]
        + [whole(outs[4].shape)] + [anywhere()] * 4,
        out_shape=outs,
        scratch_shapes=[pltpu.VMEM(x.shape, F32), pltpu.VMEM((rows, 2 * D), F32)] + exchange_buffers(nseq, rows)
        + [pltpu.VMEM(outs[5].shape, BF16), pltpu.SemaphoreType.DMA] + Exchange.sems(nseq) + Plane.sems(4),
        compiler_params=fused_params(1),
        name="mid",
    )(*args)


TEAM = 2


def flat_rows(ref):
    return ref[...].reshape((-1, ref.shape[-1]))


def per_team(shape):
    rest = len(shape) - 1
    return pl.BlockSpec((TEAM,) + tuple(shape[1:]), lambda b: (b,) + (0,) * rest)


def top_kernel(counts, x_ref, qkv_ref, bias_ref, raw_ref, gains_ref, wo_ref, wu_ref, wd_ref,
               sums_ref, prob_ref, o_ref, h_ref, u_ref, next_ref):
    batch, spans, nseq = counts
    half = batch // HALVES
    for i in range(TEAM):
        b, one = pl.program_id(0) * TEAM + i, pl.ds(i, 1)
        sums_ref[i] = pick_sums(lax.rem(b, half), (batch, spans), nseq, raw_ref[lax.div(b, half)])
        attention_forward(qkv_ref.at[one], sums_ref.at[one], bias_ref.at[one], prob_ref.at[one], o_ref.at[one])
    hidden = flat_rows(x_ref) + dot(flat_rows(o_ref), wo_ref[...])
    h_ref[...] = hidden.reshape(h_ref.shape)
    result = mlp_forward(hidden, gains_ref[3:4], wu_ref, wd_ref, u_ref)
    next_ref[...] = result.reshape(next_ref.shape).astype(next_ref.dtype)


def call_top(x, qkv, bias, raw, gains, wo, wu, wd):
    batch, tokens, _ = x.shape
    spans = tokens // SPAN
    nseq = raw.shape[1]
    outs = [sds((batch, nseq * spans, 2 * D), BF16),
            sds((batch, spans, PAIRS, SPAN + nseq * spans, 2 * SPAN), BF16), sds((batch, tokens, D), BF16),
            sds((batch, tokens, D), F32), sds((batch, tokens, wu.shape[1]), BF16), sds((batch, tokens, D), BF16)]
    args = [x, qkv, bias, raw, gains, wo, wu, wd]
    return pl.pallas_call(
        functools.partial(top_kernel, (batch, spans, nseq)),
        grid=(batch // TEAM,),
        in_specs=[per_team(a.shape) for a in args[:3]] + [whole(a.shape) for a in args[3:]],
        out_specs=[per_team(a.shape) for a in outs],
        out_shape=outs,
        compiler_params=params(),
        name="top",
    )(*args)


def mlp_back(dy32, u_ref, h_ref, o_ref, gain, wo_ref, wu_ref, wd_ref, dh_ref, gd_ref, gu_ref, go_ref, gg_ref):
    ddown = dy32.astype(BF16)
    unit, rstd = normed(flat_rows(h_ref))
    n_two = (unit * gain).astype(BF16)
    dn_two = 0.0
    for start in range(0, wu_ref.shape[1], CHUNK):
        cols = slice(start, start + CHUNK)
        dactive = dot(ddown, wd_ref[cols, :], NT)
        active, slope = gelu_both(u_ref[:, :, cols].reshape((-1, CHUNK)).astype(F32))
        gd_ref[cols, :] += dot(active.astype(BF16), ddown, TN)
        dupper = (dactive * slope).astype(BF16)
        gu_ref[:, cols] += dot(n_two, dupper, TN)
        dn_two = dn_two + dot(dupper, wu_ref[:, cols], NT)
    dnorm, grad_gain = norm_backward(dn_two, unit, rstd, gain)
    gg_ref[...] += grad_gain
    dhidden = dy32 + dnorm
    dh_ref[...] = dhidden.reshape(dh_ref.shape)
    dattn = dhidden.astype(BF16)
    go_ref[...] += dot(flat_rows(o_ref), dattn, TN)
    return dot(dattn, wo_ref[...], NT).astype(BF16)


def pile(b, counts, nseq, dsums_ref, part_acc):
    batch, spans = counts
    local = lax.rem(b, batch // HALVES)
    part_acc[...] += dot(row_picker(local, batch // HALVES, spans, nseq), dsums_ref[0], TN)


def ship(exchange, h, part_acc):
    source = exchange.sources[h]
    source[...] = part_acc[...].astype(BF16).reshape(source.shape)
    part_acc[...] = jnp.zeros_like(part_acc)
    begin(exchange.collect(h))


def gathered(exchange, h, total_ref):
    spot = exchange.spot
    complete(exchange.collect(h))
    total = exchange.sources[h][spot.seq].astype(F32)
    for d in range(spot.nseq - 1):
        total = total + exchange.lands[h][d].astype(F32)
    rows = total.shape[0]
    total_ref[h * rows : (h + 1) * rows] = total


def collect_buffers(nseq, rows):
    part = pltpu.VMEM((nseq, rows // HALVES, 2 * D), BF16)
    land = pltpu.VMEM((nseq - 1, rows // HALVES, 2 * D), BF16)
    return [pltpu.VMEM((nseq * rows // HALVES, 2 * D), F32), part, part, land, land]


def zero(*refs):
    for ref in refs:
        ref[...] = jnp.zeros_like(ref)


def base_kernel(counts, *refs):
    batch, spans = counts
    (dy_ref, u_ref, h_ref, o_ref, prob_ref, qkv_ref, sums_ref, gains_ref, wo_ref, wu_ref, wd_ref,
     dh_ref, dqkv_ref, total_ref, gd_out, gu_out, go_out, gg_ref,
     gd_ref, gu_ref, go_ref, dsums, part_acc, part_a, part_b, land_a, land_b, ex_s, ex_r) = refs
    spot = Spot()
    exchange = Exchange(spot, [part_a, part_b], [land_a, land_b], ex_s, ex_r)
    step = pl.program_id(0)

    @pl.when(step == 0)
    def _():
        spot.signal()
        zero(gd_ref, gu_ref, go_ref, gg_ref, part_acc)

    dout = mlp_back(flat_rows(dy_ref).astype(F32), u_ref, h_ref, o_ref, gains_ref[3:4], wo_ref, wu_ref, wd_ref,
                    dh_ref, gd_ref, gu_ref, go_ref, gg_ref)
    tokens = dy_ref.shape[1]
    for i in range(TEAM):
        one = pl.ds(i, 1)
        attention_backward(qkv_ref.at[one], sums_ref.at[one], prob_ref.at[one], dout[i * tokens : (i + 1) * tokens],
                           dqkv_ref.at[one], dsums)
        pile(step * TEAM + i, counts, spot.nseq, dsums, part_acc)

    @pl.when(step == batch // HALVES // TEAM - 1)
    def _():
        spot.meet()
        ship(exchange, 0, part_acc)

    @pl.when(step == batch // TEAM - 1)
    def _():
        ship(exchange, 1, part_acc)
        gd_out[...] = gd_ref[...].astype(BF16)
        gu_out[...] = gu_ref[...].astype(BF16)
        go_out[...] = go_ref[...].astype(BF16)
        gathered(exchange, 0, total_ref)
        gathered(exchange, 1, total_ref)


def call_base(dy, u, h, o, prob, qkv, sums, gains, wo, wu, wd):
    batch, tokens, _ = dy.shape
    spans = tokens // SPAN
    nseq = lax.axis_size("seq")
    rows = batch * spans
    args = [dy, u, h, o, prob, qkv, sums, gains, wo, wu, wd]
    outs = [sds(h.shape, F32), sds(qkv.shape, BF16), sds((rows, 2 * D), F32), sds(wd.shape, BF16),
            sds(wu.shape, BF16), sds(wo.shape, BF16), sds((1, D), F32)]
    return pl.pallas_call(
        functools.partial(base_kernel, (batch, spans)),
        grid=(batch // TEAM,),
        in_specs=[per_team(a.shape) for a in args[:7]] + [whole(a.shape) for a in args[7:]],
        out_specs=[per_team(a.shape) for a in outs[:2]] + [whole(a.shape) for a in outs[2:]],
        out_shape=outs,
        scratch_shapes=[pltpu.VMEM(wd.shape, F32), pltpu.VMEM(wu.shape, F32), pltpu.VMEM(wo.shape, F32),
                        pltpu.VMEM((1, nseq * spans, 2 * D), BF16)]
        + collect_buffers(nseq, rows) + Exchange.sems(nseq),
        compiler_params=fused_params(2),
        name="base",
    )(*args)


def qkv_back(unit, rstd, gain, near, share, dh, weight, gq, gg_ref, skip=()):
    n_one = (unit * gain).astype(BF16)
    dn_one = 0.0
    for part in range(3):
        cols = slice(part * D, (part + 1) * D)
        block = near(cols)
        if part > 0:
            pieces = []
            for span in range(unit.shape[0] // SPAN):
                row = share(span, slice((part - 1) * D, part * D)) * (1.0 / SPAN)
                pieces.append(block[span * SPAN : (span + 1) * SPAN].astype(F32) + row)
            block = jnp.concatenate(pieces, 0).astype(BF16)
        if part not in skip:
            gq[part][...] += dot(n_one, block, TN)
        dn_one = dn_one + dot(block, weight(cols), NT)
    dnorm, grad_gain = norm_backward(dn_one, unit, rstd, gain)
    gg_ref[...] += grad_gain
    return dh + dnorm


def turn_kernel(counts, *refs):
    batch, spans = counts
    (x_ref, near_ref, dh_ref, u_ref, h_ref, o_ref, total_ref, gains_ref, wq_ref, wo_ref, wu_ref, wd_ref,
     pd, pu, po,
     dh_out, dout_out, gd_out, gu_out, go_out, ggq_ref, gg_ref, sd, su, so, sq,
     dx_all, gq_ref, gd_ref, gu_ref, go_ref, gq_low) = refs[:32]
    rest = refs[32:]
    spot = Spot()
    fold = Fold(spot, [pd, pu, po, gq_low], [sd, su, so, sq], rest[:24], rest[24:])
    d1, u1, o1, q1 = range(4)
    step = pl.program_id(0)

    @pl.when(step == 0)
    def _():
        spot.signal()
        zero(gq_ref, gd_ref, gu_ref, go_ref, gg_ref, ggq_ref)

    @pl.when(step == 1)
    def _():
        spot.meet()
        for t in range(3):
            fold.start(t)

    when(step == 4, does(fold.combine, d1))
    when(step == 5, does(fold.combine, u1))
    when(step == 6, does(fold.combine, o1))

    @pl.when(step == batch)
    def _():
        gq_low[...] = gq_ref[...].astype(BF16).reshape(gq_low.shape)
        fold.start(q1)
        fold.middle(d1)

    when(step == batch + 1, does(fold.middle, u1), does(fold.middle, o1), does(fold.combine, q1))
    when(step == batch + 2, does(fold.column, d1))
    when(step == batch + 3, does(fold.column, u1), does(fold.column, o1), does(fold.middle, q1))
    when(step == batch + 4, does(fold.column, q1))
    when(step == batch + 5, does(fold.finish, d1))
    when(step == batch + 6, does(fold.finish, u1), does(fold.finish, o1))
    when(step == batch + 7, does(fold.finish, q1))

    @pl.when(step < batch)
    def _():
        unit, rstd = normed(x_ref[0])
        dx_all[step] = qkv_back(
            unit, rstd, gains_ref[1:2], lambda cols: near_ref[0, :, cols],
            lambda span, cols: total_ref[pl.ds(step * spans + span, 1), cols], dh_ref[0],
            lambda cols: wq_ref[:, cols], [gq_ref.at[:, part * D : (part + 1) * D] for part in range(3)], ggq_ref)

    @pl.when(step >= batch)
    def _():
        dout_out[0] = mlp_back(dx_all[step - batch], u_ref, h_ref, o_ref, gains_ref[2:3], wo_ref, wu_ref, wd_ref,
                               dh_out, gd_ref, gu_ref, go_ref, gg_ref)

    @pl.when(step == 2 * batch - 1)
    def _():
        gd_out[...] = gd_ref[...].astype(BF16)
        gu_out[...] = gu_ref[...].astype(BF16)
        go_out[...] = go_ref[...].astype(BF16)
        for t in range(4):
            fold.drain(t)


def by_owner(part):
    nz, nseq = lax.axis_size("dp"), lax.axis_size("seq")
    return part.reshape((nz, nseq // CORES, CORES, part.shape[0] // (nz * nseq)) + part.shape[1:])


def call_turn(x, near, dh, u, h, o, total, gains, wq, wo, wu, wd, pd, pu, po):
    batch, tokens, _ = x.shape
    nz = lax.axis_size("dp")
    parts = [by_owner(a) for a in (pd, pu, po)]
    owned = by_owner(sds_like(wq))
    shapes = [a.shape[3:] for a in parts] + [owned.shape[3:]]
    args = [x, near, dh, u, h, o, total, gains, wq, wo, wu, wd] + parts
    outs = [sds(h.shape, F32), sds(o.shape, BF16), sds(wd.shape, BF16), sds(wu.shape, BF16), sds(wo.shape, BF16),
            sds((1, D), F32), sds((1, D), F32)] + [sds(s, F32) for s in shapes]
    return pl.pallas_call(
        functools.partial(turn_kernel, (batch, tokens // SPAN)),
        grid=(2 * batch,),
        in_specs=[phased(a.shape, 0, batch) for a in args[:3]] + [phased(a.shape, batch, batch) for a in args[3:6]]
        + [whole(a.shape) for a in args[6:12]] + [anywhere()] * 3,
        out_specs=[phased(a.shape, batch, batch) for a in outs[:2]] + [whole(a.shape) for a in outs[2:]],
        out_shape=outs,
        scratch_shapes=[pltpu.VMEM(x.shape, F32), pltpu.VMEM(wq.shape, F32), pltpu.VMEM(wd.shape, F32),
                        pltpu.VMEM(wu.shape, F32), pltpu.VMEM(wo.shape, F32), pltpu.VMEM(owned.shape, BF16)]
        + Fold.buffers(shapes, nz) + Fold.sems(4, nz),
        compiler_params=fused_params(3),
        name="turn",
    )(*args)


def sds_like(a):
    class Shaped:
        shape = a.shape

        def reshape(self, shape):
            return sds(shape, a.dtype)

    return Shaped()


def leave_kernel(counts, *refs):
    batch, spans = counts
    (prob_ref, qkv_ref, sums_ref, dout_ref, x_ref, dh_ref, gains_ref, w0, w1, w2, g_mlp0, g_attn1, g_mlp1,
     pd, pu, po,
     dx_ref, gsum_ref, sd, su, so, s0, s1, s2,
     near_all, unit_all, rstd_all, a0, a1, a2, l0, l1, l2, gg_ref, gain_src, dsums,
     part_acc, part_a, part_b, land_a, land_b, total, ex_s, ex_r) = refs[:44]
    rest = refs[44:]
    spot = Spot()
    fold = Fold(spot, [pd, pu, po, l0, l1, l2], [sd, su, so, s0, s1, s2], rest[:36], rest[36:43])
    adder = AllSum(spot, gain_src, rest[43:])
    exchange = Exchange(spot, [part_a, part_b], [land_a, land_b], ex_s, ex_r)
    d0, u0, o0, q0, k0, v0 = range(6)
    step = pl.program_id(0)
    half = batch // HALVES

    def pour(acc, low):
        low[...] = acc[...].astype(BF16).reshape(low.shape)

    @pl.when(step == 0)
    def _():
        spot.signal()
        zero(a0, a1, a2, gg_ref, part_acc)

    @pl.when(step == 1)
    def _():
        spot.meet()
        for t in range(3):
            fold.start(t)

    when(step == 2, does(fold.combine, d0))
    when(step == half + 1, does(fold.middle, d0), does(fold.combine, u0), does(fold.combine, o0))
    when(step == batch - 1, does(fold.column, d0))

    @pl.when(step == batch)
    def _():
        pour(a0, l0)
        fold.start(q0)
        gathered(exchange, 0, total)

    when(step == batch + 2, does(fold.middle, u0), does(fold.combine, q0))
    when(step == batch + 3, does(fold.middle, o0))
    when(step == batch + half, does(gathered, exchange, 1, total))
    when(step == batch + 5, does(fold.column, u0))
    when(step == batch + 6, does(fold.column, o0), does(fold.middle, q0))
    when(step == batch + 7, does(fold.finish, d0), does(fold.column, q0))

    @pl.when(step < batch)
    def _():
        near = near_all.at[pl.ds(step, 1)]
        attention_backward(qkv_ref, sums_ref, prob_ref, dout_ref[0], near, dsums)
        pile(step, counts, spot.nseq, dsums, part_acc)
        unit, rstd = normed(x_ref[0].astype(F32))
        unit_all[step] = unit
        rstd_all[step] = rstd
        a0[...] += dot((unit * gains_ref[0:1]).astype(BF16), near_all[step, :, :D], TN)

    when(step == half - 1, does(ship, exchange, 0, part_acc))
    when(step == batch - 1, does(ship, exchange, 1, part_acc))

    @pl.when(step >= batch)
    def _():
        b = step - batch
        dx_ref[0] = qkv_back(
            unit_all[b], rstd_all[b], gains_ref[0:1], lambda cols: near_all[b, :, cols],
            lambda span, cols: total[pl.ds(b * spans + span, 1), cols], dh_ref[0],
            lambda cols: (w0, w1, w2)[cols.start // D][...], [a0, a1, a2], gg_ref, (0,))

    @pl.when(step == 2 * batch - 1)
    def _():
        pour(a1, l1)
        fold.start(k0)
        pour(a2, l2)
        fold.start(v0)
        gain_src[...] = jnp.zeros_like(gain_src)
        gain_src[0:1] = gg_ref[...]
        gain_src[1:2] = g_attn1[...]
        gain_src[2:3] = g_mlp0[...]
        gain_src[3:4] = g_mlp1[...]
        adder.start()
        fold.combine(k0)
        fold.combine(v0)
        adder.plane()
        fold.finish(u0)
        fold.finish(o0)
        fold.middle(k0)
        fold.middle(v0)
        adder.column()
        fold.column(k0)
        fold.column(v0)
        fold.finish(q0)
        gsum_ref[...] = adder.total()
        fold.finish(k0)
        fold.finish(v0)
        for t in range(6):
            fold.drain(t)
        adder.drain()


def call_leave(prob, qkv, sums, dout, x, dh, gains, w0, w1, w2, g_mlp0, g_attn1, g_mlp1, pd, pu, po):
    batch, tokens, _ = x.shape
    spans = tokens // SPAN
    nz, nseq = lax.axis_size("dp"), lax.axis_size("seq")
    rows = batch * spans
    parts = [by_owner(a) for a in (pd, pu, po)]
    square = (D, D)
    owned = (nz, nseq // CORES, CORES, D // (nz * nseq), D)
    shapes = [a.shape[3:] for a in parts] + [owned[3:]] * 3
    args = [prob, qkv, sums, dout, x, dh, gains, w0, w1, w2, g_mlp0, g_attn1, g_mlp1] + parts
    outs = [sds(dh.shape, F32), sds(gains.shape, F32)] + [sds(s, F32) for s in shapes]
    return pl.pallas_call(
        functools.partial(leave_kernel, (batch, spans)),
        grid=(2 * batch,),
        in_specs=[phased(a.shape, 0, batch) for a in args[:5]] + [phased(dh.shape, batch, batch)]
        + [whole(a.shape) for a in args[6:13]] + [anywhere()] * 3,
        out_specs=[phased(outs[0].shape, batch, batch)] + [whole(a.shape) for a in outs[1:]],
        out_shape=outs,
        scratch_shapes=[pltpu.VMEM(qkv.shape, BF16), pltpu.VMEM(x.shape, F32), pltpu.VMEM((batch, tokens, 1), F32)]
        + [pltpu.VMEM(square, F32)] * 3 + [pltpu.VMEM(owned, BF16)] * 3
        + [pltpu.VMEM((1, D), F32), pltpu.VMEM(gains.shape, F32), pltpu.VMEM((1, nseq * spans, 2 * D), BF16)]
        + collect_buffers(nseq, rows) + [pltpu.VMEM((rows, 2 * D), F32)] + Exchange.sems(nseq)
        + Fold.buffers(shapes, nz) + Fold.sems(6, nz) + AllSum.scratch(gains.shape, nz),
        compiler_params=fused_params(4),
        name="leave",
    )(*args)


def pack_kernel(plan, *refs):
    ins, outs = refs[: -len(plan)], refs[-len(plan) :]
    at = 0
    for out, layers in zip(outs, plan):
        for l, pieces in enumerate(layers):
            start = 0
            for width in pieces:
                out[l, :, start : start + width] = ins[at][...]
                at, start = at + 1, start + width


def call_pack(tensors):
    flat = [a for layers in tensors for pieces in layers for a in pieces]
    plan = [[[a.shape[1] for a in pieces] for pieces in layers] for layers in tensors]
    outs = [sds((len(layers), layers[0][0].shape[0], sum(a.shape[1] for a in layers[0])), F32) for layers in tensors]
    vmem = pl.BlockSpec(memory_space=pltpu.VMEM)
    return pl.pallas_call(
        functools.partial(pack_kernel, plan),
        in_specs=[vmem] * len(flat),
        out_specs=[vmem] * len(tensors),
        out_shape=outs,
        name="pack",
    )(*flat)


def fused(inputs, segments, w_qkv, w_out, w_up, w_down, gain_attn, gain_mlp, cotangent):
    stretch = inputs.shape[1]
    slots = gain_attn.shape[1]
    rank = lax.axis_index("dp") * lax.axis_size("seq") + lax.axis_index("seq")
    own = jnp.concatenate([gain_attn, gain_mlp], 0).astype(F32)
    own = jnp.pad(own, ((0, 4), (0, 0)))
    gain_own = lax.dynamic_update_slice(jnp.zeros((8, D), F32), own, (0, rank * slots))
    bias = mask_bias(segments, stretch)

    def flat(a):
        return a.reshape((-1, a.shape[-1]))

    qkv0, sums0, prob0, o0, gains, wk0, wv0, wq0, wo0, wu0, wd0, cq1, cu1, cd1, co1 = call_enter(
        inputs, bias, gain_own, w_qkv, w_out, w_up, w_down)
    wk0, wv0, wq0, wo0, wu0, wd0 = (flat(a) for a in (wk0, wv0, wq0, wo0, wu0, wd0))
    h0, u0, x1, qkv1, raw1, wq1, wo1, wu1, wd1 = call_mid(
        inputs, o0, gains, wo0, wu0, wd0, cq1, cu1, cd1, co1)
    wq1, wo1, wu1, wd1 = (flat(a) for a in (wq1, wo1, wu1, wd1))
    sums1, prob1, o1, h1, u1, outputs = call_top(x1, qkv1, bias, raw1, gains, wo1, wu1, wd1)
    dh1, near1, total1, gd1, gu1, go1, g_mlp1 = call_base(
        cotangent, u1, h1, o1, prob1, qkv1, sums1, gains, wo1, wu1, wd1)
    dh0, dout0, gd0, gu0, go0, g_attn1, g_mlp0, sd1, su1, so1, sq1 = call_turn(
        x1, near1, dh1, u0, h0, o0, total1, gains, wq1, wo0, wu0, wd0, gd1, gu1, go1)
    dx, gsum, sd0, su0, so0, *sq0 = call_leave(
        prob0, qkv0, sums0, dout0, inputs, dh0, gains, wq0, wk0, wv0, g_mlp0, g_attn1, g_mlp1, gd0, gu0, go0)
    gq, go, gu, gd = call_pack([[sq0, [sq1]], [[so0], [so1]], [[su0], [su1]], [[sd0], [sd1]]])
    gain_share = lax.dynamic_slice(gsum, (0, rank * slots), (4, slots))
    return outputs, dx, gq, go, gu, gd, gain_share[:2], gain_share[2:]


def choose(*args):
    square = lax.axis_size("seq") == 4 * CORES
    if square and args[2].shape[1] % 16 == 0 and args[2].shape[0] == 2:
        return fused(*args)
    return on_device(*args)


def solution(mesh):
    weights = P(None, ("dp", "seq"), None)
    gains = P(None, ("dp", "seq"))
    rows = P("dp", "seq", None)
    return jax.shard_map(
        choose,
        mesh=mesh,
        in_specs=(rows, P("dp", None), weights, weights, weights, weights, gains, gains, rows),
        out_specs=(rows, rows, weights, weights, weights, weights, gains, gains),
        check_vma=False,
    )
```
